32 devices in a mesh: mode: 8 (over z, y), atom: 4 (over x, core).
Axes of the slice: x: 2, y: 2, z: 4, core: 2. Of those that a mesh axis runs over, the one named last changes fastest.
Arguments:
- vectors: bfloat16 [15360, 1024], P('atom', 'mode'), may hold values from -0.046875 to 0.046875
- couplings: float32 [4, 3, 3, 3, 5120], P(None, None, None, None, 'atom'), may hold values from -6 to 6, as said below
- neighbours: int32 [4, 5120], P(None, 'atom'), may hold values from 0 to 5119, as said below
- frequency: float32 [1024], replicated, may hold values from 1 to 2, as said below
Outputs:
- diffusivity: float32 [1024], P('mode')
The draws below stay inside these ranges and needn't reach their ends.
Inputs may be any that keep to these rules, and one draw needn't show every extreme that they name: neighbours[k, i] differs from i by 2 to 64 positions in atom order, counted around the end, upward for k < 2 and downward otherwise; the lists are mutual: neighbours[k + 2, neighbours[k, i]] = i for k < 2; some atoms in every slab have a neighbour exactly 64 positions above and some exactly 64 below. Antisymmetric bonds: couplings[k + 2, a, q, p, j] = -couplings[k, a, p, q, neighbours[k + 2, j]] for k < 2. `frequency`: strictly ascending.
All inputs are finite; a program needn't handle non-finite values.
Results may differ from the reference program's by a relative error of at most 0.00075.
Values may be sent and summed in bfloat16 or wider, within the bound.
A program may use at most 128 MiB of HBM per device.

```python
import math
import jax
import jax.numpy as jnp
from jax import lax

MODE_DEV = 128
ATOM_DEV = 1280
NEIGHBOURS = 4
HALO = 64
PARTNERS = 4
WIDTH_MODES = 320
BAND = 1024
ATOMS = 5120


def bond_table(key):
    half = NEIGHBOURS // 2
    window = HALO // 2
    offset_base = HALO - window + 1
    windows_all = ATOMS // window
    per_slab = ATOM_DEV // window
    atom_ids = jnp.arange(ATOMS, dtype=jnp.int32)
    window_ids = jnp.arange(windows_all, dtype=jnp.int32)[:, None]
    inner_ids = jnp.arange(window, dtype=jnp.int32)[None, :]
    upward_list = []
    downward_list = []
    for slot in range(half):
        scores = jax.random.randint(jax.random.fold_in(key, 31 + slot), (windows_all, window), 0, 1 << 20) * window + inner_ids
        forced = (window_ids % per_slab == 0) & (inner_ids == 0)
        scores = jnp.where(forced, (1 << 20) * window + window, scores).astype(jnp.int32)
        rank = jnp.argsort(jnp.argsort(scores, axis=1), axis=1).astype(jnp.int32).reshape(ATOMS)
        upward = jnp.mod(atom_ids + offset_base + rank - jnp.mod(atom_ids, window), ATOMS).astype(jnp.int32)
        downward = jnp.zeros((ATOMS,), jnp.int32).at[upward].set(atom_ids)
        upward_list.append(upward)
        downward_list.append(downward)
    return jnp.stack(upward_list + downward_list).astype(jnp.int32)


def draw_neighbours(key, part):
    return bond_table(key)


def draw_couplings(key, part):
    half = NEIGHBOURS // 2
    table = bond_table(key)
    base = jnp.clip(jax.random.normal(jax.random.fold_in(key, 41), (half, 3, 3, 3, ATOMS), jnp.float32), -6.0, 6.0)
    mirrored = []
    for slot in range(half):
        taken = jnp.take(base[slot], table[half + slot], axis=3)
        mirrored.append(-jnp.transpose(taken, (0, 2, 1, 3)))
    return jnp.concatenate([base, jnp.stack(mirrored)], axis=0).astype(jnp.float32)


def draw_frequency(key, part):
    gaps = jnp.exp(jax.random.uniform(jax.random.fold_in(key, 22), (BAND,), jnp.float32, jnp.log(0.25), 0.0))
    total = jnp.sum(gaps)
    position = (jnp.cumsum(gaps) - 0.5 * gaps) / total
    return (1.0 + position).astype(jnp.float32)


def shard_levels(key, shape, cuts, low, high):
    def one(axis_at, shards_of):
        steps = jax.random.uniform(jax.random.fold_in(jax.random.fold_in(key, 6), axis_at), (shards_of,), jnp.float32, low / len(cuts), high / len(cuts))
        return jnp.repeat(jnp.exp(steps), shape[axis_at] // shards_of).reshape((-1,) + (1,) * (len(shape) - axis_at - 1))

    gain = one(*cuts[0])
    for cut in cuts[1:]:
        gain = gain * one(*cut)
    return gain


def scatter_about(own_key, shape, scale, reach, split=(), held_as=jnp.bfloat16):
    level = shard_levels(own_key, shape, split, -0.22, 0.18) if split else 1.0
    drawn = jax.random.normal(own_key, shape, jnp.float32) * scale * level
    return jnp.minimum(jnp.maximum(drawn, -reach), reach).astype(held_as)


def setup_inputs(seed: int = 0) -> dict:
    keys = jax.random.split(jax.random.key(seed), 5)
    return {
        "vectors": scatter_about(keys[0], (3 * ATOMS, BAND), (3 * ATOMS) ** -0.5, 0.046875, ((0, 4), (1, 8))),
        "couplings": draw_couplings(jax.random.fold_in(keys[4], 71), 0),
        "neighbours": draw_neighbours(jax.random.fold_in(keys[4], 71), 0),
        "frequency": draw_frequency(jax.random.fold_in(keys[4], 71), 0),
    }


def velocity(padded, local_index, couplings):
    count = local_index.shape[1]
    block_width = padded.shape[2]
    coupled = jnp.transpose(couplings, (4, 0, 1, 2, 3))
    summed = jnp.zeros((count, 3, 3, block_width), jnp.float32)
    for slot in range(local_index.shape[0]):
        picked = jnp.take(padded, local_index[slot], axis=0).astype(jnp.float32)
        summed = summed + jnp.einsum("iapq,iqm->ipam", coupled[:, slot], picked)
    return summed.astype(jnp.bfloat16).reshape(count * 3, 3 * block_width)


def lorentz(offset, half_width):
    return (half_width / math.pi) / (offset * offset + half_width * half_width)


def weighted(cross_part, row_freq, col_freq, half_width):
    reshaped = cross_part.reshape(cross_part.shape[0], 3, -1)
    squares = jnp.sum(reshaped * reshaped, axis=1)
    return jnp.sum(squares * lorentz(row_freq[:, None] - col_freq[None, :], half_width), axis=1)


def reference(vectors, couplings, neighbours, frequency):
    blocks_all = BAND // MODE_DEV
    half_width = WIDTH_MODES / BAND
    rows_all = 3 * ATOMS
    stacked = vectors.reshape(ATOMS, 3, blocks_all, MODE_DEV).transpose(2, 0, 1, 3)
    applied = lax.map(lambda block_vectors: velocity(block_vectors, neighbours, couplings), stacked)
    flat = stacked.reshape(blocks_all, rows_all, MODE_DEV)
    vec_pad = jnp.concatenate([flat, jnp.zeros((PARTNERS, rows_all, MODE_DEV), flat.dtype)])
    app_pad = jnp.concatenate([applied, jnp.zeros((PARTNERS, rows_all, 3 * MODE_DEV), applied.dtype)])
    freq_pad = jnp.concatenate([frequency, jnp.ones((PARTNERS * MODE_DEV,), frequency.dtype)]).reshape(blocks_all + PARTNERS, MODE_DEV)

    def per_block(block_index):
        own_vec = lax.dynamic_index_in_dim(vec_pad, block_index, 0, keepdims=False)
        own_app = lax.dynamic_index_in_dim(app_pad, block_index, 0, keepdims=False)
        own_freq = lax.dynamic_index_in_dim(freq_pad, block_index, 0, keepdims=False)
        own_sum = weighted(jnp.dot(own_vec.T, own_app, preferred_element_type=jnp.float32), own_freq, own_freq, half_width)
        partner_list = []
        for distance in range(1, PARTNERS + 1):
            far_vec = lax.dynamic_index_in_dim(vec_pad, block_index + distance, 0, keepdims=False)
            far_app = lax.dynamic_index_in_dim(app_pad, block_index + distance, 0, keepdims=False)
            far_freq = lax.dynamic_index_in_dim(freq_pad, block_index + distance, 0, keepdims=False)
            own_sum = own_sum + weighted(jnp.dot(own_vec.T, far_app, preferred_element_type=jnp.float32), own_freq, far_freq, half_width)
            partner_list.append(weighted(jnp.dot(far_vec.T, own_app, preferred_element_type=jnp.float32), far_freq, own_freq, half_width))
        return own_sum, jnp.stack(partner_list)

    own_all, partner_all = lax.map(per_block, jnp.arange(blocks_all, dtype=jnp.int32))
    partner_pad = jnp.concatenate([jnp.zeros((PARTNERS, PARTNERS, MODE_DEV), jnp.float32), partner_all])
    for distance in range(1, PARTNERS + 1):
        own_all = own_all + partner_pad[PARTNERS - distance:PARTNERS - distance + blocks_all, distance - 1]
    freq_own = frequency.reshape(blocks_all, MODE_DEV)
    return (math.pi / (3.0 * freq_own * freq_own) * own_all).reshape(BAND)
```

```python
import functools
import math

import jax
import jax.numpy as jnp
from jax import lax
from jax.experimental import pallas as pl
from jax.experimental.pallas import tpu as pltpu
from jax.sharding import PartitionSpec as P

HALO = 64
PARTNERS = 4
WIDTH_MODES = 320
TILE = 128
WIDE = 3 * TILE
EDGE = 3 * HALO
PERIOD = 48
SLOTS = 4
MESH = pl.DeviceIdType.MESH
BF16 = jnp.bfloat16
F32 = jnp.float32

SELF_PAIRS = ((0, 0), (1, 0), (1, 1))
NEXT_PAIRS = tuple((c, b) for c in range(2) for b in range(2) if 2 + b - c <= PARTNERS)
SKIP_PAIRS = tuple((c, b) for c in range(2) for b in range(2) if 4 + c - b <= PARTNERS)
PAIRS = len(SELF_PAIRS) + len(NEXT_PAIRS) + len(SKIP_PAIRS)


def aligned(value):
    return pl.multiple_of(value, 16)


def band_groups(lane_tile):
    first = (TILE * lane_tile) // 3
    last = (TILE * lane_tile + TILE - 1) // 3
    down = range((3 * first) // PERIOD, (3 * (last + HALO - 2) + 2) // PERIOD + 1)
    up = range((3 * (HALO + first + 2)) // PERIOD, (3 * (2 * HALO + last) + 2) // PERIOD + 1)
    return down, up


def kernel(
    sizes,
    vec,
    planes_ref,
    freq_ref,
    out_ref,
    own,
    up,
    dn,
    own_t,
    up_t,
    weights,
    spread,
    expand,
    eye,
    mixed,
    pattern,
    app_own,
    app_up,
    acc_next,
    acc_skip,
    red,
    red_in,
    given,
    taken,
    local_sem,
    y_sem,
    z_sem,
    edge_sem,
    side_sem,
    red_sem,
    fin_sem,
):
    blocks_all, groups, rows_dev, modes, half_width = sizes
    rows = rows_dev // 2
    tiles = rows // WIDE
    padded = rows + 2 * EDGE
    owners = 2 * groups
    share = modes // owners

    mode = lax.axis_index("mode")
    atom = lax.axis_index("atom")
    s = mode // 2
    y = mode % 2
    other = 1 - y
    mate = mode + 1 - 2 * y
    h = (y + atom) % 2
    supers = blocks_all // 2
    has_up = s < supers - 1
    has_dn = s > 0
    outer = (atom + 2 * h - 1 + groups) % groups
    across = (atom + 1 - 2 * h + groups) % groups

    def remote(src, dst, sems, at, device):
        return pltpu.make_async_remote_copy(
            src_ref=src,
            dst_ref=dst,
            send_sem=sems.at[(0,) + at],
            recv_sem=sems.at[(1,) + at],
            device_id=device,
            device_id_type=MESH,
        )

    barrier = pltpu.get_barrier_semaphore()

    def greet(delta):
        for side in range(2):
            for slab in range(groups):
                target = (2 * (s + delta) + side, slab)
                if delta:
                    pl.semaphore_signal(barrier, inc=1, device_id=target, device_id_type=MESH)
                else:

                    @pl.when(jnp.logical_or(side != y, slab != atom))
                    def _():
                        pl.semaphore_signal(barrier, inc=1, device_id=target, device_id_type=MESH)

    greet(0)
    pl.when(has_up)(functools.partial(greet, 1))
    pl.when(has_dn)(functools.partial(greet, -1))
    sides = has_up.astype(jnp.int32) + has_dn.astype(jnp.int32)
    pl.semaphore_wait(barrier, owners - 1 + owners * sides)

    def local_copy():
        size = rows + EDGE
        return pltpu.make_async_copy(
            vec.at[pl.ds(aligned(h * (rows - EDGE)), size), :],
            own.at[y, pl.ds(aligned((1 - h) * EDGE), size), :],
            local_sem.at[0],
        )

    def y_copy(t):
        return remote(
            vec.at[pl.ds(aligned((1 - h) * rows + t * WIDE), WIDE), :],
            own.at[y, pl.ds(aligned(EDGE + t * WIDE), WIDE), :],
            y_sem,
            (t,),
            (mate, atom),
        )

    def y_edge():
        return remote(
            vec.at[pl.ds(aligned(rows - EDGE + h * EDGE), EDGE), :],
            own.at[y, pl.ds(aligned(h * (rows + EDGE)), EDGE), :],
            edge_sem,
            (0,),
            (mate, atom),
        )

    def outer_edge():
        return remote(
            vec.at[pl.ds(aligned(h * (rows_dev - EDGE)), EDGE), :],
            own.at[y, pl.ds(aligned((1 - h) * (rows + EDGE)), EDGE), :],
            edge_sem,
            (1,),
            (mode, outer),
        )

    def across_edge():
        return remote(
            vec.at[pl.ds(aligned((1 - h) * (rows_dev - EDGE)), EDGE), :],
            own.at[y, pl.ds(aligned(h * (rows + EDGE)), EDGE), :],
            edge_sem,
            (2,),
            (mate, across),
        )

    def z_copy(upward, relay, t):
        if relay:
            src = own.at[other, pl.ds(aligned(EDGE + t * WIDE), WIDE), :]
            place = other
        else:
            src = vec.at[pl.ds(aligned(h * rows + t * WIDE), WIDE), :]
            place = y
        if upward:
            dst = dn.at[place, pl.ds(aligned(t * WIDE), WIDE), :]
            return remote(src, dst, z_sem, (0, relay, t), (mode + 2, atom))
        dst = up.at[place, pl.ds(aligned(EDGE + t * WIDE), WIDE), :]
        return remote(src, dst, z_sem, (1, relay, t), (mode - 2, atom))

    def side_copy(inner):
        if inner:
            src = EDGE + (1 - h) * (rows - EDGE)
            dst = h * (rows + EDGE)
            device = (mate, atom)
        else:
            src = EDGE + h * (rows - EDGE)
            dst = (1 - h) * (rows + EDGE)
            device = (mode, outer)
        return remote(
            up.at[:, pl.ds(aligned(src), EDGE), :],
            up.at[:, pl.ds(aligned(dst), EDGE), :],
            side_sem,
            (inner,),
            device,
        )

    local_copy().start()
    order = [tiles - 1] + list(range(tiles - 1))
    for t in order:
        y_copy(t).start()

        @pl.when(has_up)
        def _():
            z_copy(1, 0, t).start()

        @pl.when(has_dn)
        def _():
            z_copy(0, 0, t).start()

    y_edge().start()
    outer_edge().start()
    across_edge().start()

    @pl.when(jnp.logical_not(has_dn))
    def _():
        taken[0:owners] = jnp.zeros((owners, 8, modes), F32)

    @pl.when(jnp.logical_not(has_up))
    def _():
        taken[2 * owners : 3 * owners] = jnp.zeros((owners, 8, modes), F32)

    row = lax.broadcasted_iota(jnp.int32, (WIDE, WIDE), 0)
    col = lax.broadcasted_iota(jnp.int32, (WIDE, WIDE), 1)
    spread[...] = jnp.where(col == 3 * (row % TILE) + row // TILE, 1.0, 0.0).astype(BF16)
    row = lax.broadcasted_iota(jnp.int32, (TILE, TILE), 0)
    col = lax.broadcasted_iota(jnp.int32, (TILE, TILE), 1)
    eye[...] = jnp.where(row == col, 1.0, 0.0).astype(BF16)
    height = 3 * SLOTS * PERIOD
    row = lax.broadcasted_iota(jnp.int32, (height + 16 * SLOTS, PERIOD), 0)
    col = lax.broadcasted_iota(jnp.int32, (height + 16 * SLOTS, PERIOD), 1)
    value_col = 3 * (row // PERIOD) + (row % PERIOD) % 3
    place_col = 9 * SLOTS + (row - height) // 16
    want = jnp.where(row < height, value_col, place_col)
    expand[...] = jnp.where(col == want, 1.0, 0.0).astype(BF16)

    first_lane = h * (rows // 3)
    stacked = []
    for t in range(tiles):
        lanes = pl.ds(pl.multiple_of(first_lane + t * TILE, TILE), TILE)
        stacked.append(jnp.concatenate([planes_ref[p, :, lanes] for p in range(3)], axis=1))
    stacked = jnp.concatenate(stacked, axis=0)
    mixed[...] = (
        jnp.dot(stacked, spread[...], preferred_element_type=F32)
        .astype(BF16)
        .reshape(tiles, PERIOD, WIDE)
    )

    atom_row = (lax.broadcasted_iota(jnp.int32, (PERIOD, TILE), 0) // 3).astype(F32).astype(BF16)
    atom_row = atom_row.reshape(3, 16, TILE)

    def build(t):
        pattern[...] = jnp.dot(expand[...], mixed[t], preferred_element_type=F32).astype(BF16)
        for lane_tile in range(3):
            lanes = slice(lane_tile * TILE, (lane_tile + 1) * TILE)
            down, above = band_groups(lane_tile)
            for g in range(2 * WIDE // PERIOD):
                slots = ([0, 1] if g in above else []) + ([2, 3] if g in down else [])
                span = slice(g * PERIOD, (g + 1) * PERIOD)
                if not slots:
                    for a in range(3):
                        weights[t, a, span, lanes] = jnp.zeros((PERIOD, TILE), BF16)
                    continue
                here = atom_row + jnp.asarray(16.0 * g, BF16)
                flags = {}
                for k in slots:
                    target = pattern[height + 16 * k : height + 16 * (k + 1), lanes]
                    flags[k] = here == target[None]
                for a in range(3):
                    total = None
                    for k in slots:
                        first = (3 * k + a) * PERIOD
                        value = pattern[first : first + PERIOD, lanes].reshape(3, 16, TILE)
                        term = jnp.where(flags[k], value, jnp.zeros_like(value))
                        total = term if total is None else total + term
                    weights[t, a, span, lanes] = total.reshape(PERIOD, TILE)

    def first_phase(step, carry):
        build(step)
        t = (step + tiles - 1) % tiles
        y_copy(t).wait_recv()

        @pl.when(has_up)
        def _():
            z_copy(1, 1, t).start()

        @pl.when(has_dn)
        def _():
            z_copy(0, 1, t).start()

        return carry

    lax.fori_loop(0, tiles, first_phase, 0)

    def transposed(source, target, u):
        span = pl.ds(pl.multiple_of(u * WIDE, WIDE), WIDE)
        for j in range(2):
            target[j * modes : (j + 1) * modes, span] = lax.dot_general(
                eye[...], source[j, span, :], (((1,), (1,)), ((), ())), preferred_element_type=F32
            ).astype(BF16)

    def apply(source_t, target, t):
        window = source_t[:, pl.ds(pl.multiple_of(t * WIDE, WIDE), 2 * WIDE)]
        for a in range(3):
            target[a * 2 * modes : (a + 1) * 2 * modes, pl.ds(pl.multiple_of(t * WIDE, WIDE), WIDE)] = (
                jnp.dot(window, weights[t, a], preferred_element_type=F32).astype(BF16)
            )

    local_copy().wait()
    y_edge().wait_recv()
    outer_edge().wait_recv()
    across_edge().wait_recv()

    def own_transpose(u, carry):
        transposed(own, own_t, u)
        return carry

    lax.fori_loop(0, tiles + 1, own_transpose, 0)

    def own_apply(t, carry):
        apply(own_t, app_own, t)
        return carry

    lax.fori_loop(0, tiles, own_apply, 0)

    def store_pairs(first, pairs, a, block):
        for at, (c, b) in enumerate(pairs):
            piece = block[c * modes : (c + 1) * modes, b * modes : (b + 1) * modes]
            index = 3 * (first + at) + a
            red[:, index] = piece.astype(BF16).reshape(owners, share, modes)

    own_main = jnp.concatenate([own[j, EDGE : EDGE + rows, :] for j in range(2)], axis=1)
    for a in range(3):
        part = app_own[a * 2 * modes : (a + 1) * 2 * modes, :]
        store_pairs(0, SELF_PAIRS, a, jnp.dot(part, own_main, preferred_element_type=F32))

    def add_next(t, start):
        far = jnp.concatenate(
            [up[j, EDGE + t * WIDE : EDGE + (t + 1) * WIDE, :] for j in range(2)], axis=1
        )
        for a in range(3):
            part = slice(a * 2 * modes, (a + 1) * 2 * modes)
            term = jnp.dot(
                app_own[part, t * WIDE : (t + 1) * WIDE], far, preferred_element_type=F32
            )
            acc_next[part, :] = term if start else acc_next[part, :] + term

    def add_skip(t, start):
        far = jnp.concatenate([dn[j, t * WIDE : (t + 1) * WIDE, :] for j in range(2)], axis=1)
        for a in range(3):
            part = slice(a * 2 * modes, (a + 1) * 2 * modes)
            term = jnp.dot(
                app_up[part, t * WIDE : (t + 1) * WIDE], far, preferred_element_type=F32
            )
            acc_skip[part, :] = term if start else acc_skip[part, :] + term

    def await_chunk(t):
        for relay in range(2):

            @pl.when(has_up)
            def _():
                z_copy(0, relay, t).wait_recv()

            @pl.when(has_dn)
            def _():
                z_copy(1, relay, t).wait_recv()

    moved = set()
    applied = []
    arrived = set()
    for at, t in enumerate(order):
        await_chunk(t)
        arrived.add(t)
        if at == 1:

            @pl.when(has_up)
            def _():
                side_copy(0).start()
                side_copy(1).start()

        add_next(t, at == 0)
        if at == 2:

            @pl.when(has_up)
            def _():
                side_copy(0).wait_recv()
                side_copy(1).wait_recv()

        if at >= 2:
            for u in range(tiles + 1):
                need = {v for v in (u - 1, u) if 0 <= v < tiles}
                if u not in moved and need <= arrived:
                    transposed(up, up_t, u)
                    moved.add(u)
            for v in range(tiles):
                if v not in applied and {v, v + 1} <= moved:
                    apply(up_t, app_up, v)
                    add_skip(v, not applied)
                    applied.append(v)

    for a in range(3):
        part = slice(a * 2 * modes, (a + 1) * 2 * modes)
        store_pairs(len(SELF_PAIRS), NEXT_PAIRS, a, acc_next[part, :])
        store_pairs(len(SELF_PAIRS) + len(NEXT_PAIRS), SKIP_PAIRS, a, acc_skip[part, :])

    stages = []
    bit = 1
    while bit < groups:
        side = (atom // bit) % 2
        stages.append((side, (mode, atom + bit * (1 - 2 * side))))
        bit *= 2
    stages.append((y, (mate, atom)))
    base = 0
    size = owners
    landing = 0
    reductions = []
    for stage, (side, device) in enumerate(stages):
        size //= 2
        keep = base + side * size
        give = base + (1 - side) * size
        copy = remote(
            red.at[pl.ds(give, size)],
            red_in.at[pl.ds(landing, size)],
            red_sem,
            (stage,),
            device,
        )
        copy.start()
        copy.wait_recv()
        reductions.append(copy)
        for i in range(size):
            red[keep + i] = (
                red[keep + i].astype(F32) + red_in[landing + i].astype(F32)
            ).astype(BF16)
        landing += size
        base = keep
    mine = base

    lane = lax.broadcasted_iota(jnp.int32, (share, modes), 1)
    spot = lane == lax.broadcasted_iota(jnp.int32, (share, modes), 0) + mine * share

    def frequency(block):
        index = jnp.clip(block, 0, blocks_all - 1)
        return freq_ref[pl.ds(index, 1), :]

    def folded(value):
        return jnp.sum(value.reshape(share // 8, 8, modes), axis=0)

    sums = [jnp.zeros((8, modes), F32) for _ in range(6)]
    index = 0
    for pairs, c_base, b_base, valid in (
        (SELF_PAIRS, 2, 2, None),
        (NEXT_PAIRS, 2, 4, has_up),
        (SKIP_PAIRS, 4, 0, jnp.logical_and(has_up, has_dn)),
    ):
        for c, b in pairs:
            squares = jnp.zeros((share, modes), F32)
            for a in range(3):
                value = red[mine, 3 * index + a].astype(F32)
                squares = squares + value * value
            index += 1
            c_row = frequency(2 * s - 2 + c_base + c)
            b_row = frequency(2 * s - 2 + b_base + b)
            c_col = jnp.sum(jnp.where(spot, c_row, 0.0), axis=1, keepdims=True)
            offset = b_row - c_col
            terms = squares * (half_width / math.pi / (offset * offset + half_width * half_width))
            if valid is not None:
                terms = jnp.where(valid, terms, 0.0)
            sums[b_base + b] = sums[b_base + b] + folded(terms)
            if c_base + c != b_base + b:
                col_sum = jnp.sum(terms, axis=1, keepdims=True)
                sums[c_base + c] = sums[c_base + c] + folded(jnp.where(spot, col_sum, 0.0))
    for i in range(6):
        given[i] = sums[i]

    rank = y * groups + atom

    def final_copy(delta, side, slab):
        slot = (1 - delta) * owners + rank
        return pltpu.make_async_remote_copy(
            src_ref=given.at[2 * (delta + 1) + side],
            dst_ref=taken.at[slot],
            send_sem=fin_sem.at[0, (delta + 1) * owners + side * groups + slab],
            recv_sem=fin_sem.at[1, slot],
            device_id=(2 * (s + delta) + side, slab),
            device_id_type=MESH,
        )

    def final_wait(delta, side, slab):
        slot = (delta + 1) * owners + side * groups + slab
        return pltpu.make_async_remote_copy(
            src_ref=given.at[0],
            dst_ref=taken.at[slot],
            send_sem=fin_sem.at[0, slot],
            recv_sem=fin_sem.at[1, slot],
            device_id=(2 * (s + delta) + side, slab),
            device_id_type=MESH,
        )

    def for_all(action):
        for delta, valid in ((0, None), (1, has_up), (-1, has_dn)):
            for side in range(2):
                for slab in range(groups):
                    if valid is None:
                        condition = jnp.logical_or(side != y, slab != atom)
                    else:
                        condition = valid
                    pl.when(condition)(functools.partial(action, delta, side, slab))

    for_all(lambda *at: final_copy(*at).start())
    taken[owners + rank] = given[2 + y]
    for_all(lambda *at: final_wait(*at).wait_recv())
    total = jnp.sum(jnp.sum(taken[...], axis=0), axis=0, keepdims=True)
    own_freq = frequency(mode)
    out_ref[...] = math.pi / (3.0 * own_freq * own_freq) * total

    for_all(lambda *at: final_copy(*at).wait_send())
    for copy in reductions:
        copy.wait_send()
    y_edge().wait_send()
    outer_edge().wait_send()
    across_edge().wait_send()
    for t in range(tiles):
        y_copy(t).wait_send()

    @pl.when(has_up)
    def _():
        side_copy(0).wait_send()
        side_copy(1).wait_send()
        for relay in range(2):
            for t in range(tiles):
                z_copy(1, relay, t).wait_send()

    @pl.when(has_dn)
    def _():
        for relay in range(2):
            for t in range(tiles):
                z_copy(0, relay, t).wait_send()


def local(vectors, couplings, neighbours, frequency):
    rows_dev, modes = vectors.shape
    atoms_dev = rows_dev // 3
    blocks_all = lax.axis_size("mode")
    groups = lax.axis_size("atom")
    total_atoms = atoms_dev * groups
    half_width = WIDTH_MODES / (modes * blocks_all)
    rows = rows_dev // 2
    tiles = rows // WIDE
    padded = rows + 2 * EDGE
    owners = 2 * groups

    here = lax.axis_index("atom") * atoms_dev + jnp.arange(atoms_dev, dtype=jnp.int32)
    offset = neighbours - here[None, :]
    offset = jnp.where(offset > HALO, offset - total_atoms, offset)
    offset = jnp.where(offset < -HALO, offset + total_atoms, offset)
    window = (offset + HALO + here[None, :] % TILE).astype(BF16)
    values = couplings.transpose(2, 0, 1, 3, 4).reshape(3, 9 * SLOTS, atoms_dev).astype(BF16)
    planes = jnp.concatenate(
        [
            values,
            jnp.broadcast_to(window[None], (3, SLOTS, atoms_dev)),
            jnp.zeros((3, PERIOD - 10 * SLOTS, atoms_dev), BF16),
        ],
        axis=1,
    )
    sizes = (blocks_all, groups, rows_dev, modes, half_width)
    dma = pltpu.SemaphoreType.DMA
    result = pl.pallas_call(
        functools.partial(kernel, sizes),
        out_shape=jax.ShapeDtypeStruct((1, modes), F32),
        in_specs=[
            pl.BlockSpec(memory_space=pl.ANY),
            pl.BlockSpec(memory_space=pltpu.VMEM),
            pl.BlockSpec(memory_space=pltpu.VMEM),
        ],
        out_specs=pl.BlockSpec(memory_space=pltpu.VMEM),
        scratch_shapes=[
            pltpu.VMEM((2, padded, modes), BF16),
            pltpu.VMEM((2, padded, modes), BF16),
            pltpu.VMEM((2, rows, modes), BF16),
            pltpu.VMEM((2 * modes, padded), BF16),
            pltpu.VMEM((2 * modes, padded), BF16),
            pltpu.VMEM((tiles, 3, 2 * WIDE, WIDE), BF16),
            pltpu.VMEM((WIDE, WIDE), BF16),
            pltpu.VMEM((3 * SLOTS * PERIOD + 16 * SLOTS, PERIOD), BF16),
            pltpu.VMEM((TILE, TILE), BF16),
            pltpu.VMEM((tiles, PERIOD, WIDE), BF16),
            pltpu.VMEM((3 * SLOTS * PERIOD + 16 * SLOTS, WIDE), BF16),
            pltpu.VMEM((6 * modes, rows), BF16),
            pltpu.VMEM((6 * modes, rows), BF16),
            pltpu.VMEM((6 * modes, 2 * modes), F32),
            pltpu.VMEM((6 * modes, 2 * modes), F32),
            pltpu.VMEM((owners, 3 * PAIRS, modes // owners, modes), BF16),
            pltpu.VMEM((owners - 1, 3 * PAIRS, modes // owners, modes), BF16),
            pltpu.VMEM((6, 8, modes), F32),
            pltpu.VMEM((3 * owners, 8, modes), F32),
            dma((1,)),
            dma((2, tiles)),
            dma((2, 2, 2, tiles)),
            dma((2, 3)),
            dma((2, 2)),
            dma((2, 4)),
            dma((2, 3 * owners)),
        ],
        compiler_params=pltpu.CompilerParams(
            collective_id=0, has_side_effects=True, vmem_limit_bytes=56 * 1024 * 1024
        ),
        name="diffusivity",
    )(vectors, planes, frequency.reshape(blocks_all, modes))
    return result.reshape(modes)


def solution(mesh):
    return jax.shard_map(
        local,
        mesh=mesh,
        in_specs=(P("atom", "mode"), P(None, None, None, None, "atom"), P(None, "atom"), P()),
        out_specs=P("mode"),
        check_vma=False,
    )
```

```python
import functools
import math

import jax
import jax.numpy as jnp
from jax import lax
from jax.experimental import pallas as pl
from jax.experimental.pallas import tpu as pltpu
from jax.sharding import PartitionSpec as P

HALO = 64
PARTNERS = 4
WIDTH_MODES = 320
TILE = 128
WIDE = 3 * TILE
EDGE = 3 * HALO
PERIOD = 48
SLOTS = 4
MESH = pl.DeviceIdType.MESH
BF16 = jnp.bfloat16
F32 = jnp.float32

SELF_PAIRS = ((0, 0), (1, 0), (1, 1))


def aligned(value):
    return pl.multiple_of(value, 16)


def band_groups(lane_tile):
    first = (TILE * lane_tile) // 3
    last = (TILE * lane_tile + TILE - 1) // 3
    down = range((3 * first) // PERIOD, (3 * (last + HALO - 2) + 2) // PERIOD + 1)
    up = range((3 * (HALO + first + 2)) // PERIOD, (3 * (2 * HALO + last) + 2) // PERIOD + 1)
    return down, up


def kernel(
    sizes,
    vec,
    couplings,
    neighbours,
    frequencies,
    out_ref,
    own,
    up,
    dn,
    own_t,
    up_t,
    raw,
    near,
    freq_ref,
    gathered,
    weights,
    spread,
    expand,
    eye,
    mixed,
    pattern,
    app_own,
    app_up,
    acc_next,
    acc_skip,
    acc_mixed,
    red_self,
    in_self,
    red_early,
    in_early,
    from_mate,
    red_next,
    in_next,
    red_skip,
    in_skip,
    in_mixed,
    given,
    taken,
    local_sem,
    y_sem,
    z_sem,
    edge_sem,
    side_sem,
    self_sem,
    early_sem,
    next_sem,
    skip_sem,
    mixed_sem,
    fin_sem,
):
    blocks_all, groups, rows_dev, modes, half_width = sizes
    rows = rows_dev // 2
    atoms = rows // 3
    tiles = rows // WIDE
    owners = 2 * groups
    share = modes // owners
    part = modes // groups

    mode = lax.axis_index("mode")
    atom = lax.axis_index("atom")
    s = mode // 2
    y = mode % 2
    other = 1 - y
    mate = mode + 1 - 2 * y
    h = (y + atom) % 2
    supers = blocks_all // 2
    has_up = s < supers - 1
    has_dn = s > 0
    outer = (atom + 2 * h - 1 + groups) % groups
    across = (atom + 1 - 2 * h + groups) % groups

    def remote(src, dst, sems, at, device):
        return pltpu.make_async_remote_copy(
            src_ref=src,
            dst_ref=dst,
            send_sem=sems.at[(0,) + at],
            recv_sem=sems.at[(1,) + at],
            device_id=device,
            device_id_type=MESH,
        )

    def local_copy():
        size = rows + EDGE
        return pltpu.make_async_copy(
            vec.at[pl.ds(aligned(h * (rows - EDGE)), size), :],
            own.at[y, pl.ds(aligned((1 - h) * EDGE), size), :],
            local_sem.at[0],
        )

    half_lanes = pl.ds(pl.multiple_of(h * atoms, TILE), atoms)
    loads = [
        pltpu.make_async_copy(couplings.at[:, :, half_lanes], raw, local_sem.at[1]),
        pltpu.make_async_copy(neighbours.at[:, half_lanes], near, local_sem.at[2]),
        pltpu.make_async_copy(frequencies, freq_ref, local_sem.at[3]),
    ]
    for load in loads:
        load.start()
    local_copy().start()

    barrier = pltpu.get_barrier_semaphore()

    def greet(device):
        pl.semaphore_signal(barrier, inc=1, device_id=device, device_id_type=MESH)

    pl.when(has_up)(lambda: greet((mode + 2, atom)))
    pl.when(has_dn)(lambda: greet((mode - 2, atom)))
    for step in range(groups):
        slab = (atom + step) % groups
        greet((mate, slab))
        if step:
            greet((mode, slab))
    sides = has_up.astype(jnp.int32) + has_dn.astype(jnp.int32)
    pl.semaphore_wait(barrier, owners - 1 + sides)

    def y_copy(t):
        return remote(
            vec.at[pl.ds(aligned((1 - h) * rows + t * WIDE), WIDE), :],
            own.at[y, pl.ds(aligned(EDGE + t * WIDE), WIDE), :],
            y_sem,
            (t,),
            (mate, atom),
        )

    def y_edge():
        return remote(
            vec.at[pl.ds(aligned(rows - EDGE + h * EDGE), EDGE), :],
            own.at[y, pl.ds(aligned(h * (rows + EDGE)), EDGE), :],
            edge_sem,
            (0,),
            (mate, atom),
        )

    def outer_edge():
        return remote(
            vec.at[pl.ds(aligned(h * (rows_dev - EDGE)), EDGE), :],
            own.at[y, pl.ds(aligned((1 - h) * (rows + EDGE)), EDGE), :],
            edge_sem,
            (1,),
            (mode, outer),
        )

    def across_edge():
        return remote(
            vec.at[pl.ds(aligned((1 - h) * (rows_dev - EDGE)), EDGE), :],
            own.at[y, pl.ds(aligned(h * (rows + EDGE)), EDGE), :],
            edge_sem,
            (2,),
            (mate, across),
        )

    def z_copy(upward, relay, t):
        if relay:
            src = own.at[other, pl.ds(aligned(EDGE + t * WIDE), WIDE), :]
        else:
            src = vec.at[pl.ds(aligned(h * rows + t * WIDE), WIDE), :]
        if upward:
            dst = dn.at[relay, pl.ds(aligned(t * WIDE), WIDE), :]
            return remote(src, dst, z_sem, (0, relay, t), (mode + 2, atom))
        dst = up.at[relay, pl.ds(aligned(EDGE + t * WIDE), WIDE), :]
        return remote(src, dst, z_sem, (1, relay, t), (mode - 2, atom))

    def side_copy(relay, inner):
        if inner:
            src = EDGE + (1 - h) * (rows - EDGE)
            dst = h * (rows + EDGE)
            device = (mate, atom)
            place = 1 - relay
        else:
            src = EDGE + h * (rows - EDGE)
            dst = (1 - h) * (rows + EDGE)
            device = (mode, outer)
            place = relay
        return pltpu.make_async_remote_copy(
            src_ref=up.at[relay, pl.ds(aligned(src), EDGE), :],
            dst_ref=up.at[place, pl.ds(aligned(dst), EDGE), :],
            send_sem=side_sem.at[0, relay, inner],
            recv_sem=side_sem.at[1, place, inner],
            device_id=device,
            device_id_type=MESH,
        )

    def side_wait(place, inner):
        return pltpu.make_async_remote_copy(
            src_ref=up.at[place, pl.ds(0, EDGE), :],
            dst_ref=up.at[place, pl.ds(0, EDGE), :],
            send_sem=side_sem.at[0, place, inner],
            recv_sem=side_sem.at[1, place, inner],
            device_id=(mate, atom),
            device_id_type=MESH,
        )

    order = [tiles - 1] + list(range(tiles - 1))
    for at, t in enumerate(order):
        y_copy(t).start()

        @pl.when(has_up)
        def _():
            z_copy(1, 0, t).start()

        @pl.when(has_dn)
        def _():
            z_copy(0, 0, t).start()

        if at == 1:
            y_edge().start()
            outer_edge().start()
            across_edge().start()

    @pl.when(jnp.logical_not(has_dn))
    def _():
        taken[0:owners] = jnp.zeros((owners, 8, modes), F32)

    @pl.when(jnp.logical_not(has_up))
    def _():
        taken[2 * owners : 3 * owners] = jnp.zeros((owners, 8, modes), F32)

    given[...] = jnp.zeros((6, 8, modes), F32)

    row = lax.broadcasted_iota(jnp.int32, (WIDE, WIDE), 0)
    col = lax.broadcasted_iota(jnp.int32, (WIDE, WIDE), 1)
    spread[...] = jnp.where(col == 3 * (row % TILE) + row // TILE, 1.0, 0.0).astype(BF16)
    row = lax.broadcasted_iota(jnp.int32, (TILE, TILE), 0)
    col = lax.broadcasted_iota(jnp.int32, (TILE, TILE), 1)
    eye[...] = jnp.where(row == col, 1.0, 0.0).astype(BF16)
    height = 3 * SLOTS * PERIOD
    row = lax.broadcasted_iota(jnp.int32, (height + 16 * SLOTS, PERIOD), 0)
    col = lax.broadcasted_iota(jnp.int32, (height + 16 * SLOTS, PERIOD), 1)
    pair = row // PERIOD
    value_col = (3 * (pair % 3) + (row % PERIOD) % 3) * SLOTS + pair // 3
    place_col = 9 * SLOTS + (row - height) // 16
    want = jnp.where(row < height, value_col, place_col)
    expand[...] = jnp.where(col == want, 1.0, 0.0).astype(BF16)

    for load in loads:
        load.wait()
    lane = lax.broadcasted_iota(jnp.int32, (SLOTS, atoms), 1)
    here = atom * (2 * atoms) + h * atoms + lane
    offset = near[...] - here
    total_atoms = 2 * atoms * groups
    offset = jnp.where(offset > HALO, offset - total_atoms, offset)
    offset = jnp.where(offset < -HALO, offset + total_atoms, offset)
    place = (offset + HALO + lane % TILE).astype(F32)
    for p in range(3):
        for a in range(3):
            for q in range(3):
                first = SLOTS * (3 * a + q)
                gathered[p, first : first + SLOTS, :] = raw[9 * a + 3 * p + q]
        gathered[p, 9 * SLOTS : 10 * SLOTS, :] = place
        gathered[p, 10 * SLOTS : PERIOD, :] = jnp.zeros((PERIOD - 10 * SLOTS, atoms), F32)
    stacked = []
    for t in range(tiles):
        lanes = slice(t * TILE, (t + 1) * TILE)
        stacked.append(
            jnp.concatenate([gathered[p, :, lanes].astype(BF16) for p in range(3)], axis=1)
        )
    stacked = jnp.concatenate(stacked, axis=0)
    mixed[...] = (
        jnp.dot(stacked, spread[...], preferred_element_type=F32)
        .astype(BF16)
        .reshape(tiles, PERIOD, WIDE)
    )

    atom_row = (lax.broadcasted_iota(jnp.int32, (PERIOD, TILE), 0) // 3).astype(F32).astype(BF16)
    atom_row = atom_row.reshape(3, 16, TILE)

    def build(t):
        pattern[...] = jnp.dot(expand[...], mixed[t], preferred_element_type=F32).astype(BF16)
        for lane_tile in range(3):
            lanes = slice(lane_tile * TILE, (lane_tile + 1) * TILE)
            down, above = band_groups(lane_tile)
            for g in range(2 * WIDE // PERIOD):
                slots = ([0, 1] if g in above else []) + ([2, 3] if g in down else [])
                span = slice(g * PERIOD, (g + 1) * PERIOD)
                if not slots:
                    for a in range(3):
                        weights[t, a, span, lanes] = jnp.zeros((PERIOD, TILE), BF16)
                    continue
                here = atom_row + jnp.asarray(16.0 * g, BF16)
                flags = {}
                for k in slots:
                    target = pattern[height + 16 * k : height + 16 * (k + 1), lanes]
                    flags[k] = here == target[None]
                for a in range(3):
                    total = None
                    for k in slots:
                        first = (3 * k + a) * PERIOD
                        value = pattern[first : first + PERIOD, lanes].reshape(3, 16, TILE)
                        term = jnp.where(flags[k], value, jnp.zeros_like(value))
                        total = term if total is None else total + term
                    weights[t, a, span, lanes] = total.reshape(PERIOD, TILE)

    def build_step(t, carry):
        build(t)
        return carry

    lax.fori_loop(0, tiles, build_step, 0)

    def transposed(source, target, u):
        span = pl.ds(pl.multiple_of(u * WIDE, WIDE), WIDE)
        target[:, span] = lax.dot_general(
            eye[...], source[span, :], (((1,), (1,)), ((), ())), preferred_element_type=F32
        ).astype(BF16)

    def apply_own(t):
        window = own_t[:, t * WIDE : (t + 2) * WIDE]
        for a in range(3):
            app_own[a * 2 * modes : (a + 1) * 2 * modes, t * WIDE : (t + 1) * WIDE] = jnp.dot(
                window, weights[t, a], preferred_element_type=F32
            ).astype(BF16)

    def apply_up(relay, t):
        window = up_t[relay, :, t * WIDE : (t + 2) * WIDE]
        for a in range(3):
            app_up[relay, a * modes : (a + 1) * modes, t * WIDE : (t + 1) * WIDE] = jnp.dot(
                window, weights[t, a], preferred_element_type=F32
            ).astype(BF16)

    def schedule(arrived, edges, moved, done):
        blocks = []
        for u in range(tiles + 1):
            need = {v for v in (u - 1, u) if 0 <= v < tiles}
            if u not in moved and need <= arrived and (edges or 0 < u < tiles):
                blocks.append(u)
                moved.add(u)
        ready = [v for v in range(tiles) if v not in done and {v, v + 1} <= moved]
        done.update(ready)
        return blocks, ready

    def own_step(arrived, edges, moved, done):
        blocks, ready = schedule(arrived, edges, moved, done)
        for u in blocks:
            for j in range(2):
                transposed(own.at[j], own_t.at[j * modes : (j + 1) * modes], u)
        for v in ready:
            apply_own(v)

    local_copy().wait()
    moved, done, arrived = set(), set(), set()
    for at, t in enumerate(order):
        y_copy(t).wait_recv()

        @pl.when(has_up)
        def _():
            z_copy(1, 1, t).start()

        @pl.when(has_dn)
        def _():
            z_copy(0, 1, t).start()

        arrived.add(t)
        if at == 3:
            y_edge().wait_recv()
            outer_edge().wait_recv()
            across_edge().wait_recv()
        if at == 2:

            @pl.when(has_up)
            def _():
                for v in order[:2]:
                    z_copy(0, 0, v).wait_recv()
                side_copy(0, 0).start()
                side_copy(0, 1).start()

        own_step(arrived, at >= 3, moved, done)

    bits = []
    bit = 1
    while bit < groups:
        side = (atom // bit) % 2
        bits.append((side, (mode, atom + bit * (1 - 2 * side))))
        bit *= 2
    mate_bit = (y, (mate, atom))

    class Halving:
        def __init__(self, buffer, landing, sems, stages):
            self.buffer, self.landing, self.sems, self.stages = buffer, landing, sems, stages
            self.base, self.size, self.at, self.stage = 0, buffer.shape[0], 0, 0
            self.copies = []

        def send(self):
            side, device = self.stages[self.stage]
            self.size //= 2
            self.keep = self.base + side * self.size
            copy = remote(
                self.buffer.at[pl.ds(self.base + (1 - side) * self.size, self.size)],
                self.landing.at[pl.ds(self.at, self.size)],
                self.sems,
                (self.stage,),
                device,
            )
            copy.start()
            self.copies.append(copy)

        def receive(self):
            self.copies[-1].wait_recv()
            for i in range(self.size):
                self.buffer[self.keep + i] = (
                    self.buffer[self.keep + i].astype(F32)
                    + self.landing[self.at + i].astype(F32)
                ).astype(BF16)
            self.at += self.size
            self.base = self.keep
            self.stage += 1

    def store(buffer, index, piece):
        count = buffer.shape[0]
        buffer[:, index] = piece.astype(BF16).reshape(count, modes // count, modes)

    own_main = jnp.concatenate([own[j, EDGE : EDGE + rows, :] for j in range(2)], axis=1)
    for a in range(3):
        product = jnp.dot(
            app_own[a * 2 * modes : (a + 1) * 2 * modes, :],
            own_main,
            preferred_element_type=F32,
        )
        for at, (c, b) in enumerate(SELF_PAIRS):
            store(
                red_self,
                3 * at + a,
                product[c * modes : (c + 1) * modes, b * modes : (b + 1) * modes],
            )
    self_sum = Halving(red_self, in_self, self_sem, bits + [mate_bit])
    self_sum.send()

    def await_chunks(relay, from_up, from_dn):
        @pl.when(has_up)
        def _():
            for t in from_up:
                z_copy(0, relay, t).wait_recv()

        @pl.when(has_dn)
        def _():
            for t in from_dn:
                z_copy(1, relay, t).wait_recv()

    await_chunks(0, order[2:], order)
    for a in range(3):
        product = jnp.dot(
            app_own[a * 2 * modes : (a + 1) * 2 * modes, :],
            up[0, EDGE : EDGE + rows, :],
            preferred_element_type=F32,
        )
        for c in range(2):
            store(red_early, 3 * c + a, product[c * modes : (c + 1) * modes])
    self_sum.receive()
    self_sum.send()

    @pl.when(has_up)
    def _():
        side_wait(0, 0).wait_recv()

    for u in range(1, tiles):
        transposed(up.at[0], up_t.at[0], u)
    for v in range(1, tiles - 1):
        apply_up(0, v)

    def add_next(t, start):
        for a in range(3):
            rows_a = slice(a * 2 * modes, (a + 1) * 2 * modes)
            term = jnp.dot(
                app_own[rows_a, t * WIDE : (t + 1) * WIDE],
                up[1, EDGE + t * WIDE : EDGE + (t + 1) * WIDE, :],
                preferred_element_type=F32,
            )
            acc_next[rows_a, :] = term if start else acc_next[rows_a, :] + term

    def add_skip(t, start):
        span = slice(t * WIDE, (t + 1) * WIDE)
        term = jnp.dot(app_up[1, :, span], dn[1, span, :], preferred_element_type=F32)
        acc_skip[...] = term if start else acc_skip[...] + term
        term = jnp.dot(app_up[y, :, span], dn[other, span, :], preferred_element_type=F32)
        acc_mixed[...] = term if start else acc_mixed[...] + term

    early_sum = Halving(red_early, in_early, early_sem, bits)

    def hand_over():
        return remote(red_early.at[early_sum.base], from_mate, early_sem, (len(bits),), mate_bit[1])

    def finish_direct():
        @pl.when(has_up)
        def _():
            side_wait(0, 1).wait_recv()

        for u in (0, tiles):
            transposed(up.at[0], up_t.at[0], u)
        for v in (0, tiles - 1):
            apply_up(0, v)
        product = jnp.dot(app_up[0], dn[0], preferred_element_type=F32)
        for a in range(3):
            store(red_early, 6 + a, product[a * modes : (a + 1) * modes])

    moved, done, arrived = set(), set(), set()
    started = False
    for at, t in enumerate(order):
        await_chunks(1, [t], [t])
        arrived.add(t)
        if at == 1:

            @pl.when(has_up)
            def _():
                side_copy(1, 0).start()
                side_copy(1, 1).start()

        add_next(t, at == 0)
        if at == 1:
            self_sum.receive()
            self_sum.send()
        if at == 2:
            finish_direct()
            early_sum.send()

            @pl.when(has_up)
            def _():
                side_wait(1, 0).wait_recv()
                side_wait(1, 1).wait_recv()

        if at == 3:
            self_sum.receive()
            early_sum.receive()
            early_sum.send()
        if at == tiles - 1:
            early_sum.receive()
            handed = hand_over()
            handed.start()
            for a in range(3):
                for c in range(2):
                    first = a * 2 * modes + c * modes
                    store(red_next, 3 * c + a, acc_next[first : first + modes, :])
            next_sum = Halving(red_next, in_next, next_sem, bits)
            next_sum.send()
        if at >= 2:
            blocks, ready = schedule(arrived, True, moved, done)
            for u in blocks:
                transposed(up.at[1], up_t.at[1], u)
            for v in ready:
                apply_up(1, v)
                add_skip(v, not started)
                started = True

    for a in range(3):
        rows_a = slice(a * modes, (a + 1) * modes)
        store(red_skip, a, acc_skip[rows_a, :])
        store(red_skip, 3 + a, acc_mixed[rows_a, :])
    skip_sum = Halving(red_skip, in_skip, skip_sem, bits[:-1])
    for _ in bits[:-1]:
        skip_sum.send()
        next_sum.receive()
        next_sum.send()
        skip_sum.receive()
    side, last = bits[-1]
    keep = skip_sum.base + side
    pass_on = skip_sum.base + 1 - side
    mine_rows = pl.ds(aligned(y * share), share)
    mate_rows = pl.ds(aligned(other * share), share)
    last_copies = [
        remote(
            red_skip.at[pass_on, pl.ds(0, 3)],
            in_skip.at[in_skip.shape[0] - 1, pl.ds(0, 3)],
            mixed_sem,
            (0,),
            last,
        ),
        remote(
            red_skip.at[pass_on, pl.ds(3, 3), mine_rows], in_mixed.at[0], mixed_sem, (1,), last
        ),
        remote(
            red_skip.at[keep, pl.ds(3, 3), mate_rows], in_mixed.at[1], mixed_sem, (2,), mate_bit[1]
        ),
        remote(
            red_skip.at[pass_on, pl.ds(3, 3), mate_rows],
            in_mixed.at[2],
            mixed_sem,
            (3,),
            (mate, last[1]),
        ),
    ]
    for copy in last_copies:
        copy.start()

    def frequency(block):
        index = jnp.clip(block, 0, blocks_all - 1)
        return freq_ref[pl.ds(index, 1), :]

    def account(values, first_row, count, c_index, b_index, valid, same=False):
        lane = lax.broadcasted_iota(jnp.int32, (count, modes), 1)
        spot = lane == lax.broadcasted_iota(jnp.int32, (count, modes), 0) + first_row
        squares = None
        for value in values:
            square = value * value
            squares = square if squares is None else squares + square
        c_row = frequency(2 * s - 2 + c_index)
        b_row = frequency(2 * s - 2 + b_index)
        c_col = jnp.sum(jnp.where(spot, c_row, 0.0), axis=1, keepdims=True)
        offset = b_row - c_col
        terms = squares * (half_width / math.pi / (offset * offset + half_width * half_width))
        if valid is not None:
            terms = jnp.where(valid, terms, 0.0)

        def folded(value):
            return jnp.sum(value.reshape(count // 8, 8, modes), axis=0)

        given[b_index] = given[b_index] + folded(terms)
        if not same:
            col_sum = jnp.sum(terms, axis=1, keepdims=True)
            given[c_index] = given[c_index] + folded(jnp.where(spot, col_sum, 0.0))

    for at, (c, b) in enumerate(SELF_PAIRS):
        values = [red_self[self_sum.base, 3 * at + a].astype(F32) for a in range(3)]
        account(values, self_sum.base * share, share, 2 + c, 2 + b, None, c == b)

    handed.wait_recv()
    next_sum.receive()
    spot_row = next_sum.base * part
    for c in range(2):
        values = [
            red_next[next_sum.base, 3 * c + a].astype(F32) + from_mate[3 * c + a].astype(F32)
            for a in range(3)
        ]
        account(values, spot_row, part, 2 + c, 4 + other, has_up)

    both = jnp.logical_and(has_up, has_dn)
    for copy in last_copies:
        copy.wait_recv()
    values = [
        red_skip[keep, a].astype(F32)
        + in_skip[in_skip.shape[0] - 1, a].astype(F32)
        + from_mate[6 + a].astype(F32)
        for a in range(3)
    ]
    account(values, keep * part, part, 4 + other, other, both)
    values = []
    for a in range(3):
        value = red_skip[keep, 3 + a, mine_rows].astype(F32)
        for i in range(3):
            value = value + in_mixed[i, a].astype(F32)
        values.append(value)
    account(values, keep * part + y * share, share, 4, 1, both)

    rank = y * groups + atom

    def final_copy(delta, side, slab):
        slot = (1 - delta) * owners + rank
        return pltpu.make_async_remote_copy(
            src_ref=given.at[2 * (delta + 1) + side],
            dst_ref=taken.at[slot],
            send_sem=fin_sem.at[0, (delta + 1) * owners + side * groups + slab],
            recv_sem=fin_sem.at[1, slot],
            device_id=(2 * (s + delta) + side, slab),
            device_id_type=MESH,
        )

    def final_wait(delta, side, slab):
        slot = (delta + 1) * owners + side * groups + slab
        return pltpu.make_async_remote_copy(
            src_ref=given.at[0],
            dst_ref=taken.at[slot],
            send_sem=fin_sem.at[0, slot],
            recv_sem=fin_sem.at[1, slot],
            device_id=(2 * (s + delta) + side, slab),
            device_id_type=MESH,
        )

    def for_all(action):
        for delta, valid in ((0, None), (1, has_up), (-1, has_dn)):
            for side in range(2):
                for slab in range(groups):
                    if valid is None:
                        condition = jnp.logical_or(side != y, slab != atom)
                    else:
                        condition = valid
                    pl.when(condition)(functools.partial(action, delta, side, slab))

    for_all(lambda *at: final_copy(*at).start())
    taken[owners + rank] = given[2 + y]
    for_all(lambda *at: final_wait(*at).wait_recv())
    total = jnp.sum(jnp.sum(taken[...], axis=0), axis=0, keepdims=True)
    own_freq = frequency(mode)
    out_ref[...] = total / (own_freq * own_freq)

    for_all(lambda *at: final_copy(*at).wait_send())
    for copy in self_sum.copies + early_sum.copies + next_sum.copies + skip_sum.copies:
        copy.wait_send()
    for copy in last_copies + [handed]:
        copy.wait_send()
    y_edge().wait_send()
    outer_edge().wait_send()
    across_edge().wait_send()
    for t in range(tiles):
        y_copy(t).wait_send()

    @pl.when(has_up)
    def _():
        for relay in range(2):
            side_copy(relay, 0).wait_send()
            side_copy(relay, 1).wait_send()
            for t in range(tiles):
                z_copy(1, relay, t).wait_send()

    @pl.when(has_dn)
    def _():
        for relay in range(2):
            for t in range(tiles):
                z_copy(0, relay, t).wait_send()


def local(vectors, couplings, neighbours, frequency):
    rows_dev, modes = vectors.shape
    blocks_all = lax.axis_size("mode")
    groups = lax.axis_size("atom")
    half_width = WIDTH_MODES / (modes * blocks_all)
    rows = rows_dev // 2
    tiles = rows // WIDE
    padded = rows + 2 * EDGE
    owners = 2 * groups
    share = modes // owners
    part = modes // groups
    levels = groups.bit_length() - 1

    blocks = couplings.transpose(1, 2, 3, 0, 4).reshape(27, SLOTS, rows_dev // 3)
    sizes = (blocks_all, groups, rows_dev, modes, half_width)
    dma = pltpu.SemaphoreType.DMA
    result = pl.pallas_call(
        functools.partial(kernel, sizes),
        out_shape=jax.ShapeDtypeStruct((1, modes), F32),
        in_specs=[pl.BlockSpec(memory_space=pltpu.HBM)] * 4,
        out_specs=pl.BlockSpec(memory_space=pltpu.VMEM),
        scratch_shapes=[
            pltpu.VMEM((2, padded, modes), BF16),
            pltpu.VMEM((2, padded, modes), BF16),
            pltpu.VMEM((2, rows, modes), BF16),
            pltpu.VMEM((2 * modes, padded), BF16),
            pltpu.VMEM((2, modes, padded), BF16),
            pltpu.VMEM((27, SLOTS, rows // 3), F32),
            pltpu.VMEM((SLOTS, rows // 3), jnp.int32),
            pltpu.VMEM((blocks_all, modes), F32),
            pltpu.VMEM((3, PERIOD, rows // 3), F32),
            pltpu.VMEM((tiles, 3, 2 * WIDE, WIDE), BF16),
            pltpu.VMEM((WIDE, WIDE), BF16),
            pltpu.VMEM((3 * SLOTS * PERIOD + 16 * SLOTS, PERIOD), BF16),
            pltpu.VMEM((TILE, TILE), BF16),
            pltpu.VMEM((tiles, PERIOD, WIDE), BF16),
            pltpu.VMEM((3 * SLOTS * PERIOD + 16 * SLOTS, WIDE), BF16),
            pltpu.VMEM((6 * modes, rows), BF16),
            pltpu.VMEM((2, 3 * modes, rows), BF16),
            pltpu.VMEM((6 * modes, modes), F32),
            pltpu.VMEM((3 * modes, modes), F32),
            pltpu.VMEM((3 * modes, modes), F32),
            pltpu.VMEM((owners, 9, share, modes), BF16),
            pltpu.VMEM((owners - 1, 9, share, modes), BF16),
            pltpu.VMEM((groups, 9, part, modes), BF16),
            pltpu.VMEM((groups - 1, 9, part, modes), BF16),
            pltpu.VMEM((9, part, modes), BF16),
            pltpu.VMEM((groups, 6, part, modes), BF16),
            pltpu.VMEM((groups - 1, 6, part, modes), BF16),
            pltpu.VMEM((groups, 6, part, modes), BF16),
            pltpu.VMEM((groups - 1, 6, part, modes), BF16),
            pltpu.VMEM((3, 3, share, modes), BF16),
            pltpu.VMEM((6, 8, modes), F32),
            pltpu.VMEM((3 * owners, 8, modes), F32),
            dma((4,)),
            dma((2, tiles)),
            dma((2, 2, 2, tiles)),
            dma((2, 3)),
            dma((2, 2, 2)),
            dma((2, levels + 1)),
            dma((2, levels + 1)),
            dma((2, levels)),
            dma((2, levels)),
            dma((2, 4)),
            dma((2, 3 * owners)),
        ],
        compiler_params=pltpu.CompilerParams(
            collective_id=0, has_side_effects=True, vmem_limit_bytes=56 * 1024 * 1024
        ),
        name="diffusivity",
    )(vectors, blocks, neighbours, frequency.reshape(blocks_all, modes))
    return result.reshape(modes) * (math.pi / 3.0)


def solution(mesh):
    return jax.shard_map(
        local,
        mesh=mesh,
        in_specs=(P("atom", "mode"), P(None, None, None, None, "atom"), P(None, "atom"), P()),
        out_specs=P("mode"),
        check_vma=False,
    )
```

```python
import functools
import math

import jax
import jax.numpy as jnp
from jax import lax
from jax.experimental import pallas as pl
from jax.experimental.pallas import tpu as pltpu
from jax.sharding import PartitionSpec as P

HALO = 64
PARTNERS = 4
WIDTH_MODES = 320
TILE = 128
WIDE = 3 * TILE
EDGE = 3 * HALO
PERIOD = 48
SLOTS = 4
MESH = pl.DeviceIdType.MESH
BF16 = jnp.bfloat16
F32 = jnp.float32

SELF_PAIRS = ((0, 0), (1, 0), (1, 1))


def aligned(value):
    return pl.multiple_of(value, 16)


def band_groups(lane_tile):
    first = (TILE * lane_tile) // 3
    last = (TILE * lane_tile + TILE - 1) // 3
    down = range((3 * first) // PERIOD, (3 * (last + HALO - 2) + 2) // PERIOD + 1)
    up = range((3 * (HALO + first + 2)) // PERIOD, (3 * (2 * HALO + last) + 2) // PERIOD + 1)
    return down, up


def kernel(
    sizes,
    vec,
    couplings,
    neighbours,
    frequencies,
    out_ref,
    own,
    up,
    dn,
    own_t,
    up_t,
    raw,
    near,
    freq_ref,
    gathered,
    weights,
    spread,
    expand,
    eye,
    mixed,
    pattern,
    app_own,
    app_up,
    acc_next,
    acc_skip,
    acc_mixed,
    red_self,
    in_self,
    red_early,
    in_early,
    red_direct,
    in_direct,
    from_mate,
    red_next,
    in_next,
    red_skip,
    in_skip,
    in_mixed,
    given,
    packed,
    taken,
    local_sem,
    y_sem,
    z_sem,
    edge_sem,
    side_sem,
    self_sem,
    early_sem,
    direct_sem,
    next_sem,
    skip_sem,
    mixed_sem,
    fin_sem,
):
    blocks_all, groups, rows_dev, modes, half_width = sizes
    rows = rows_dev // 2
    atoms = rows // 3
    tiles = rows // WIDE
    owners = 2 * groups
    share = modes // owners
    part = modes // groups

    mode = lax.axis_index("mode")
    atom = lax.axis_index("atom")
    s = mode // 2
    y = mode % 2
    other = 1 - y
    mate = mode + 1 - 2 * y
    h = (y + atom) % 2
    supers = blocks_all // 2
    has_up = s < supers - 1
    has_dn = s > 0
    outer = (atom + 2 * h - 1 + groups) % groups
    across = (atom + 1 - 2 * h + groups) % groups

    def remote(src, dst, sems, at, device):
        return pltpu.make_async_remote_copy(
            src_ref=src,
            dst_ref=dst,
            send_sem=sems.at[(0,) + at],
            recv_sem=sems.at[(1,) + at],
            device_id=device,
            device_id_type=MESH,
        )

    def local_copy():
        size = rows + EDGE
        return pltpu.make_async_copy(
            vec.at[pl.ds(aligned(h * (rows - EDGE)), size), :],
            own.at[y, pl.ds(aligned((1 - h) * EDGE), size), :],
            local_sem.at[0],
        )

    half_lanes = pl.ds(pl.multiple_of(h * atoms, TILE), atoms)
    loads = [
        pltpu.make_async_copy(couplings.at[:, :, half_lanes], raw, local_sem.at[1]),
        pltpu.make_async_copy(neighbours.at[:, half_lanes], near, local_sem.at[2]),
        pltpu.make_async_copy(frequencies, freq_ref, local_sem.at[3]),
    ]
    for load in loads:
        load.start()
    local_copy().start()

    barrier = pltpu.get_barrier_semaphore()

    def greet(device):
        pl.semaphore_signal(barrier, inc=1, device_id=device, device_id_type=MESH)

    pl.when(has_up)(lambda: greet((mode + 2, atom)))
    pl.when(has_dn)(lambda: greet((mode - 2, atom)))
    for step in range(groups):
        slab = (atom + step) % groups
        greet((mate, slab))
        if step:
            greet((mode, slab))
    sides = has_up.astype(jnp.int32) + has_dn.astype(jnp.int32)
    pl.semaphore_wait(barrier, owners - 1 + sides)

    def y_copy(t):
        return remote(
            vec.at[pl.ds(aligned((1 - h) * rows + t * WIDE), WIDE), :],
            own.at[y, pl.ds(aligned(EDGE + t * WIDE), WIDE), :],
            y_sem,
            (t,),
            (mate, atom),
        )

    def y_edge():
        return remote(
            vec.at[pl.ds(aligned(rows - EDGE + h * EDGE), EDGE), :],
            own.at[y, pl.ds(aligned(h * (rows + EDGE)), EDGE), :],
            edge_sem,
            (0,),
            (mate, atom),
        )

    def outer_edge():
        return remote(
            vec.at[pl.ds(aligned(h * (rows_dev - EDGE)), EDGE), :],
            own.at[y, pl.ds(aligned((1 - h) * (rows + EDGE)), EDGE), :],
            edge_sem,
            (1,),
            (mode, outer),
        )

    def across_edge():
        return remote(
            vec.at[pl.ds(aligned((1 - h) * (rows_dev - EDGE)), EDGE), :],
            own.at[y, pl.ds(aligned(h * (rows + EDGE)), EDGE), :],
            edge_sem,
            (2,),
            (mate, across),
        )

    def z_copy(upward, relay, t):
        if relay:
            src = own.at[other, pl.ds(aligned(EDGE + t * WIDE), WIDE), :]
        else:
            src = vec.at[pl.ds(aligned(h * rows + t * WIDE), WIDE), :]
        if upward:
            dst = dn.at[relay, pl.ds(aligned(t * WIDE), WIDE), :]
            return remote(src, dst, z_sem, (0, relay, t), (mode + 2, atom))
        dst = up.at[relay, pl.ds(aligned(EDGE + t * WIDE), WIDE), :]
        return remote(src, dst, z_sem, (1, relay, t), (mode - 2, atom))

    def side_copy(relay, inner):
        if inner:
            src = EDGE + (1 - h) * (rows - EDGE)
            dst = h * (rows + EDGE)
            device = (mate, atom)
            place = 1 - relay
        else:
            src = EDGE + h * (rows - EDGE)
            dst = (1 - h) * (rows + EDGE)
            device = (mode, outer)
            place = relay
        return pltpu.make_async_remote_copy(
            src_ref=up.at[relay, pl.ds(aligned(src), EDGE), :],
            dst_ref=up.at[place, pl.ds(aligned(dst), EDGE), :],
            send_sem=side_sem.at[0, relay, inner],
            recv_sem=side_sem.at[1, place, inner],
            device_id=device,
            device_id_type=MESH,
        )

    def side_wait(place, inner):
        return pltpu.make_async_remote_copy(
            src_ref=up.at[place, pl.ds(0, EDGE), :],
            dst_ref=up.at[place, pl.ds(0, EDGE), :],
            send_sem=side_sem.at[0, place, inner],
            recv_sem=side_sem.at[1, place, inner],
            device_id=(mate, atom),
            device_id_type=MESH,
        )

    order = [tiles - 1] + list(range(tiles - 1))
    for at, t in enumerate(order):
        y_copy(t).start()

        @pl.when(has_up)
        def _():
            z_copy(1, 0, t).start()

        @pl.when(has_dn)
        def _():
            z_copy(0, 0, t).start()

        if at == 1:
            y_edge().start()
            outer_edge().start()
            across_edge().start()

    @pl.when(jnp.logical_not(has_dn))
    def _():
        taken[0:owners] = jnp.zeros((owners, 8, modes), F32)

    @pl.when(jnp.logical_not(has_up))
    def _():
        taken[2 * owners : 3 * owners] = jnp.zeros((owners, 8, modes), F32)

    given[...] = jnp.zeros((6, 8, modes), F32)

    row = lax.broadcasted_iota(jnp.int32, (WIDE, WIDE), 0)
    col = lax.broadcasted_iota(jnp.int32, (WIDE, WIDE), 1)
    spread[...] = jnp.where(col == 3 * (row % TILE) + row // TILE, 1.0, 0.0).astype(BF16)
    row = lax.broadcasted_iota(jnp.int32, (TILE, TILE), 0)
    col = lax.broadcasted_iota(jnp.int32, (TILE, TILE), 1)
    eye[...] = jnp.where(row == col, 1.0, 0.0).astype(BF16)
    height = 3 * SLOTS * PERIOD
    row = lax.broadcasted_iota(jnp.int32, (height + 16 * SLOTS, PERIOD), 0)
    col = lax.broadcasted_iota(jnp.int32, (height + 16 * SLOTS, PERIOD), 1)
    pair = row // PERIOD
    value_col = (3 * (pair % 3) + (row % PERIOD) % 3) * SLOTS + pair // 3
    place_col = 9 * SLOTS + (row - height) // 16
    want = jnp.where(row < height, value_col, place_col)
    expand[...] = jnp.where(col == want, 1.0, 0.0).astype(BF16)

    for load in loads:
        load.wait()
    lane = lax.broadcasted_iota(jnp.int32, (SLOTS, atoms), 1)
    here = atom * (2 * atoms) + h * atoms + lane
    offset = near[...] - here
    total_atoms = 2 * atoms * groups
    offset = jnp.where(offset > HALO, offset - total_atoms, offset)
    offset = jnp.where(offset < -HALO, offset + total_atoms, offset)
    place = (offset + HALO + lane % TILE).astype(F32)
    for p in range(3):
        for a in range(3):
            for q in range(3):
                first = SLOTS * (3 * a + q)
                gathered[p, first : first + SLOTS, :] = raw[9 * a + 3 * p + q]
        gathered[p, 9 * SLOTS : 10 * SLOTS, :] = place
        gathered[p, 10 * SLOTS : PERIOD, :] = jnp.zeros((PERIOD - 10 * SLOTS, atoms), F32)
    stacked = []
    for t in range(tiles):
        lanes = slice(t * TILE, (t + 1) * TILE)
        stacked.append(
            jnp.concatenate([gathered[p, :, lanes].astype(BF16) for p in range(3)], axis=1)
        )
    stacked = jnp.concatenate(stacked, axis=0)
    mixed[...] = (
        jnp.dot(stacked, spread[...], preferred_element_type=F32)
        .astype(BF16)
        .reshape(tiles, PERIOD, WIDE)
    )

    atom_row = (lax.broadcasted_iota(jnp.int32, (PERIOD, TILE), 0) // 3).astype(F32).astype(BF16)
    atom_row = atom_row.reshape(3, 16, TILE)

    def build(t):
        pattern[...] = jnp.dot(expand[...], mixed[t], preferred_element_type=F32).astype(BF16)
        for lane_tile in range(3):
            lanes = slice(lane_tile * TILE, (lane_tile + 1) * TILE)
            down, above = band_groups(lane_tile)
            for g in range(2 * WIDE // PERIOD):
                slots = ([0, 1] if g in above else []) + ([2, 3] if g in down else [])
                span = slice(g * PERIOD, (g + 1) * PERIOD)
                if not slots:
                    for a in range(3):
                        weights[t, a, span, lanes] = jnp.zeros((PERIOD, TILE), BF16)
                    continue
                here = atom_row + jnp.asarray(16.0 * g, BF16)
                flags = {}
                for k in slots:
                    target = pattern[height + 16 * k : height + 16 * (k + 1), lanes]
                    flags[k] = here == target[None]
                for a in range(3):
                    total = None
                    for k in slots:
                        first = (3 * k + a) * PERIOD
                        value = pattern[first : first + PERIOD, lanes].reshape(3, 16, TILE)
                        term = jnp.where(flags[k], value, jnp.zeros_like(value))
                        total = term if total is None else total + term
                    weights[t, a, span, lanes] = total.reshape(PERIOD, TILE)

    def build_step(t, carry):
        build(t)
        return carry

    lax.fori_loop(0, tiles, build_step, 0)

    def transposed(source, target, u):
        span = pl.ds(pl.multiple_of(u * WIDE, WIDE), WIDE)
        target[:, span] = lax.dot_general(
            eye[...], source[span, :], (((1,), (1,)), ((), ())), preferred_element_type=F32
        ).astype(BF16)

    def apply_own(parity, t):
        window = own_t[parity, :, t * WIDE : (t + 2) * WIDE]
        for a in range(3):
            app_own[parity, a * modes : (a + 1) * modes, t * WIDE : (t + 1) * WIDE] = jnp.dot(
                window, weights[t, a], preferred_element_type=F32
            ).astype(BF16)

    def apply_up(relay, t):
        window = up_t[relay, :, t * WIDE : (t + 2) * WIDE]
        for a in range(3):
            app_up[relay, a * modes : (a + 1) * modes, t * WIDE : (t + 1) * WIDE] = jnp.dot(
                window, weights[t, a], preferred_element_type=F32
            ).astype(BF16)

    def schedule(arrived, moved, done):
        blocks = []
        for u in range(tiles + 1):
            need = {v for v in (u - 1, u) if 0 <= v < tiles}
            if u not in moved and need <= arrived:
                blocks.append(u)
                moved.add(u)
        ready = [v for v in range(tiles) if v not in done and {v, v + 1} <= moved]
        done.update(ready)
        return blocks, ready

    def forward(t):
        y_copy(t).wait_recv()

        @pl.when(has_up)
        def _():
            z_copy(1, 1, t).start()

        @pl.when(has_dn)
        def _():
            z_copy(0, 1, t).start()

    def await_chunks(relay, from_up, from_dn):
        @pl.when(has_up)
        def _():
            for t in from_up:
                z_copy(0, relay, t).wait_recv()

        @pl.when(has_dn)
        def _():
            for t in from_dn:
                z_copy(1, relay, t).wait_recv()

    forward(order[0])
    local_copy().wait()
    outer_edge().wait_recv()
    for u in range(tiles + 1):
        transposed(own.at[y], own_t.at[y], u)
    for v in range(tiles):
        apply_own(y, v)
        if v == 1:
            forward(order[1])
    await_chunks(0, order[:2], [])

    @pl.when(has_up)
    def _():
        side_copy(0, 0).start()
        side_copy(0, 1).start()

    await_chunks(0, order[2:3], [])
    transposed(up.at[0], up_t.at[0], 1)
    forward(order[2])
    await_chunks(0, order[3:4], [])
    transposed(up.at[0], up_t.at[0], 2)
    apply_up(0, 1)
    forward(order[3])
    await_chunks(0, order[4:], order)
    for u in range(3, tiles):
        transposed(up.at[0], up_t.at[0], u)
    for v in range(2, tiles - 1):
        apply_up(0, v)
    forward(order[4])
    for t in order[5:]:
        forward(t)
    y_edge().wait_recv()
    across_edge().wait_recv()
    for u in range(tiles + 1):
        transposed(own.at[other], own_t.at[other], u)
    for v in range(tiles):
        apply_own(other, v)

    bits = []
    bit = 1
    while bit < groups:
        side = (atom // bit) % 2
        bits.append((side, (mode, atom + bit * (1 - 2 * side))))
        bit *= 2
    mate_bit = (y, (mate, atom))

    class Halving:
        def __init__(self, buffer, landing, sems, stages):
            self.buffer, self.landing, self.sems, self.stages = buffer, landing, sems, stages
            self.base, self.size, self.at, self.stage = 0, buffer.shape[0], 0, 0
            self.copies = []

        def send(self):
            side, device = self.stages[self.stage]
            self.size //= 2
            self.keep = self.base + side * self.size
            copy = remote(
                self.buffer.at[pl.ds(self.base + (1 - side) * self.size, self.size)],
                self.landing.at[pl.ds(self.at, self.size)],
                self.sems,
                (self.stage,),
                device,
            )
            copy.start()
            self.copies.append(copy)

        def receive(self):
            self.copies[-1].wait_recv()
            for i in range(self.size):
                self.buffer[self.keep + i] = (
                    self.buffer[self.keep + i].astype(F32)
                    + self.landing[self.at + i].astype(F32)
                ).astype(BF16)
            self.at += self.size
            self.base = self.keep
            self.stage += 1

    def store(buffer, index, piece):
        count = buffer.shape[0]
        buffer[:, index] = piece.astype(BF16).reshape(count, modes // count, modes)

    early_sum = Halving(red_early, in_early, early_sem, bits)
    for c in range(2):
        product = jnp.dot(app_own[c], up[0, EDGE : EDGE + rows, :], preferred_element_type=F32)
        for a in range(3):
            store(red_early, 3 * c + a, product[a * modes : (a + 1) * modes])
    early_sum.send()
    for at, (c, b) in enumerate(SELF_PAIRS):
        product = jnp.dot(app_own[c], own[b, EDGE : EDGE + rows, :], preferred_element_type=F32)
        for a in range(3):
            store(red_self, 3 * at + a, product[a * modes : (a + 1) * modes])
    self_sum = Halving(red_self, in_self, self_sem, bits + [mate_bit])
    self_sum.send()

    @pl.when(has_up)
    def _():
        side_wait(0, 0).wait_recv()

    def add_next(t, start):
        span = slice(t * WIDE, (t + 1) * WIDE)
        for c in range(2):
            term = jnp.dot(
                app_own[c, :, span],
                up[1, EDGE + t * WIDE : EDGE + (t + 1) * WIDE, :],
                preferred_element_type=F32,
            )
            acc_next[c] = term if start else acc_next[c] + term

    def add_skip(t, start):
        span = slice(t * WIDE, (t + 1) * WIDE)
        term = jnp.dot(app_up[1, :, span], dn[1, span, :], preferred_element_type=F32)
        acc_skip[...] = term if start else acc_skip[...] + term
        term = jnp.dot(app_up[y, :, span], dn[other, span, :], preferred_element_type=F32)
        acc_mixed[...] = term if start else acc_mixed[...] + term

    direct_sum = Halving(red_direct, in_direct, direct_sem, bits)

    def hand_over(source, place, sems):
        copy = remote(
            source.buffer.at[source.base],
            from_mate.at[pl.ds(place, source.buffer.shape[1])],
            sems,
            (len(bits),),
            mate_bit[1],
        )
        copy.start()
        return copy

    def finish_direct():
        @pl.when(has_up)
        def _():
            side_wait(0, 1).wait_recv()

        for u in (0, tiles):
            transposed(up.at[0], up_t.at[0], u)
        for v in (0, tiles - 1):
            apply_up(0, v)
        product = jnp.dot(app_up[0], dn[0], preferred_element_type=F32)
        for a in range(3):
            store(red_direct, a, product[a * modes : (a + 1) * modes])

    moved, done, arrived = set(), set(), set()
    started = False
    handed = []
    for at, t in enumerate(order):
        await_chunks(1, [t], [t])
        arrived.add(t)
        if at == 1:

            @pl.when(has_up)
            def _():
                side_copy(1, 0).start()
                side_copy(1, 1).start()

        add_next(t, at == 0)
        if at == 0:
            self_sum.receive()
            self_sum.send()
            early_sum.receive()
            early_sum.send()
        if at == 1:
            self_sum.receive()
            self_sum.send()
        if at == 2:
            finish_direct()
            direct_sum.send()
            early_sum.receive()
            handed.append(hand_over(early_sum, 0, early_sem))

            @pl.when(has_up)
            def _():
                side_wait(1, 0).wait_recv()
                side_wait(1, 1).wait_recv()

        if at == 3:
            self_sum.receive()
            direct_sum.receive()
            direct_sum.send()
        if at == tiles - 1:
            for c in range(2):
                for a in range(3):
                    store(red_next, 3 * c + a, acc_next[c, a * modes : (a + 1) * modes, :])
            next_sum = Halving(red_next, in_next, next_sem, bits)
            next_sum.send()
            direct_sum.receive()
            handed.append(hand_over(direct_sum, 6, direct_sem))
        if at >= 2:
            blocks, ready = schedule(arrived, moved, done)
            for u in blocks:
                transposed(up.at[1], up_t.at[1], u)
            for v in ready:
                apply_up(1, v)
                add_skip(v, not started)
                started = True

    for a in range(3):
        rows_a = slice(a * modes, (a + 1) * modes)
        store(red_skip, a, acc_skip[rows_a, :])
        store(red_skip, 3 + a, acc_mixed[rows_a, :])
    skip_sum = Halving(red_skip, in_skip, skip_sem, bits[:-1])
    for _ in bits[:-1]:
        skip_sum.send()
        next_sum.receive()
        next_sum.send()
        skip_sum.receive()
    side, last = bits[-1]
    keep = skip_sum.base + side
    pass_on = skip_sum.base + 1 - side
    mine_rows = pl.ds(aligned(y * share), share)
    mate_rows = pl.ds(aligned(other * share), share)
    last_copies = [
        remote(
            red_skip.at[pass_on, pl.ds(0, 3)],
            in_skip.at[in_skip.shape[0] - 1, pl.ds(0, 3)],
            mixed_sem,
            (0,),
            last,
        ),
        remote(
            red_skip.at[pass_on, pl.ds(3, 3), mine_rows], in_mixed.at[0], mixed_sem, (1,), last
        ),
        remote(
            red_skip.at[keep, pl.ds(3, 3), mate_rows], in_mixed.at[1], mixed_sem, (2,), mate_bit[1]
        ),
        remote(
            red_skip.at[pass_on, pl.ds(3, 3), mate_rows],
            in_mixed.at[2],
            mixed_sem,
            (3,),
            (mate, last[1]),
        ),
    ]
    for copy in last_copies:
        copy.start()

    def frequency(block):
        index = jnp.clip(block, 0, blocks_all - 1)
        return freq_ref[pl.ds(index, 1), :]

    def account(values, first_row, count, c_index, b_index, valid, same=False):
        lane = lax.broadcasted_iota(jnp.int32, (count, modes), 1)
        spot = lane == lax.broadcasted_iota(jnp.int32, (count, modes), 0) + first_row
        squares = None
        for value in values:
            square = value * value
            squares = square if squares is None else squares + square
        c_row = frequency(2 * s - 2 + c_index)
        b_row = frequency(2 * s - 2 + b_index)
        c_col = jnp.sum(jnp.where(spot, c_row, 0.0), axis=1, keepdims=True)
        offset = b_row - c_col
        terms = squares * (half_width / math.pi / (offset * offset + half_width * half_width))
        if valid is not None:
            terms = jnp.where(valid, terms, 0.0)

        def folded(value):
            return jnp.sum(value.reshape(count // 8, 8, modes), axis=0)

        given[b_index] = given[b_index] + folded(terms)
        if not same:
            col_sum = jnp.sum(terms, axis=1, keepdims=True)
            given[c_index] = given[c_index] + folded(jnp.where(spot, col_sum, 0.0))

    for at, (c, b) in enumerate(SELF_PAIRS):
        values = [red_self[self_sum.base, 3 * at + a].astype(F32) for a in range(3)]
        account(values, self_sum.base * share, share, 2 + c, 2 + b, None, c == b)

    for copy in handed:
        copy.wait_recv()
    next_sum.receive()
    spot_row = next_sum.base * part
    for c in range(2):
        values = [
            red_next[next_sum.base, 3 * c + a].astype(F32) + from_mate[3 * c + a].astype(F32)
            for a in range(3)
        ]
        account(values, spot_row, part, 2 + c, 4 + other, has_up)

    both = jnp.logical_and(has_up, has_dn)
    for copy in last_copies:
        copy.wait_recv()
    values = [
        red_skip[keep, a].astype(F32)
        + in_skip[in_skip.shape[0] - 1, a].astype(F32)
        + from_mate[6 + a].astype(F32)
        for a in range(3)
    ]
    account(values, keep * part, part, 4 + other, other, both)
    values = []
    for a in range(3):
        value = red_skip[keep, 3 + a, mine_rows].astype(F32)
        for i in range(3):
            value = value + in_mixed[i, a].astype(F32)
        values.append(value)
    account(values, keep * part + y * share, share, 4, 1, both)

    rank = y * groups + atom

    def final_copy(delta, side, slab):
        slot = (1 - delta) * owners + rank
        return pltpu.make_async_remote_copy(
            src_ref=packed.at[2 * (delta + 1) + side, pl.ds(0, 1)],
            dst_ref=taken.at[slot, pl.ds(0, 1)],
            send_sem=fin_sem.at[0, (delta + 1) * owners + side * groups + slab],
            recv_sem=fin_sem.at[1, slot],
            device_id=(2 * (s + delta) + side, slab),
            device_id_type=MESH,
        )

    def final_wait(delta, side, slab):
        slot = (delta + 1) * owners + side * groups + slab
        return pltpu.make_async_remote_copy(
            src_ref=packed.at[0, pl.ds(0, 1)],
            dst_ref=taken.at[slot, pl.ds(0, 1)],
            send_sem=fin_sem.at[0, slot],
            recv_sem=fin_sem.at[1, slot],
            device_id=(2 * (s + delta) + side, slab),
            device_id_type=MESH,
        )

    def for_all(action):
        for delta, valid in ((0, None), (1, has_up), (-1, has_dn)):
            for side in range(2):
                for slab in range(groups):
                    if valid is None:
                        condition = jnp.logical_or(side != y, slab != atom)
                    else:
                        condition = valid
                    pl.when(condition)(functools.partial(action, delta, side, slab))

    packed[:, 0:1, :] = jnp.sum(given[...], axis=1, keepdims=True)
    for_all(lambda *at: final_copy(*at).start())
    taken[owners + rank, 0:1] = packed[2 + y, 0:1]
    for_all(lambda *at: final_wait(*at).wait_recv())
    total = jnp.sum(taken[:, 0:1, :], axis=0)
    own_freq = frequency(mode)
    out_ref[...] = total / (own_freq * own_freq)

    for_all(lambda *at: final_copy(*at).wait_send())
    for group in (self_sum, early_sum, direct_sum, next_sum, skip_sum):
        for copy in group.copies:
            copy.wait_send()
    for copy in last_copies + handed:
        copy.wait_send()
    y_edge().wait_send()
    outer_edge().wait_send()
    across_edge().wait_send()
    for t in range(tiles):
        y_copy(t).wait_send()

    @pl.when(has_up)
    def _():
        for relay in range(2):
            side_copy(relay, 0).wait_send()
            side_copy(relay, 1).wait_send()
            for t in range(tiles):
                z_copy(1, relay, t).wait_send()

    @pl.when(has_dn)
    def _():
        for relay in range(2):
            for t in range(tiles):
                z_copy(0, relay, t).wait_send()


def local(vectors, couplings, neighbours, frequency):
    rows_dev, modes = vectors.shape
    blocks_all = lax.axis_size("mode")
    groups = lax.axis_size("atom")
    half_width = WIDTH_MODES / (modes * blocks_all)
    rows = rows_dev // 2
    tiles = rows // WIDE
    padded = rows + 2 * EDGE
    owners = 2 * groups
    share = modes // owners
    part = modes // groups
    levels = groups.bit_length() - 1

    blocks = couplings.transpose(1, 2, 3, 0, 4).reshape(27, SLOTS, rows_dev // 3)
    sizes = (blocks_all, groups, rows_dev, modes, half_width)
    dma = pltpu.SemaphoreType.DMA
    result = pl.pallas_call(
        functools.partial(kernel, sizes),
        out_shape=jax.ShapeDtypeStruct((1, modes), F32),
        in_specs=[pl.BlockSpec(memory_space=pltpu.HBM)] * 4,
        out_specs=pl.BlockSpec(memory_space=pltpu.VMEM),
        scratch_shapes=[
            pltpu.VMEM((2, padded, modes), BF16),
            pltpu.VMEM((2, padded, modes), BF16),
            pltpu.VMEM((2, rows, modes), BF16),
            pltpu.VMEM((2, modes, padded), BF16),
            pltpu.VMEM((2, modes, padded), BF16),
            pltpu.VMEM((27, SLOTS, rows // 3), F32),
            pltpu.VMEM((SLOTS, rows // 3), jnp.int32),
            pltpu.VMEM((blocks_all, modes), F32),
            pltpu.VMEM((3, PERIOD, rows // 3), F32),
            pltpu.VMEM((tiles, 3, 2 * WIDE, WIDE), BF16),
            pltpu.VMEM((WIDE, WIDE), BF16),
            pltpu.VMEM((3 * SLOTS * PERIOD + 16 * SLOTS, PERIOD), BF16),
            pltpu.VMEM((TILE, TILE), BF16),
            pltpu.VMEM((tiles, PERIOD, WIDE), BF16),
            pltpu.VMEM((3 * SLOTS * PERIOD + 16 * SLOTS, WIDE), BF16),
            pltpu.VMEM((2, 3 * modes, rows), BF16),
            pltpu.VMEM((2, 3 * modes, rows), BF16),
            pltpu.VMEM((2, 3 * modes, modes), F32),
            pltpu.VMEM((3 * modes, modes), F32),
            pltpu.VMEM((3 * modes, modes), F32),
            pltpu.VMEM((owners, 9, share, modes), BF16),
            pltpu.VMEM((owners - 1, 9, share, modes), BF16),
            pltpu.VMEM((groups, 6, part, modes), BF16),
            pltpu.VMEM((groups - 1, 6, part, modes), BF16),
            pltpu.VMEM((groups, 3, part, modes), BF16),
            pltpu.VMEM((groups - 1, 3, part, modes), BF16),
            pltpu.VMEM((9, part, modes), BF16),
            pltpu.VMEM((groups, 6, part, modes), BF16),
            pltpu.VMEM((groups - 1, 6, part, modes), BF16),
            pltpu.VMEM((groups, 6, part, modes), BF16),
            pltpu.VMEM((groups - 1, 6, part, modes), BF16),
            pltpu.VMEM((3, 3, share, modes), BF16),
            pltpu.VMEM((6, 8, modes), F32),
            pltpu.VMEM((6, 8, modes), F32),
            pltpu.VMEM((3 * owners, 8, modes), F32),
            dma((4,)),
            dma((2, tiles)),
            dma((2, 2, 2, tiles)),
            dma((2, 3)),
            dma((2, 2, 2)),
            dma((2, levels + 1)),
            dma((2, levels + 1)),
            dma((2, levels + 1)),
            dma((2, levels)),
            dma((2, levels)),
            dma((2, 4)),
            dma((2, 3 * owners)),
        ],
        compiler_params=pltpu.CompilerParams(
            collective_id=0, has_side_effects=True, vmem_limit_bytes=56 * 1024 * 1024
        ),
        name="diffusivity",
    )(vectors, blocks, neighbours, frequency.reshape(blocks_all, modes))
    return result.reshape(modes) * (math.pi / 3.0)


def solution(mesh):
    return jax.shard_map(
        local,
        mesh=mesh,
        in_specs=(P("atom", "mode"), P(None, None, None, None, "atom"), P(None, "atom"), P()),
        out_specs=P("mode"),
        check_vma=False,
    )
```

```python
import functools
import math

import jax
import jax.numpy as jnp
from jax import lax
from jax.experimental import pallas as pl
from jax.experimental.pallas import tpu as pltpu
from jax.sharding import PartitionSpec as P

HALO = 64
PARTNERS = 4
WIDTH_MODES = 320
TILE = 128
WIDE = 3 * TILE
EDGE = 3 * HALO
PERIOD = 48
SLOTS = 4
MESH = pl.DeviceIdType.MESH
BF16 = jnp.bfloat16
F32 = jnp.float32

SELF_PAIRS = ((0, 0), (1, 0), (1, 1))


def aligned(value):
    return pl.multiple_of(value, 16)


def band_groups(lane_tile):
    first = (TILE * lane_tile) // 3
    last = (TILE * lane_tile + TILE - 1) // 3
    down = range((3 * first) // PERIOD, (3 * (last + HALO - 2) + 2) // PERIOD + 1)
    up = range((3 * (HALO + first + 2)) // PERIOD, (3 * (2 * HALO + last) + 2) // PERIOD + 1)
    return down, up


def kernel(
    sizes,
    vec,
    couplings,
    neighbours,
    frequencies,
    out_ref,
    own,
    up,
    dn,
    own_t,
    up_t,
    raw,
    near,
    freq_ref,
    gathered,
    weights,
    spread,
    expand,
    eye,
    mixed,
    pattern,
    app_own,
    app_up,
    acc_next,
    acc_skip,
    acc_mixed,
    red_self,
    in_self,
    red_early,
    in_early,
    red_direct,
    in_direct,
    from_mate,
    red_next,
    in_next,
    red_skip,
    in_skip,
    in_mixed,
    given,
    packed,
    taken,
    local_sem,
    y_sem,
    z_sem,
    edge_sem,
    side_sem,
    self_sem,
    early_sem,
    direct_sem,
    next_sem,
    skip_sem,
    mixed_sem,
    fin_sem,
):
    blocks_all, groups, rows_dev, modes, half_width = sizes
    rows = rows_dev // 2
    atoms = rows // 3
    tiles = rows // WIDE
    owners = 2 * groups
    share = modes // owners
    part = modes // groups

    mode = lax.axis_index("mode")
    atom = lax.axis_index("atom")
    s = mode // 2
    y = mode % 2
    other = 1 - y
    mate = mode + 1 - 2 * y
    h = (y + atom) % 2
    supers = blocks_all // 2
    has_up = s < supers - 1
    has_dn = s > 0
    outer = (atom + 2 * h - 1 + groups) % groups
    across = (atom + 1 - 2 * h + groups) % groups

    def remote(src, dst, sems, at, device):
        return pltpu.make_async_remote_copy(
            src_ref=src,
            dst_ref=dst,
            send_sem=sems.at[(0,) + at],
            recv_sem=sems.at[(1,) + at],
            device_id=device,
            device_id_type=MESH,
        )

    def local_copy():
        size = rows + EDGE
        return pltpu.make_async_copy(
            vec.at[pl.ds(aligned(h * (rows - EDGE)), size), :],
            own.at[y, pl.ds(aligned((1 - h) * EDGE), size), :],
            local_sem.at[0],
        )

    half_lanes = pl.ds(pl.multiple_of(h * atoms, TILE), atoms)
    loads = [
        pltpu.make_async_copy(couplings.at[:, :, half_lanes], raw, local_sem.at[1]),
        pltpu.make_async_copy(neighbours.at[:, half_lanes], near, local_sem.at[2]),
        pltpu.make_async_copy(frequencies, freq_ref, local_sem.at[3]),
    ]
    for load in loads:
        load.start()
    local_copy().start()

    barrier = pltpu.get_barrier_semaphore()

    def greet(device):
        pl.semaphore_signal(barrier, inc=1, device_id=device, device_id_type=MESH)

    pl.when(has_up)(lambda: greet((mode + 2, atom)))
    pl.when(has_dn)(lambda: greet((mode - 2, atom)))
    for step in range(groups):
        slab = (atom + step) % groups
        greet((mate, slab))
        if step:
            greet((mode, slab))
    sides = has_up.astype(jnp.int32) + has_dn.astype(jnp.int32)
    pl.semaphore_wait(barrier, owners - 1 + sides)

    def y_copy(t):
        return remote(
            vec.at[pl.ds(aligned((1 - h) * rows + t * WIDE), WIDE), :],
            own.at[y, pl.ds(aligned(EDGE + t * WIDE), WIDE), :],
            y_sem,
            (t,),
            (mate, atom),
        )

    def y_edge():
        return remote(
            vec.at[pl.ds(aligned(rows - EDGE + h * EDGE), EDGE), :],
            own.at[y, pl.ds(aligned(h * (rows + EDGE)), EDGE), :],
            edge_sem,
            (0,),
            (mate, atom),
        )

    def outer_edge():
        return remote(
            vec.at[pl.ds(aligned(h * (rows_dev - EDGE)), EDGE), :],
            own.at[y, pl.ds(aligned((1 - h) * (rows + EDGE)), EDGE), :],
            edge_sem,
            (1,),
            (mode, outer),
        )

    def across_edge():
        return remote(
            vec.at[pl.ds(aligned((1 - h) * (rows_dev - EDGE)), EDGE), :],
            own.at[y, pl.ds(aligned(h * (rows + EDGE)), EDGE), :],
            edge_sem,
            (2,),
            (mate, across),
        )

    def z_copy(upward, relay, t):
        if relay:
            src = own.at[other, pl.ds(aligned(EDGE + t * WIDE), WIDE), :]
        else:
            src = vec.at[pl.ds(aligned(h * rows + t * WIDE), WIDE), :]
        if upward:
            dst = dn.at[relay, pl.ds(aligned(t * WIDE), WIDE), :]
            return remote(src, dst, z_sem, (0, relay, t), (mode + 2, atom))
        dst = up.at[relay, pl.ds(aligned(EDGE + t * WIDE), WIDE), :]
        return remote(src, dst, z_sem, (1, relay, t), (mode - 2, atom))

    def side_copy(relay, inner):
        if inner:
            src = EDGE + (1 - h) * (rows - EDGE)
            dst = h * (rows + EDGE)
            device = (mate, atom)
            place = 1 - relay
        else:
            src = EDGE + h * (rows - EDGE)
            dst = (1 - h) * (rows + EDGE)
            device = (mode, outer)
            place = relay
        return pltpu.make_async_remote_copy(
            src_ref=up.at[relay, pl.ds(aligned(src), EDGE), :],
            dst_ref=up.at[place, pl.ds(aligned(dst), EDGE), :],
            send_sem=side_sem.at[0, relay, inner],
            recv_sem=side_sem.at[1, place, inner],
            device_id=device,
            device_id_type=MESH,
        )

    def side_wait(place, inner):
        return pltpu.make_async_remote_copy(
            src_ref=up.at[place, pl.ds(0, EDGE), :],
            dst_ref=up.at[place, pl.ds(0, EDGE), :],
            send_sem=side_sem.at[0, place, inner],
            recv_sem=side_sem.at[1, place, inner],
            device_id=(mate, atom),
            device_id_type=MESH,
        )

    order = [tiles - 1] + list(range(tiles - 1))
    for at, t in enumerate(order):
        y_copy(t).start()

        @pl.when(has_up)
        def _():
            z_copy(1, 0, t).start()

        @pl.when(has_dn)
        def _():
            z_copy(0, 0, t).start()

        if at == 1:
            y_edge().start()
            outer_edge().start()
            across_edge().start()

    @pl.when(jnp.logical_not(has_dn))
    def _():
        taken[0:owners] = jnp.zeros((owners, 8, modes), F32)

    @pl.when(jnp.logical_not(has_up))
    def _():
        taken[2 * owners : 3 * owners] = jnp.zeros((owners, 8, modes), F32)

    given[...] = jnp.zeros((6, 8, modes), F32)

    row = lax.broadcasted_iota(jnp.int32, (WIDE, WIDE), 0)
    col = lax.broadcasted_iota(jnp.int32, (WIDE, WIDE), 1)
    spread[...] = jnp.where(col == 3 * (row % TILE) + row // TILE, 1.0, 0.0).astype(BF16)
    row = lax.broadcasted_iota(jnp.int32, (TILE, TILE), 0)
    col = lax.broadcasted_iota(jnp.int32, (TILE, TILE), 1)
    eye[...] = jnp.where(row == col, 1.0, 0.0).astype(BF16)
    height = 3 * SLOTS * PERIOD
    row = lax.broadcasted_iota(jnp.int32, (height + 16 * SLOTS, PERIOD), 0)
    col = lax.broadcasted_iota(jnp.int32, (height + 16 * SLOTS, PERIOD), 1)
    pair = row // PERIOD
    value_col = (3 * (pair % 3) + (row % PERIOD) % 3) * SLOTS + pair // 3
    place_col = 9 * SLOTS + (row - height) // 16
    want = jnp.where(row < height, value_col, place_col)
    expand[...] = jnp.where(col == want, 1.0, 0.0).astype(BF16)

    for load in loads:
        load.wait()
    lane = lax.broadcasted_iota(jnp.int32, (SLOTS, atoms), 1)
    here = atom * (2 * atoms) + h * atoms + lane
    offset = near[...] - here
    total_atoms = 2 * atoms * groups
    offset = jnp.where(offset > HALO, offset - total_atoms, offset)
    offset = jnp.where(offset < -HALO, offset + total_atoms, offset)
    place = (offset + HALO + lane % TILE).astype(F32)
    for p in range(3):
        for a in range(3):
            for q in range(3):
                first = SLOTS * (3 * a + q)
                gathered[p, first : first + SLOTS, :] = raw[9 * a + 3 * p + q]
        gathered[p, 9 * SLOTS : 10 * SLOTS, :] = place
        gathered[p, 10 * SLOTS : PERIOD, :] = jnp.zeros((PERIOD - 10 * SLOTS, atoms), F32)
    stacked = []
    for t in range(tiles):
        lanes = slice(t * TILE, (t + 1) * TILE)
        stacked.append(
            jnp.concatenate([gathered[p, :, lanes].astype(BF16) for p in range(3)], axis=1)
        )
    stacked = jnp.concatenate(stacked, axis=0)
    mixed[...] = (
        jnp.dot(stacked, spread[...], preferred_element_type=F32)
        .astype(BF16)
        .reshape(tiles, PERIOD, WIDE)
    )

    atom_row = (lax.broadcasted_iota(jnp.int32, (PERIOD, TILE), 0) // 3).astype(F32).astype(BF16)
    atom_row = atom_row.reshape(3, 16, TILE)

    def build(t):
        pattern[...] = jnp.dot(expand[...], mixed[t], preferred_element_type=F32).astype(BF16)
        for lane_tile in range(3):
            lanes = slice(lane_tile * TILE, (lane_tile + 1) * TILE)
            down, above = band_groups(lane_tile)
            for g in range(2 * WIDE // PERIOD):
                slots = ([0, 1] if g in above else []) + ([2, 3] if g in down else [])
                span = slice(g * PERIOD, (g + 1) * PERIOD)
                if not slots:
                    for a in range(3):
                        weights[t, a, span, lanes] = jnp.zeros((PERIOD, TILE), BF16)
                    continue
                here = atom_row + jnp.asarray(16.0 * g, BF16)
                flags = {}
                for k in slots:
                    target = pattern[height + 16 * k : height + 16 * (k + 1), lanes]
                    flags[k] = here == target[None]
                for a in range(3):
                    total = None
                    for k in slots:
                        first = (3 * k + a) * PERIOD
                        value = pattern[first : first + PERIOD, lanes].reshape(3, 16, TILE)
                        term = jnp.where(flags[k], value, jnp.zeros_like(value))
                        total = term if total is None else total + term
                    weights[t, a, span, lanes] = total.reshape(PERIOD, TILE)

    def build_step(t, carry):
        build(t)
        return carry

    lax.fori_loop(0, tiles, build_step, 0)

    def transposed(source, target, u):
        span = pl.ds(pl.multiple_of(u * WIDE, WIDE), WIDE)
        target[:, span] = lax.dot_general(
            eye[...], source[span, :], (((1,), (1,)), ((), ())), preferred_element_type=F32
        ).astype(BF16)

    def apply_own(parity, t):
        window = own_t[parity, :, t * WIDE : (t + 2) * WIDE]
        for a in range(3):
            app_own[parity, a * modes : (a + 1) * modes, t * WIDE : (t + 1) * WIDE] = jnp.dot(
                window, weights[t, a], preferred_element_type=F32
            ).astype(BF16)

    def apply_up(relay, t):
        window = up_t[relay, :, t * WIDE : (t + 2) * WIDE]
        for a in range(3):
            app_up[relay, a * modes : (a + 1) * modes, t * WIDE : (t + 1) * WIDE] = jnp.dot(
                window, weights[t, a], preferred_element_type=F32
            ).astype(BF16)

    def schedule(arrived, moved, done):
        blocks = []
        for u in range(tiles + 1):
            need = {v for v in (u - 1, u) if 0 <= v < tiles}
            if u not in moved and need <= arrived:
                blocks.append(u)
                moved.add(u)
        ready = [v for v in range(tiles) if v not in done and {v, v + 1} <= moved]
        done.update(ready)
        return blocks, ready

    def forward(t):
        y_copy(t).wait_recv()

        @pl.when(has_up)
        def _():
            z_copy(1, 1, t).start()

        @pl.when(has_dn)
        def _():
            z_copy(0, 1, t).start()

    def await_chunks(relay, from_up, from_dn):
        @pl.when(has_up)
        def _():
            for t in from_up:
                z_copy(0, relay, t).wait_recv()

        @pl.when(has_dn)
        def _():
            for t in from_dn:
                z_copy(1, relay, t).wait_recv()

    forward(order[0])
    local_copy().wait()
    outer_edge().wait_recv()
    for u in range(tiles + 1):
        transposed(own.at[y], own_t.at[y], u)
    for v in range(tiles):
        apply_own(y, v)
        if v == 1:
            forward(order[1])
    await_chunks(0, order[:2], [])

    @pl.when(has_up)
    def _():
        side_copy(0, 0).start()
        side_copy(0, 1).start()

    moved, done, arrived = set(), set(), set(order[:2])

    def own_step():
        blocks, ready = schedule(arrived, moved, done)
        for u in blocks:
            transposed(own.at[other], own_t.at[other], u)
        for v in ready:
            apply_own(other, v)

    await_chunks(0, order[2:3], [])
    transposed(up.at[0], up_t.at[0], 1)
    forward(order[2])
    arrived.add(order[2])
    y_edge().wait_recv()
    across_edge().wait_recv()
    own_step()
    await_chunks(0, order[3:4], [])
    transposed(up.at[0], up_t.at[0], 2)
    apply_up(0, 1)
    forward(order[3])
    arrived.add(order[3])
    own_step()
    await_chunks(0, order[4:], order)
    for u in range(3, tiles):
        transposed(up.at[0], up_t.at[0], u)
    for v in range(2, tiles - 1):
        apply_up(0, v)

    def store(buffer, index, piece):
        count = buffer.shape[0]
        buffer[:, index] = piece.astype(BF16).reshape(count, modes // count, modes)

    def early(c):
        product = jnp.dot(app_own[c], up[0, EDGE : EDGE + rows, :], preferred_element_type=F32)
        for a in range(3):
            store(red_early, 3 * c + a, product[a * modes : (a + 1) * modes])

    early(y)
    for t in order[4:]:
        forward(t)
        arrived.add(t)
        own_step()
    early(other)

    bits = []
    bit = 1
    while bit < groups:
        side = (atom // bit) % 2
        bits.append((side, (mode, atom + bit * (1 - 2 * side))))
        bit *= 2
    mate_bit = (y, (mate, atom))

    def owner_of(slab):
        place = 0
        bit = 1
        while bit < groups:
            place = 2 * place + (slab // bit) % 2
            bit *= 2
        return place

    mine = owner_of(atom)

    class Halving:
        def __init__(self, buffer, landing, sems, stages):
            self.buffer, self.landing, self.sems, self.stages = buffer, landing, sems, stages
            self.base, self.size, self.at, self.stage = 0, buffer.shape[0], 0, 0
            self.copies = []

        def send(self):
            side, device = self.stages[self.stage]
            self.size //= 2
            self.keep = self.base + side * self.size
            copy = remote(
                self.buffer.at[pl.ds(self.base + (1 - side) * self.size, self.size)],
                self.landing.at[pl.ds(self.at, self.size)],
                self.sems,
                (self.stage,),
                device,
            )
            copy.start()
            self.copies.append(copy)

        def receive(self):
            self.copies[-1].wait_recv()
            for i in range(self.size):
                self.buffer[self.keep + i] = (
                    self.buffer[self.keep + i].astype(F32)
                    + self.landing[self.at + i].astype(F32)
                ).astype(BF16)
            self.at += self.size
            self.base = self.keep
            self.stage += 1

    early_sum = Halving(red_early, in_early, early_sem, bits)
    early_sum.send()
    own_main = jnp.concatenate([own[j, EDGE : EDGE + rows, :] for j in range(2)], axis=1)
    for c in range(2):
        blocks = own_main if c else own[0, EDGE : EDGE + rows, :]
        product = jnp.dot(app_own[c], blocks, preferred_element_type=F32)
        for at, (first, b) in enumerate(SELF_PAIRS):
            if first == c:
                for a in range(3):
                    piece = product[a * modes : (a + 1) * modes, b * modes : (b + 1) * modes]
                    store(red_self, 3 * at + a, piece)
    self_sum = Halving(red_self, in_self, self_sem, bits + [mate_bit])
    self_sum.send()

    @pl.when(has_up)
    def _():
        side_wait(0, 0).wait_recv()

    def add_next(t, start):
        span = slice(t * WIDE, (t + 1) * WIDE)
        for c in range(2):
            term = jnp.dot(
                app_own[c, :, span],
                up[1, EDGE + t * WIDE : EDGE + (t + 1) * WIDE, :],
                preferred_element_type=F32,
            )
            acc_next[c] = term if start else acc_next[c] + term

    def add_skip(t, start):
        span = slice(t * WIDE, (t + 1) * WIDE)
        term = jnp.dot(app_up[1, :, span], dn[1, span, :], preferred_element_type=F32)
        acc_skip[...] = term if start else acc_skip[...] + term
        term = jnp.dot(app_up[y, :, span], dn[other, span, :], preferred_element_type=F32)
        acc_mixed[...] = term if start else acc_mixed[...] + term

    direct_sum = Halving(red_direct, in_direct, direct_sem, bits)

    def hand_over(source, place, sems):
        copy = remote(
            source.buffer.at[source.base],
            from_mate.at[pl.ds(place, source.buffer.shape[1])],
            sems,
            (len(bits),),
            mate_bit[1],
        )
        copy.start()
        return copy

    def finish_direct():
        @pl.when(has_up)
        def _():
            side_wait(0, 1).wait_recv()

        for u in (0, tiles):
            transposed(up.at[0], up_t.at[0], u)
        for v in (0, tiles - 1):
            apply_up(0, v)
        product = jnp.dot(app_up[0], dn[0], preferred_element_type=F32)
        for a in range(3):
            store(red_direct, a, product[a * modes : (a + 1) * modes])

    moved, done, arrived = set(), set(), set()
    started = False
    handed = []
    next_copies = []
    skip_copies = []

    def direct_copy(source, landing, sems, step):
        target = (atom + step) % groups
        return remote(
            source.at[owner_of(target)], landing.at[step - 1], sems, (step - 1,), (mode, target)
        )

    for at, t in enumerate(order):
        await_chunks(1, [t], [t])
        arrived.add(t)
        if at == 1:

            @pl.when(has_up)
            def _():
                side_copy(1, 0).start()
                side_copy(1, 1).start()

        add_next(t, at == 0)
        if at == 0:
            self_sum.receive()
            self_sum.send()
            early_sum.receive()
            early_sum.send()
        if at == 1:
            self_sum.receive()
            self_sum.send()
        if at == 2:
            finish_direct()
            direct_sum.send()
            early_sum.receive()
            handed.append(hand_over(early_sum, 0, early_sem))

            @pl.when(has_up)
            def _():
                side_wait(1, 0).wait_recv()
                side_wait(1, 1).wait_recv()

        if at == 3:
            self_sum.receive()
            direct_sum.receive()
            direct_sum.send()
        if at == tiles - 1:
            for c in range(2):
                for a in range(3):
                    store(red_next, 3 * c + a, acc_next[c, a * modes : (a + 1) * modes, :])
            for step in range(1, groups):
                next_copies.append(direct_copy(red_next, in_next, next_sem, step))
                next_copies[-1].start()
            direct_sum.receive()
            handed.append(hand_over(direct_sum, 6, direct_sem))
        if at >= 2:
            blocks, ready = schedule(arrived, moved, done)
            for u in blocks:
                transposed(up.at[1], up_t.at[1], u)
            for v in ready:
                apply_up(1, v)
                add_skip(v, not started)
                started = True

    for a in range(3):
        rows_a = slice(a * modes, (a + 1) * modes)
        store(red_skip, a, acc_skip[rows_a, :])
        store(red_skip, 3 + a, acc_mixed[rows_a, :])
    keep = mine
    mine_rows = pl.ds(aligned(y * share), share)
    mate_rows = pl.ds(aligned(other * share), share)
    for step in list(range(1, groups)) + [0]:
        target = (atom + step) % groups
        if step:
            skip_copies.append(
                remote(
                    red_skip.at[owner_of(target), pl.ds(0, 3)],
                    in_skip.at[step - 1],
                    skip_sem,
                    (step - 1,),
                    (mode, target),
                )
            )
            skip_copies.append(
                remote(
                    red_skip.at[owner_of(target), pl.ds(3, 3), mine_rows],
                    in_mixed.at[step - 1],
                    mixed_sem,
                    (step - 1,),
                    (mode, target),
                )
            )
        skip_copies.append(
            remote(
                red_skip.at[owner_of(target), pl.ds(3, 3), mate_rows],
                in_mixed.at[groups - 1 + step],
                mixed_sem,
                (groups - 1 + step,),
                (mate, target),
            )
        )
    for copy in skip_copies:
        copy.start()

    def frequency(block):
        index = jnp.clip(block, 0, blocks_all - 1)
        return freq_ref[pl.ds(index, 1), :]

    def account(values, first_row, count, c_index, b_index, valid, same=False):
        lane = lax.broadcasted_iota(jnp.int32, (count, modes), 1)
        spot = lane == lax.broadcasted_iota(jnp.int32, (count, modes), 0) + first_row
        squares = None
        for value in values:
            square = value * value
            squares = square if squares is None else squares + square
        c_row = frequency(2 * s - 2 + c_index)
        b_row = frequency(2 * s - 2 + b_index)
        c_col = jnp.sum(jnp.where(spot, c_row, 0.0), axis=1, keepdims=True)
        offset = b_row - c_col
        terms = squares * (half_width / math.pi / (offset * offset + half_width * half_width))
        if valid is not None:
            terms = jnp.where(valid, terms, 0.0)

        def folded(value):
            return jnp.sum(value.reshape(count // 8, 8, modes), axis=0)

        given[b_index] = given[b_index] + folded(terms)
        if not same:
            col_sum = jnp.sum(terms, axis=1, keepdims=True)
            given[c_index] = given[c_index] + folded(jnp.where(spot, col_sum, 0.0))

    for at, (c, b) in enumerate(SELF_PAIRS):
        values = [red_self[self_sum.base, 3 * at + a].astype(F32) for a in range(3)]
        account(values, self_sum.base * share, share, 2 + c, 2 + b, None, c == b)

    for copy in handed:
        copy.wait_recv()
    for copy in next_copies:
        copy.wait_recv()
    for c in range(2):
        values = []
        for a in range(3):
            row = 3 * c + a
            value = red_next[keep, row].astype(F32) + from_mate[row].astype(F32)
            for step in range(1, groups):
                value = value + in_next[step - 1, row].astype(F32)
            values.append(value)
        account(values, mine * part, part, 2 + c, 4 + other, has_up)

    both = jnp.logical_and(has_up, has_dn)
    for copy in skip_copies:
        copy.wait_recv()
    values = []
    for a in range(3):
        value = red_skip[keep, a].astype(F32) + from_mate[6 + a].astype(F32)
        for step in range(1, groups):
            value = value + in_skip[step - 1, a].astype(F32)
        values.append(value)
    account(values, mine * part, part, 4 + other, other, both)
    values = []
    for a in range(3):
        value = red_skip[keep, 3 + a, mine_rows].astype(F32)
        for i in range(owners - 1):
            value = value + in_mixed[i, a].astype(F32)
        values.append(value)
    account(values, mine * part + y * share, share, 4, 1, both)

    rank = y * groups + atom

    def final_copy(delta, side, slab):
        slot = (1 - delta) * owners + rank
        return pltpu.make_async_remote_copy(
            src_ref=packed.at[2 * (delta + 1) + side, pl.ds(0, 1)],
            dst_ref=taken.at[slot, pl.ds(0, 1)],
            send_sem=fin_sem.at[0, (delta + 1) * owners + side * groups + slab],
            recv_sem=fin_sem.at[1, slot],
            device_id=(2 * (s + delta) + side, slab),
            device_id_type=MESH,
        )

    def final_wait(delta, side, slab):
        slot = (delta + 1) * owners + side * groups + slab
        return pltpu.make_async_remote_copy(
            src_ref=packed.at[0, pl.ds(0, 1)],
            dst_ref=taken.at[slot, pl.ds(0, 1)],
            send_sem=fin_sem.at[0, slot],
            recv_sem=fin_sem.at[1, slot],
            device_id=(2 * (s + delta) + side, slab),
            device_id_type=MESH,
        )

    def for_all(action):
        for delta, valid in ((0, None), (1, has_up), (-1, has_dn)):
            for side in range(2):
                for slab in range(groups):
                    if valid is None:
                        condition = jnp.logical_or(side != y, slab != atom)
                    else:
                        condition = valid
                    pl.when(condition)(functools.partial(action, delta, side, slab))

    packed[:, 0:1, :] = jnp.sum(given[...], axis=1, keepdims=True)
    for_all(lambda *at: final_copy(*at).start())
    taken[owners + rank, 0:1] = packed[2 + y, 0:1]
    for_all(lambda *at: final_wait(*at).wait_recv())
    total = jnp.sum(taken[:, 0:1, :], axis=0)
    own_freq = frequency(mode)
    out_ref[...] = total / (own_freq * own_freq)

    for_all(lambda *at: final_copy(*at).wait_send())
    for group in (self_sum, early_sum, direct_sum):
        for copy in group.copies:
            copy.wait_send()
    for copy in next_copies + skip_copies + handed:
        copy.wait_send()
    y_edge().wait_send()
    outer_edge().wait_send()
    across_edge().wait_send()
    for t in range(tiles):
        y_copy(t).wait_send()

    @pl.when(has_up)
    def _():
        for relay in range(2):
            side_copy(relay, 0).wait_send()
            side_copy(relay, 1).wait_send()
            for t in range(tiles):
                z_copy(1, relay, t).wait_send()

    @pl.when(has_dn)
    def _():
        for relay in range(2):
            for t in range(tiles):
                z_copy(0, relay, t).wait_send()


def local(vectors, couplings, neighbours, frequency):
    rows_dev, modes = vectors.shape
    blocks_all = lax.axis_size("mode")
    groups = lax.axis_size("atom")
    half_width = WIDTH_MODES / (modes * blocks_all)
    rows = rows_dev // 2
    tiles = rows // WIDE
    padded = rows + 2 * EDGE
    owners = 2 * groups
    share = modes // owners
    part = modes // groups
    levels = groups.bit_length() - 1

    blocks = couplings.transpose(1, 2, 3, 0, 4).reshape(27, SLOTS, rows_dev // 3)
    sizes = (blocks_all, groups, rows_dev, modes, half_width)
    dma = pltpu.SemaphoreType.DMA
    result = pl.pallas_call(
        functools.partial(kernel, sizes),
        out_shape=jax.ShapeDtypeStruct((1, modes), F32),
        in_specs=[pl.BlockSpec(memory_space=pltpu.HBM)] * 4,
        out_specs=pl.BlockSpec(memory_space=pltpu.VMEM),
        scratch_shapes=[
            pltpu.VMEM((2, padded, modes), BF16),
            pltpu.VMEM((2, padded, modes), BF16),
            pltpu.VMEM((2, rows, modes), BF16),
            pltpu.VMEM((2, modes, padded), BF16),
            pltpu.VMEM((2, modes, padded), BF16),
            pltpu.VMEM((27, SLOTS, rows // 3), F32),
            pltpu.VMEM((SLOTS, rows // 3), jnp.int32),
            pltpu.VMEM((blocks_all, modes), F32),
            pltpu.VMEM((3, PERIOD, rows // 3), F32),
            pltpu.VMEM((tiles, 3, 2 * WIDE, WIDE), BF16),
            pltpu.VMEM((WIDE, WIDE), BF16),
            pltpu.VMEM((3 * SLOTS * PERIOD + 16 * SLOTS, PERIOD), BF16),
            pltpu.VMEM((TILE, TILE), BF16),
            pltpu.VMEM((tiles, PERIOD, WIDE), BF16),
            pltpu.VMEM((3 * SLOTS * PERIOD + 16 * SLOTS, WIDE), BF16),
            pltpu.VMEM((2, 3 * modes, rows), BF16),
            pltpu.VMEM((2, 3 * modes, rows), BF16),
            pltpu.VMEM((2, 3 * modes, modes), F32),
            pltpu.VMEM((3 * modes, modes), F32),
            pltpu.VMEM((3 * modes, modes), F32),
            pltpu.VMEM((owners, 9, share, modes), BF16),
            pltpu.VMEM((owners - 1, 9, share, modes), BF16),
            pltpu.VMEM((groups, 6, part, modes), BF16),
            pltpu.VMEM((groups - 1, 6, part, modes), BF16),
            pltpu.VMEM((groups, 3, part, modes), BF16),
            pltpu.VMEM((groups - 1, 3, part, modes), BF16),
            pltpu.VMEM((9, part, modes), BF16),
            pltpu.VMEM((groups, 6, part, modes), BF16),
            pltpu.VMEM((groups - 1, 6, part, modes), BF16),
            pltpu.VMEM((groups, 6, part, modes), BF16),
            pltpu.VMEM((groups - 1, 3, part, modes), BF16),
            pltpu.VMEM((owners - 1, 3, share, modes), BF16),
            pltpu.VMEM((6, 8, modes), F32),
            pltpu.VMEM((6, 8, modes), F32),
            pltpu.VMEM((3 * owners, 8, modes), F32),
            dma((4,)),
            dma((2, tiles)),
            dma((2, 2, 2, tiles)),
            dma((2, 3)),
            dma((2, 2, 2)),
            dma((2, levels + 1)),
            dma((2, levels + 1)),
            dma((2, levels + 1)),
            dma((2, groups - 1)),
            dma((2, groups - 1)),
            dma((2, owners - 1)),
            dma((2, 3 * owners)),
        ],
        compiler_params=pltpu.CompilerParams(
            collective_id=0, has_side_effects=True, vmem_limit_bytes=56 * 1024 * 1024
        ),
        name="diffusivity",
    )(vectors, blocks, neighbours, frequency.reshape(blocks_all, modes))
    return result.reshape(modes) * (math.pi / 3.0)


def solution(mesh):
    return jax.shard_map(
        local,
        mesh=mesh,
        in_specs=(P("atom", "mode"), P(None, None, None, None, "atom"), P(None, "atom"), P()),
        out_specs=P("mode"),
        check_vma=False,
    )
```

```python
import functools
import math

import jax
import jax.numpy as jnp
from jax import lax
from jax.experimental import pallas as pl
from jax.experimental.pallas import tpu as pltpu
from jax.sharding import PartitionSpec as P

HALO = 64
PARTNERS = 4
WIDTH_MODES = 320
TILE = 128
WIDE = 3 * TILE
EDGE = 3 * HALO
PERIOD = 48
SLOTS = 4
MESH = pl.DeviceIdType.MESH
BF16 = jnp.bfloat16
F32 = jnp.float32

SELF_PAIRS = ((0, 0), (1, 0), (1, 1))


def aligned(value):
    return pl.multiple_of(value, 16)


def band_groups(lane_tile):
    first = (TILE * lane_tile) // 3
    last = (TILE * lane_tile + TILE - 1) // 3
    down = range((3 * first) // PERIOD, (3 * (last + HALO - 2) + 2) // PERIOD + 1)
    up = range((3 * (HALO + first + 2)) // PERIOD, (3 * (2 * HALO + last) + 2) // PERIOD + 1)
    return down, up


def kernel(
    sizes,
    vec,
    couplings,
    neighbours,
    frequencies,
    out_ref,
    own,
    up,
    dn,
    own_t,
    up_t,
    raw,
    near,
    freq_ref,
    gathered,
    weights,
    spread,
    expand,
    eye,
    mixed,
    pattern,
    app_own,
    app_up,
    acc_next,
    acc_skip,
    acc_mixed,
    red_self,
    in_self,
    self_mate,
    red_early,
    in_early,
    red_direct,
    in_direct,
    from_mate,
    red_next,
    in_next,
    red_skip,
    in_skip,
    in_mixed,
    given,
    packed,
    taken,
    local_sem,
    y_sem,
    z_sem,
    edge_sem,
    side_sem,
    self_sem,
    early_sem,
    direct_sem,
    next_sem,
    skip_sem,
    mixed_sem,
    fin_sem,
):
    blocks_all, groups, rows_dev, modes, half_width = sizes
    rows = rows_dev // 2
    atoms = rows // 3
    tiles = rows // WIDE
    owners = 2 * groups
    share = modes // owners
    part = modes // groups

    mode = lax.axis_index("mode")
    atom = lax.axis_index("atom")
    s = mode // 2
    y = mode % 2
    other = 1 - y
    mate = mode + 1 - 2 * y
    h = (y + atom) % 2
    supers = blocks_all // 2
    has_up = s < supers - 1
    has_dn = s > 0
    outer = (atom + 2 * h - 1 + groups) % groups
    across = (atom + 1 - 2 * h + groups) % groups

    def remote(src, dst, sems, at, device):
        return pltpu.make_async_remote_copy(
            src_ref=src,
            dst_ref=dst,
            send_sem=sems.at[(0,) + at],
            recv_sem=sems.at[(1,) + at],
            device_id=device,
            device_id_type=MESH,
        )

    def local_copy():
        size = rows + EDGE
        return pltpu.make_async_copy(
            vec.at[pl.ds(aligned(h * (rows - EDGE)), size), :],
            own.at[y, pl.ds(aligned((1 - h) * EDGE), size), :],
            local_sem.at[0],
        )

    half_lanes = pl.ds(pl.multiple_of(h * atoms, TILE), atoms)
    loads = [
        pltpu.make_async_copy(couplings.at[:, :, half_lanes], raw, local_sem.at[1]),
        pltpu.make_async_copy(neighbours.at[:, half_lanes], near, local_sem.at[2]),
        pltpu.make_async_copy(frequencies, freq_ref, local_sem.at[3]),
    ]
    for load in loads:
        load.start()
    local_copy().start()

    barrier = pltpu.get_barrier_semaphore()

    def greet(device):
        pl.semaphore_signal(barrier, inc=1, device_id=device, device_id_type=MESH)

    pl.when(has_up)(lambda: greet((mode + 2, atom)))
    pl.when(has_dn)(lambda: greet((mode - 2, atom)))
    for step in range(groups):
        slab = (atom + step) % groups
        greet((mate, slab))
        if step:
            greet((mode, slab))
    sides = has_up.astype(jnp.int32) + has_dn.astype(jnp.int32)
    pl.semaphore_wait(barrier, owners - 1 + sides)

    def y_copy(t):
        return remote(
            vec.at[pl.ds(aligned((1 - h) * rows + t * WIDE), WIDE), :],
            own.at[y, pl.ds(aligned(EDGE + t * WIDE), WIDE), :],
            y_sem,
            (t,),
            (mate, atom),
        )

    def y_edge():
        return remote(
            vec.at[pl.ds(aligned(rows - EDGE + h * EDGE), EDGE), :],
            own.at[y, pl.ds(aligned(h * (rows + EDGE)), EDGE), :],
            edge_sem,
            (0,),
            (mate, atom),
        )

    def outer_edge():
        return remote(
            vec.at[pl.ds(aligned(h * (rows_dev - EDGE)), EDGE), :],
            own.at[y, pl.ds(aligned((1 - h) * (rows + EDGE)), EDGE), :],
            edge_sem,
            (1,),
            (mode, outer),
        )

    def across_edge():
        return remote(
            vec.at[pl.ds(aligned((1 - h) * (rows_dev - EDGE)), EDGE), :],
            own.at[y, pl.ds(aligned(h * (rows + EDGE)), EDGE), :],
            edge_sem,
            (2,),
            (mate, across),
        )

    def z_copy(upward, relay, t):
        if relay:
            src = own.at[other, pl.ds(aligned(EDGE + t * WIDE), WIDE), :]
        else:
            src = vec.at[pl.ds(aligned(h * rows + t * WIDE), WIDE), :]
        if upward:
            dst = dn.at[relay, pl.ds(aligned(t * WIDE), WIDE), :]
            return remote(src, dst, z_sem, (0, relay, t), (mode + 2, atom))
        dst = up.at[relay, pl.ds(aligned(EDGE + t * WIDE), WIDE), :]
        return remote(src, dst, z_sem, (1, relay, t), (mode - 2, atom))

    def side_copy(relay, inner):
        if inner:
            src = EDGE + (1 - h) * (rows - EDGE)
            dst = h * (rows + EDGE)
            device = (mate, atom)
            place = 1 - relay
        else:
            src = EDGE + h * (rows - EDGE)
            dst = (1 - h) * (rows + EDGE)
            device = (mode, outer)
            place = relay
        return pltpu.make_async_remote_copy(
            src_ref=up.at[relay, pl.ds(aligned(src), EDGE), :],
            dst_ref=up.at[place, pl.ds(aligned(dst), EDGE), :],
            send_sem=side_sem.at[0, relay, inner],
            recv_sem=side_sem.at[1, place, inner],
            device_id=device,
            device_id_type=MESH,
        )

    def side_wait(place, inner):
        return pltpu.make_async_remote_copy(
            src_ref=up.at[place, pl.ds(0, EDGE), :],
            dst_ref=up.at[place, pl.ds(0, EDGE), :],
            send_sem=side_sem.at[0, place, inner],
            recv_sem=side_sem.at[1, place, inner],
            device_id=(mate, atom),
            device_id_type=MESH,
        )

    order = [tiles - 1] + list(range(tiles - 1))
    for at, t in enumerate(order):
        y_copy(t).start()

        @pl.when(has_up)
        def _():
            z_copy(1, 0, t).start()

        @pl.when(has_dn)
        def _():
            z_copy(0, 0, t).start()

        if at == 1:
            y_edge().start()
            outer_edge().start()
            across_edge().start()

    @pl.when(jnp.logical_not(has_dn))
    def _():
        taken[0:owners] = jnp.zeros((owners, 8, modes), F32)

    @pl.when(jnp.logical_not(has_up))
    def _():
        taken[2 * owners : 3 * owners] = jnp.zeros((owners, 8, modes), F32)

    given[...] = jnp.zeros((6, 8, modes), F32)

    row = lax.broadcasted_iota(jnp.int32, (WIDE, WIDE), 0)
    col = lax.broadcasted_iota(jnp.int32, (WIDE, WIDE), 1)
    spread[...] = jnp.where(col == 3 * (row % TILE) + row // TILE, 1.0, 0.0).astype(BF16)
    row = lax.broadcasted_iota(jnp.int32, (TILE, TILE), 0)
    col = lax.broadcasted_iota(jnp.int32, (TILE, TILE), 1)
    eye[...] = jnp.where(row == col, 1.0, 0.0).astype(BF16)
    height = 3 * SLOTS * PERIOD
    row = lax.broadcasted_iota(jnp.int32, (height + 16 * SLOTS, PERIOD), 0)
    col = lax.broadcasted_iota(jnp.int32, (height + 16 * SLOTS, PERIOD), 1)
    pair = row // PERIOD
    value_col = (3 * (pair % 3) + (row % PERIOD) % 3) * SLOTS + pair // 3
    place_col = 9 * SLOTS + (row - height) // 16
    want = jnp.where(row < height, value_col, place_col)
    expand[...] = jnp.where(col == want, 1.0, 0.0).astype(BF16)

    for load in loads:
        load.wait()
    lane = lax.broadcasted_iota(jnp.int32, (SLOTS, atoms), 1)
    here = atom * (2 * atoms) + h * atoms + lane
    offset = near[...] - here
    total_atoms = 2 * atoms * groups
    offset = jnp.where(offset > HALO, offset - total_atoms, offset)
    offset = jnp.where(offset < -HALO, offset + total_atoms, offset)
    place = (offset + HALO + lane % TILE).astype(F32)
    for p in range(3):
        for a in range(3):
            for q in range(3):
                first = SLOTS * (3 * a + q)
                gathered[p, first : first + SLOTS, :] = raw[9 * a + 3 * p + q]
        gathered[p, 9 * SLOTS : 10 * SLOTS, :] = place
        gathered[p, 10 * SLOTS : PERIOD, :] = jnp.zeros((PERIOD - 10 * SLOTS, atoms), F32)
    stacked = []
    for t in range(tiles):
        lanes = slice(t * TILE, (t + 1) * TILE)
        stacked.append(
            jnp.concatenate([gathered[p, :, lanes].astype(BF16) for p in range(3)], axis=1)
        )
    stacked = jnp.concatenate(stacked, axis=0)
    mixed[...] = (
        jnp.dot(stacked, spread[...], preferred_element_type=F32)
        .astype(BF16)
        .reshape(tiles, PERIOD, WIDE)
    )

    atom_row = (lax.broadcasted_iota(jnp.int32, (PERIOD, TILE), 0) // 3).astype(F32).astype(BF16)
    atom_row = atom_row.reshape(3, 16, TILE)

    def build(t):
        pattern[...] = jnp.dot(expand[...], mixed[t], preferred_element_type=F32).astype(BF16)
        for lane_tile in range(3):
            lanes = slice(lane_tile * TILE, (lane_tile + 1) * TILE)
            down, above = band_groups(lane_tile)
            for g in range(2 * WIDE // PERIOD):
                slots = ([0, 1] if g in above else []) + ([2, 3] if g in down else [])
                span = slice(g * PERIOD, (g + 1) * PERIOD)
                if not slots:
                    for a in range(3):
                        weights[t, a, span, lanes] = jnp.zeros((PERIOD, TILE), BF16)
                    continue
                here = atom_row + jnp.asarray(16.0 * g, BF16)
                flags = {}
                for k in slots:
                    target = pattern[height + 16 * k : height + 16 * (k + 1), lanes]
                    flags[k] = here == target[None]
                for a in range(3):
                    total = None
                    for k in slots:
                        first = (3 * k + a) * PERIOD
                        value = pattern[first : first + PERIOD, lanes].reshape(3, 16, TILE)
                        term = jnp.where(flags[k], value, jnp.zeros_like(value))
                        total = term if total is None else total + term
                    weights[t, a, span, lanes] = total.reshape(PERIOD, TILE)

    def build_step(t, carry):
        build(t)
        return carry

    lax.fori_loop(0, tiles, build_step, 0)

    def transposed(source, target, u):
        span = pl.ds(pl.multiple_of(u * WIDE, WIDE), WIDE)
        target[:, span] = lax.dot_general(
            eye[...], source[span, :], (((1,), (1,)), ((), ())), preferred_element_type=F32
        ).astype(BF16)

    def apply_own(parity, t):
        window = own_t[parity, :, t * WIDE : (t + 2) * WIDE]
        for a in range(3):
            app_own[parity, a * modes : (a + 1) * modes, t * WIDE : (t + 1) * WIDE] = jnp.dot(
                window, weights[t, a], preferred_element_type=F32
            ).astype(BF16)

    def apply_up(relay, t):
        window = up_t[relay, :, t * WIDE : (t + 2) * WIDE]
        for a in range(3):
            app_up[relay, a * modes : (a + 1) * modes, t * WIDE : (t + 1) * WIDE] = jnp.dot(
                window, weights[t, a], preferred_element_type=F32
            ).astype(BF16)

    def schedule(arrived, moved, done):
        blocks = []
        for u in range(tiles + 1):
            need = {v for v in (u - 1, u) if 0 <= v < tiles}
            if u not in moved and need <= arrived:
                blocks.append(u)
                moved.add(u)
        ready = [v for v in range(tiles) if v not in done and {v, v + 1} <= moved]
        done.update(ready)
        return blocks, ready

    def forward(t):
        y_copy(t).wait_recv()

        @pl.when(has_up)
        def _():
            z_copy(1, 1, t).start()

        @pl.when(has_dn)
        def _():
            z_copy(0, 1, t).start()

    def await_chunks(relay, from_up, from_dn):
        @pl.when(has_up)
        def _():
            for t in from_up:
                z_copy(0, relay, t).wait_recv()

        @pl.when(has_dn)
        def _():
            for t in from_dn:
                z_copy(1, relay, t).wait_recv()

    forward(order[0])
    local_copy().wait()
    outer_edge().wait_recv()
    for u in range(tiles + 1):
        transposed(own.at[y], own_t.at[y], u)
    for v in range(tiles):
        apply_own(y, v)
        if v == 1:
            forward(order[1])
    await_chunks(0, order[:2], [])

    @pl.when(has_up)
    def _():
        side_copy(0, 0).start()
        side_copy(0, 1).start()

    moved, done, arrived = set(), set(), set(order[:2])

    def own_step():
        blocks, ready = schedule(arrived, moved, done)
        for u in blocks:
            transposed(own.at[other], own_t.at[other], u)
        for v in ready:
            apply_own(other, v)

    await_chunks(0, order[2:3], [])
    transposed(up.at[0], up_t.at[0], 1)
    forward(order[2])
    arrived.add(order[2])
    y_edge().wait_recv()
    across_edge().wait_recv()
    own_step()
    await_chunks(0, order[3:4], [])
    transposed(up.at[0], up_t.at[0], 2)
    apply_up(0, 1)
    forward(order[3])
    arrived.add(order[3])
    own_step()
    await_chunks(0, order[4:], order)
    for u in range(3, tiles):
        transposed(up.at[0], up_t.at[0], u)
    for v in range(2, tiles - 1):
        apply_up(0, v)

    def store(buffer, index, piece):
        count = buffer.shape[0]
        buffer[:, index] = piece.astype(BF16).reshape(count, modes // count, modes)

    def early(c):
        product = jnp.dot(app_own[c], up[0, EDGE : EDGE + rows, :], preferred_element_type=F32)
        for a in range(3):
            store(red_early, 3 * c + a, product[a * modes : (a + 1) * modes])

    early(y)
    for t in order[4:]:
        forward(t)
        arrived.add(t)
        own_step()
    early(other)

    def owner_of(slab):
        place = 0
        bit = 1
        while bit < groups:
            place = 2 * place + (slab // bit) % 2
            bit *= 2
        return place

    mine = owner_of(atom)
    mine_rows = pl.ds(aligned(y * share), share)
    mate_rows = pl.ds(aligned(other * share), share)

    class Scatter:
        def __init__(self, buffer, landing, sems):
            self.buffer, self.landing, self.sems = buffer, landing, sems
            self.copies = []

        def send(self):
            for step in range(1, groups):
                target = (atom + step) % groups
                copy = remote(
                    self.buffer.at[owner_of(target)],
                    self.landing.at[step - 1],
                    self.sems,
                    (step - 1,),
                    (mode, target),
                )
                copy.start()
                self.copies.append(copy)

        def value(self, row):
            total = self.buffer[mine, row].astype(F32)
            for step in range(1, groups):
                total = total + self.landing[step - 1, row].astype(F32)
            return total

        def await_all(self):
            for copy in self.copies[: groups - 1]:
                copy.wait_recv()

        def hand_over(self, target, rows_sent):
            self.await_all()
            for row in range(self.buffer.shape[1]):
                self.buffer[mine, row] = self.value(row).astype(BF16)
            source = self.buffer.at[mine]
            if rows_sent is not None:
                source = source.at[:, rows_sent]
            copy = remote(source, target, self.sems, (groups - 1,), (mate, atom))
            copy.start()
            self.copies.append(copy)

    early_sum = Scatter(red_early, in_early, early_sem)
    early_sum.send()
    own_main = jnp.concatenate([own[j, EDGE : EDGE + rows, :] for j in range(2)], axis=1)
    for c in range(2):
        blocks = own_main if c else own[0, EDGE : EDGE + rows, :]
        product = jnp.dot(app_own[c], blocks, preferred_element_type=F32)
        for at, (first, b) in enumerate(SELF_PAIRS):
            if first == c:
                for a in range(3):
                    piece = product[a * modes : (a + 1) * modes, b * modes : (b + 1) * modes]
                    store(red_self, 3 * at + a, piece)
    self_sum = Scatter(red_self, in_self, self_sem)
    self_sum.send()

    @pl.when(has_up)
    def _():
        side_wait(0, 0).wait_recv()

    def add_next(t, start):
        span = slice(t * WIDE, (t + 1) * WIDE)
        for c in range(2):
            term = jnp.dot(
                app_own[c, :, span],
                up[1, EDGE + t * WIDE : EDGE + (t + 1) * WIDE, :],
                preferred_element_type=F32,
            )
            acc_next[c] = term if start else acc_next[c] + term

    def add_skip(first, last, start):
        span = slice(first * WIDE, (last + 1) * WIDE)
        term = jnp.dot(app_up[1, :, span], dn[1, span, :], preferred_element_type=F32)
        acc_skip[...] = term if start else acc_skip[...] + term
        term = jnp.dot(app_up[y, :, span], dn[other, span, :], preferred_element_type=F32)
        acc_mixed[...] = term if start else acc_mixed[...] + term

    direct_sum = Scatter(red_direct, in_direct, direct_sem)
    next_sum = Scatter(red_next, in_next, next_sem)

    def finish_direct():
        @pl.when(has_up)
        def _():
            side_wait(0, 1).wait_recv()

        for u in (0, tiles):
            transposed(up.at[0], up_t.at[0], u)
        for v in (0, tiles - 1):
            apply_up(0, v)
        product = jnp.dot(app_up[0], dn[0], preferred_element_type=F32)
        for a in range(3):
            store(red_direct, a, product[a * modes : (a + 1) * modes])

    moved, done, arrived = set(), set(), set()
    started = False
    skip_copies = []
    for at, t in enumerate(order):
        await_chunks(1, [t], [t])
        arrived.add(t)
        if at == 1:

            @pl.when(has_up)
            def _():
                side_copy(1, 0).start()
                side_copy(1, 1).start()

        add_next(t, at == 0)
        if at == 1:
            early_sum.hand_over(from_mate.at[pl.ds(0, 6)], None)
        if at == 2:
            finish_direct()
            direct_sum.send()

            @pl.when(has_up)
            def _():
                side_wait(1, 0).wait_recv()
                side_wait(1, 1).wait_recv()

        if at == 3:
            self_sum.hand_over(self_mate, mate_rows)
        if at == tiles - 1:
            for c in range(2):
                for a in range(3):
                    store(red_next, 3 * c + a, acc_next[c, a * modes : (a + 1) * modes, :])
            next_sum.send()
            direct_sum.hand_over(from_mate.at[pl.ds(6, 3)], None)
        if at >= 2:
            blocks, ready = schedule(arrived, moved, done)
            for u in blocks:
                transposed(up.at[1], up_t.at[1], u)
            for v in ready:
                apply_up(1, v)
            runs = [v for v in ready if v - 1 not in ready]
            for v in runs:
                last = v
                while last + 1 in ready:
                    last += 1
                add_skip(v, last, not started)
                started = True

    for a in range(3):
        rows_a = slice(a * modes, (a + 1) * modes)
        store(red_skip, a, acc_skip[rows_a, :])
        store(red_skip, 3 + a, acc_mixed[rows_a, :])
    for step in list(range(1, groups)) + [0]:
        target = (atom + step) % groups
        if step:
            skip_copies.append(
                remote(
                    red_skip.at[owner_of(target), pl.ds(0, 3)],
                    in_skip.at[step - 1],
                    skip_sem,
                    (step - 1,),
                    (mode, target),
                )
            )
            skip_copies.append(
                remote(
                    red_skip.at[owner_of(target), pl.ds(3, 3), mine_rows],
                    in_mixed.at[step - 1],
                    mixed_sem,
                    (step - 1,),
                    (mode, target),
                )
            )
        skip_copies.append(
            remote(
                red_skip.at[owner_of(target), pl.ds(3, 3), mate_rows],
                in_mixed.at[groups - 1 + step],
                mixed_sem,
                (groups - 1 + step,),
                (mate, target),
            )
        )
    for copy in skip_copies:
        copy.start()

    def frequency(block):
        index = jnp.clip(block, 0, blocks_all - 1)
        return freq_ref[pl.ds(index, 1), :]

    def account(values, first_row, count, c_index, b_index, valid, same=False):
        lane = lax.broadcasted_iota(jnp.int32, (count, modes), 1)
        spot = lane == lax.broadcasted_iota(jnp.int32, (count, modes), 0) + first_row
        squares = None
        for value in values:
            square = value * value
            squares = square if squares is None else squares + square
        c_row = frequency(2 * s - 2 + c_index)
        b_row = frequency(2 * s - 2 + b_index)
        c_col = jnp.sum(jnp.where(spot, c_row, 0.0), axis=1, keepdims=True)
        offset = b_row - c_col
        terms = squares * (half_width / math.pi / (offset * offset + half_width * half_width))
        if valid is not None:
            terms = jnp.where(valid, terms, 0.0)

        def folded(value):
            return jnp.sum(value.reshape(count // 8, 8, modes), axis=0)

        given[b_index] = given[b_index] + folded(terms)
        if not same:
            col_sum = jnp.sum(terms, axis=1, keepdims=True)
            given[c_index] = given[c_index] + folded(jnp.where(spot, col_sum, 0.0))

    self_sum.copies[-1].wait_recv()
    for at, (c, b) in enumerate(SELF_PAIRS):
        values = [
            red_self[mine, 3 * at + a, mine_rows].astype(F32) + self_mate[3 * at + a].astype(F32)
            for a in range(3)
        ]
        account(values, mine * part + y * share, share, 2 + c, 2 + b, None, c == b)

    early_sum.copies[-1].wait_recv()
    direct_sum.copies[-1].wait_recv()
    next_sum.await_all()
    for c in range(2):
        values = [
            next_sum.value(3 * c + a) + from_mate[3 * c + a].astype(F32) for a in range(3)
        ]
        account(values, mine * part, part, 2 + c, 4 + other, has_up)

    both = jnp.logical_and(has_up, has_dn)
    for copy in skip_copies:
        copy.wait_recv()
    values = []
    for a in range(3):
        value = red_skip[mine, a].astype(F32) + from_mate[6 + a].astype(F32)
        for step in range(1, groups):
            value = value + in_skip[step - 1, a].astype(F32)
        values.append(value)
    account(values, mine * part, part, 4 + other, other, both)
    values = []
    for a in range(3):
        value = red_skip[mine, 3 + a, mine_rows].astype(F32)
        for i in range(owners - 1):
            value = value + in_mixed[i, a].astype(F32)
        values.append(value)
    account(values, mine * part + y * share, share, 4, 1, both)

    rank = y * groups + atom

    def final_copy(delta, side, slab):
        slot = (1 - delta) * owners + rank
        return pltpu.make_async_remote_copy(
            src_ref=packed.at[2 * (delta + 1) + side, pl.ds(0, 1)],
            dst_ref=taken.at[slot, pl.ds(0, 1)],
            send_sem=fin_sem.at[0, (delta + 1) * owners + side * groups + slab],
            recv_sem=fin_sem.at[1, slot],
            device_id=(2 * (s + delta) + side, slab),
            device_id_type=MESH,
        )

    def final_wait(delta, side, slab):
        slot = (delta + 1) * owners + side * groups + slab
        return pltpu.make_async_remote_copy(
            src_ref=packed.at[0, pl.ds(0, 1)],
            dst_ref=taken.at[slot, pl.ds(0, 1)],
            send_sem=fin_sem.at[0, slot],
            recv_sem=fin_sem.at[1, slot],
            device_id=(2 * (s + delta) + side, slab),
            device_id_type=MESH,
        )

    def for_all(action):
        for delta, valid in ((0, None), (1, has_up), (-1, has_dn)):
            for side in range(2):
                for slab in range(groups):
                    if valid is None:
                        condition = jnp.logical_or(side != y, slab != atom)
                    else:
                        condition = valid
                    pl.when(condition)(functools.partial(action, delta, side, slab))

    packed[:, 0:1, :] = jnp.sum(given[...], axis=1, keepdims=True)
    for_all(lambda *at: final_copy(*at).start())
    taken[owners + rank, 0:1] = packed[2 + y, 0:1]
    for_all(lambda *at: final_wait(*at).wait_recv())
    total = jnp.sum(taken[:, 0:1, :], axis=0)
    own_freq = frequency(mode)
    out_ref[...] = total / (own_freq * own_freq)

    for_all(lambda *at: final_copy(*at).wait_send())
    for group in (self_sum, early_sum, direct_sum, next_sum):
        for copy in group.copies:
            copy.wait_send()
    for copy in skip_copies:
        copy.wait_send()
    y_edge().wait_send()
    outer_edge().wait_send()
    across_edge().wait_send()
    for t in range(tiles):
        y_copy(t).wait_send()

    @pl.when(has_up)
    def _():
        for relay in range(2):
            side_copy(relay, 0).wait_send()
            side_copy(relay, 1).wait_send()
            for t in range(tiles):
                z_copy(1, relay, t).wait_send()

    @pl.when(has_dn)
    def _():
        for relay in range(2):
            for t in range(tiles):
                z_copy(0, relay, t).wait_send()


def local(vectors, couplings, neighbours, frequency):
    rows_dev, modes = vectors.shape
    blocks_all = lax.axis_size("mode")
    groups = lax.axis_size("atom")
    half_width = WIDTH_MODES / (modes * blocks_all)
    rows = rows_dev // 2
    tiles = rows // WIDE
    padded = rows + 2 * EDGE
    owners = 2 * groups
    share = modes // owners
    part = modes // groups

    blocks = couplings.transpose(1, 2, 3, 0, 4).reshape(27, SLOTS, rows_dev // 3)
    sizes = (blocks_all, groups, rows_dev, modes, half_width)
    dma = pltpu.SemaphoreType.DMA
    result = pl.pallas_call(
        functools.partial(kernel, sizes),
        out_shape=jax.ShapeDtypeStruct((1, modes), F32),
        in_specs=[pl.BlockSpec(memory_space=pltpu.HBM)] * 4,
        out_specs=pl.BlockSpec(memory_space=pltpu.VMEM),
        scratch_shapes=[
            pltpu.VMEM((2, padded, modes), BF16),
            pltpu.VMEM((2, padded, modes), BF16),
            pltpu.VMEM((2, rows, modes), BF16),
            pltpu.VMEM((2, modes, padded), BF16),
            pltpu.VMEM((2, modes, padded), BF16),
            pltpu.VMEM((27, SLOTS, rows // 3), F32),
            pltpu.VMEM((SLOTS, rows // 3), jnp.int32),
            pltpu.VMEM((blocks_all, modes), F32),
            pltpu.VMEM((3, PERIOD, rows // 3), F32),
            pltpu.VMEM((tiles, 3, 2 * WIDE, WIDE), BF16),
            pltpu.VMEM((WIDE, WIDE), BF16),
            pltpu.VMEM((3 * SLOTS * PERIOD + 16 * SLOTS, PERIOD), BF16),
            pltpu.VMEM((TILE, TILE), BF16),
            pltpu.VMEM((tiles, PERIOD, WIDE), BF16),
            pltpu.VMEM((3 * SLOTS * PERIOD + 16 * SLOTS, WIDE), BF16),
            pltpu.VMEM((2, 3 * modes, rows), BF16),
            pltpu.VMEM((2, 3 * modes, rows), BF16),
            pltpu.VMEM((2, 3 * modes, modes), F32),
            pltpu.VMEM((3 * modes, modes), F32),
            pltpu.VMEM((3 * modes, modes), F32),
            pltpu.VMEM((groups, 9, part, modes), BF16),
            pltpu.VMEM((groups - 1, 9, part, modes), BF16),
            pltpu.VMEM((9, share, modes), BF16),
            pltpu.VMEM((groups, 6, part, modes), BF16),
            pltpu.VMEM((groups - 1, 6, part, modes), BF16),
            pltpu.VMEM((groups, 3, part, modes), BF16),
            pltpu.VMEM((groups - 1, 3, part, modes), BF16),
            pltpu.VMEM((9, part, modes), BF16),
            pltpu.VMEM((groups, 6, part, modes), BF16),
            pltpu.VMEM((groups - 1, 6, part, modes), BF16),
            pltpu.VMEM((groups, 6, part, modes), BF16),
            pltpu.VMEM((groups - 1, 3, part, modes), BF16),
            pltpu.VMEM((owners - 1, 3, share, modes), BF16),
            pltpu.VMEM((6, 8, modes), F32),
            pltpu.VMEM((6, 8, modes), F32),
            pltpu.VMEM((3 * owners, 8, modes), F32),
            dma((4,)),
            dma((2, tiles)),
            dma((2, 2, 2, tiles)),
            dma((2, 3)),
            dma((2, 2, 2)),
            dma((2, groups)),
            dma((2, groups)),
            dma((2, groups)),
            dma((2, groups - 1)),
            dma((2, groups - 1)),
            dma((2, owners - 1)),
            dma((2, 3 * owners)),
        ],
        compiler_params=pltpu.CompilerParams(
            collective_id=0, has_side_effects=True, vmem_limit_bytes=56 * 1024 * 1024
        ),
        name="diffusivity",
    )(vectors, blocks, neighbours, frequency.reshape(blocks_all, modes))
    return result.reshape(modes) * (math.pi / 3.0)


def solution(mesh):
    return jax.shard_map(
        local,
        mesh=mesh,
        in_specs=(P("atom", "mode"), P(None, None, None, None, "atom"), P(None, "atom"), P()),
        out_specs=P("mode"),
        check_vma=False,
    )
```

```python
import functools
import math

import jax
import jax.numpy as jnp
from jax import lax
from jax.experimental import pallas as pl
from jax.experimental.pallas import tpu as pltpu
from jax.sharding import PartitionSpec as P

HALO = 64
PARTNERS = 4
WIDTH_MODES = 320
TILE = 128
WIDE = 3 * TILE
EDGE = 3 * HALO
PERIOD = 48
SLOTS = 4
MESH = pl.DeviceIdType.MESH
BF16 = jnp.bfloat16
F32 = jnp.float32

SELF_PAIRS = ((0, 0), (1, 0), (1, 1))


def aligned(value):
    return pl.multiple_of(value, 16)


def band_groups(lane_tile):
    first = (TILE * lane_tile) // 3
    last = (TILE * lane_tile + TILE - 1) // 3
    down = range((3 * first) // PERIOD, (3 * (last + HALO - 2) + 2) // PERIOD + 1)
    up = range((3 * (HALO + first + 2)) // PERIOD, (3 * (2 * HALO + last) + 2) // PERIOD + 1)
    return down, up


def kernel(
    sizes,
    vec,
    couplings,
    neighbours,
    frequencies,
    out_ref,
    own,
    up,
    dn,
    own_t,
    up_t,
    raw,
    near,
    freq_ref,
    gathered,
    weights,
    spread,
    expand,
    eye,
    mixed,
    pattern,
    app_own,
    app_up,
    acc_next,
    acc_skip,
    acc_mixed,
    red_self,
    in_self,
    self_mate,
    red_early,
    in_early,
    red_direct,
    in_direct,
    from_mate,
    red_next,
    in_next,
    red_skip,
    in_skip,
    in_mixed,
    given,
    packed,
    taken,
    local_sem,
    y_sem,
    z_sem,
    edge_sem,
    side_sem,
    self_sem,
    early_sem,
    direct_sem,
    next_sem,
    skip_sem,
    mixed_sem,
    fin_sem,
):
    blocks_all, groups, rows_dev, modes, half_width = sizes
    rows = rows_dev // 2
    atoms = rows // 3
    tiles = rows // WIDE
    owners = 2 * groups
    share = modes // owners
    part = modes // groups

    mode = lax.axis_index("mode")
    atom = lax.axis_index("atom")
    s = mode // 2
    y = mode % 2
    other = 1 - y
    mate = mode + 1 - 2 * y
    h = (y + atom) % 2
    supers = blocks_all // 2
    has_up = s < supers - 1
    has_dn = s > 0
    outer = (atom + 2 * h - 1 + groups) % groups
    across = (atom + 1 - 2 * h + groups) % groups

    def remote(src, dst, sems, at, device):
        return pltpu.make_async_remote_copy(
            src_ref=src,
            dst_ref=dst,
            send_sem=sems.at[(0,) + at],
            recv_sem=sems.at[(1,) + at],
            device_id=device,
            device_id_type=MESH,
        )

    def local_copy():
        size = rows + EDGE
        return pltpu.make_async_copy(
            vec.at[pl.ds(aligned(h * (rows - EDGE)), size), :],
            own.at[y, pl.ds(aligned((1 - h) * EDGE), size), :],
            local_sem.at[0],
        )

    half_lanes = pl.ds(pl.multiple_of(h * atoms, TILE), atoms)
    loads = [
        pltpu.make_async_copy(couplings.at[:, :, half_lanes], raw, local_sem.at[1]),
        pltpu.make_async_copy(neighbours.at[:, half_lanes], near, local_sem.at[2]),
        pltpu.make_async_copy(frequencies, freq_ref, local_sem.at[3]),
    ]
    for load in loads:
        load.start()
    local_copy().start()

    barrier = pltpu.get_barrier_semaphore()

    def greet(device):
        pl.semaphore_signal(barrier, inc=1, device_id=device, device_id_type=MESH)

    pl.when(has_up)(lambda: greet((mode + 2, atom)))
    pl.when(has_dn)(lambda: greet((mode - 2, atom)))
    for step in range(groups):
        slab = (atom + step) % groups
        greet((mate, slab))
        if step:
            greet((mode, slab))
    sides = has_up.astype(jnp.int32) + has_dn.astype(jnp.int32)
    pl.semaphore_wait(barrier, owners - 1 + sides)

    def y_copy(t):
        return remote(
            vec.at[pl.ds(aligned((1 - h) * rows + t * WIDE), WIDE), :],
            own.at[y, pl.ds(aligned(EDGE + t * WIDE), WIDE), :],
            y_sem,
            (t,),
            (mate, atom),
        )

    def y_edge():
        return remote(
            vec.at[pl.ds(aligned(rows - EDGE + h * EDGE), EDGE), :],
            own.at[y, pl.ds(aligned(h * (rows + EDGE)), EDGE), :],
            edge_sem,
            (0,),
            (mate, atom),
        )

    def outer_edge():
        return remote(
            vec.at[pl.ds(aligned(h * (rows_dev - EDGE)), EDGE), :],
            own.at[y, pl.ds(aligned((1 - h) * (rows + EDGE)), EDGE), :],
            edge_sem,
            (1,),
            (mode, outer),
        )

    def across_edge():
        return remote(
            vec.at[pl.ds(aligned((1 - h) * (rows_dev - EDGE)), EDGE), :],
            own.at[y, pl.ds(aligned(h * (rows + EDGE)), EDGE), :],
            edge_sem,
            (2,),
            (mate, across),
        )

    def z_copy(upward, relay, t):
        if relay:
            src = own.at[other, pl.ds(aligned(EDGE + t * WIDE), WIDE), :]
        else:
            src = vec.at[pl.ds(aligned(h * rows + t * WIDE), WIDE), :]
        if upward:
            dst = dn.at[relay, pl.ds(aligned(t * WIDE), WIDE), :]
            return remote(src, dst, z_sem, (0, relay, t), (mode + 2, atom))
        dst = up.at[relay, pl.ds(aligned(EDGE + t * WIDE), WIDE), :]
        return remote(src, dst, z_sem, (1, relay, t), (mode - 2, atom))

    def side_copy(relay, inner):
        if inner:
            src = EDGE + (1 - h) * (rows - EDGE)
            dst = h * (rows + EDGE)
            device = (mate, atom)
            place = 1 - relay
        else:
            src = EDGE + h * (rows - EDGE)
            dst = (1 - h) * (rows + EDGE)
            device = (mode, outer)
            place = relay
        return pltpu.make_async_remote_copy(
            src_ref=up.at[relay, pl.ds(aligned(src), EDGE), :],
            dst_ref=up.at[place, pl.ds(aligned(dst), EDGE), :],
            send_sem=side_sem.at[0, relay, inner],
            recv_sem=side_sem.at[1, place, inner],
            device_id=device,
            device_id_type=MESH,
        )

    def side_wait(place, inner):
        return pltpu.make_async_remote_copy(
            src_ref=up.at[place, pl.ds(0, EDGE), :],
            dst_ref=up.at[place, pl.ds(0, EDGE), :],
            send_sem=side_sem.at[0, place, inner],
            recv_sem=side_sem.at[1, place, inner],
            device_id=(mate, atom),
            device_id_type=MESH,
        )

    order = [tiles - 1] + list(range(tiles - 1))
    for at, t in enumerate(order):
        y_copy(t).start()

        @pl.when(has_up)
        def _():
            z_copy(1, 0, t).start()

        @pl.when(has_dn)
        def _():
            z_copy(0, 0, t).start()

        if at == 1:
            y_edge().start()
            outer_edge().start()
            across_edge().start()

    @pl.when(jnp.logical_not(has_dn))
    def _():
        taken[0:owners] = jnp.zeros((owners, 8, modes), F32)

    @pl.when(jnp.logical_not(has_up))
    def _():
        taken[2 * owners : 3 * owners] = jnp.zeros((owners, 8, modes), F32)

    given[...] = jnp.zeros((6, 8, modes), F32)

    row = lax.broadcasted_iota(jnp.int32, (WIDE, WIDE), 0)
    col = lax.broadcasted_iota(jnp.int32, (WIDE, WIDE), 1)
    spread[...] = jnp.where(col == 3 * (row % TILE) + row // TILE, 1.0, 0.0).astype(BF16)
    row = lax.broadcasted_iota(jnp.int32, (TILE, TILE), 0)
    col = lax.broadcasted_iota(jnp.int32, (TILE, TILE), 1)
    eye[...] = jnp.where(row == col, 1.0, 0.0).astype(BF16)
    height = 3 * SLOTS * PERIOD
    row = lax.broadcasted_iota(jnp.int32, (height + 16 * SLOTS, PERIOD), 0)
    col = lax.broadcasted_iota(jnp.int32, (height + 16 * SLOTS, PERIOD), 1)
    pair = row // PERIOD
    value_col = (3 * (pair % 3) + (row % PERIOD) % 3) * SLOTS + pair // 3
    place_col = 9 * SLOTS + (row - height) // 16
    want = jnp.where(row < height, value_col, place_col)
    expand[...] = jnp.where(col == want, 1.0, 0.0).astype(BF16)

    for load in loads:
        load.wait()
    lane = lax.broadcasted_iota(jnp.int32, (SLOTS, atoms), 1)
    here = atom * (2 * atoms) + h * atoms + lane
    offset = near[...] - here
    total_atoms = 2 * atoms * groups
    offset = jnp.where(offset > HALO, offset - total_atoms, offset)
    offset = jnp.where(offset < -HALO, offset + total_atoms, offset)
    place = (offset + HALO + lane % TILE).astype(F32)
    for p in range(3):
        for a in range(3):
            for q in range(3):
                first = SLOTS * (3 * a + q)
                gathered[p, first : first + SLOTS, :] = raw[9 * a + 3 * p + q]
        gathered[p, 9 * SLOTS : 10 * SLOTS, :] = place
        gathered[p, 10 * SLOTS : PERIOD, :] = jnp.zeros((PERIOD - 10 * SLOTS, atoms), F32)
    stacked = []
    for t in range(tiles):
        lanes = slice(t * TILE, (t + 1) * TILE)
        stacked.append(
            jnp.concatenate([gathered[p, :, lanes].astype(BF16) for p in range(3)], axis=1)
        )
    stacked = jnp.concatenate(stacked, axis=0)
    mixed[...] = (
        jnp.dot(stacked, spread[...], preferred_element_type=F32)
        .astype(BF16)
        .reshape(tiles, PERIOD, WIDE)
    )

    atom_row = (lax.broadcasted_iota(jnp.int32, (PERIOD, TILE), 0) // 3).astype(F32).astype(BF16)
    atom_row = atom_row.reshape(3, 16, TILE)

    def build(t):
        pattern[...] = jnp.dot(expand[...], mixed[t], preferred_element_type=F32).astype(BF16)
        for lane_tile in range(3):
            lanes = slice(lane_tile * TILE, (lane_tile + 1) * TILE)
            down, above = band_groups(lane_tile)
            for g in range(2 * WIDE // PERIOD):
                slots = ([0, 1] if g in above else []) + ([2, 3] if g in down else [])
                span = slice(g * PERIOD, (g + 1) * PERIOD)
                if not slots:
                    for a in range(3):
                        weights[t, a, span, lanes] = jnp.zeros((PERIOD, TILE), BF16)
                    continue
                here = atom_row + jnp.asarray(16.0 * g, BF16)
                flags = {}
                for k in slots:
                    target = pattern[height + 16 * k : height + 16 * (k + 1), lanes]
                    flags[k] = here == target[None]
                for a in range(3):
                    total = None
                    for k in slots:
                        first = (3 * k + a) * PERIOD
                        value = pattern[first : first + PERIOD, lanes].reshape(3, 16, TILE)
                        term = jnp.where(flags[k], value, jnp.zeros_like(value))
                        total = term if total is None else total + term
                    weights[t, a, span, lanes] = total.reshape(PERIOD, TILE)

    def build_step(t, carry):
        build(t)
        return carry

    lax.fori_loop(0, tiles, build_step, 0)

    def transposed(source, target, u):
        span = pl.ds(pl.multiple_of(u * WIDE, WIDE), WIDE)
        target[:, span] = lax.dot_general(
            eye[...], source[span, :], (((1,), (1,)), ((), ())), preferred_element_type=F32
        ).astype(BF16)

    def apply_own(parity, t):
        window = own_t[parity, :, t * WIDE : (t + 2) * WIDE]
        for a in range(3):
            app_own[parity, a * modes : (a + 1) * modes, t * WIDE : (t + 1) * WIDE] = jnp.dot(
                window, weights[t, a], preferred_element_type=F32
            ).astype(BF16)

    def apply_up(relay, t):
        window = up_t[relay, :, t * WIDE : (t + 2) * WIDE]
        for a in range(3):
            app_up[relay, a * modes : (a + 1) * modes, t * WIDE : (t + 1) * WIDE] = jnp.dot(
                window, weights[t, a], preferred_element_type=F32
            ).astype(BF16)

    def schedule(arrived, moved, done):
        blocks = []
        for u in range(tiles + 1):
            need = {v for v in (u - 1, u) if 0 <= v < tiles}
            if u not in moved and need <= arrived:
                blocks.append(u)
                moved.add(u)
        ready = [v for v in range(tiles) if v not in done and {v, v + 1} <= moved]
        done.update(ready)
        return blocks, ready

    def forward(t):
        y_copy(t).wait_recv()

        @pl.when(has_up)
        def _():
            z_copy(1, 1, t).start()

        @pl.when(has_dn)
        def _():
            z_copy(0, 1, t).start()

    def await_chunks(relay, from_up, from_dn):
        @pl.when(has_up)
        def _():
            for t in from_up:
                z_copy(0, relay, t).wait_recv()

        @pl.when(has_dn)
        def _():
            for t in from_dn:
                z_copy(1, relay, t).wait_recv()

    forward(order[0])
    local_copy().wait()
    outer_edge().wait_recv()
    for u in range(tiles + 1):
        transposed(own.at[y], own_t.at[y], u)
    for v in range(tiles):
        apply_own(y, v)
        if v == 1:
            forward(order[1])
    await_chunks(0, order[:2], [])

    @pl.when(has_up)
    def _():
        side_copy(0, 0).start()
        side_copy(0, 1).start()

    moved, done, arrived = set(), set(), set(order[:2])

    def own_step():
        blocks, ready = schedule(arrived, moved, done)
        for u in blocks:
            transposed(own.at[other], own_t.at[other], u)
        for v in ready:
            apply_own(other, v)

    await_chunks(0, order[2:3], [])
    transposed(up.at[0], up_t.at[0], 1)
    forward(order[2])
    arrived.add(order[2])
    y_edge().wait_recv()
    across_edge().wait_recv()
    own_step()
    await_chunks(0, order[3:4], [])
    transposed(up.at[0], up_t.at[0], 2)
    apply_up(0, 1)
    forward(order[3])
    arrived.add(order[3])
    own_step()
    await_chunks(0, order[4:], order)
    for u in range(3, tiles):
        transposed(up.at[0], up_t.at[0], u)
    for v in range(2, tiles - 1):
        apply_up(0, v)

    def store(buffer, index, piece):
        count = buffer.shape[0]
        buffer[:, index] = piece.astype(BF16).reshape(count, modes // count, modes)

    def early(c):
        product = jnp.dot(app_own[c], up[0, EDGE : EDGE + rows, :], preferred_element_type=F32)
        for a in range(3):
            store(red_early, 3 * c + a, product[a * modes : (a + 1) * modes])

    early(y)
    for t in order[4:]:
        forward(t)
        arrived.add(t)
        own_step()
    early(other)

    def owner_of(slab):
        place = 0
        bit = 1
        while bit < groups:
            place = 2 * place + (slab // bit) % 2
            bit *= 2
        return place

    mine = owner_of(atom)
    mine_rows = pl.ds(aligned(y * share), share)
    mate_rows = pl.ds(aligned(other * share), share)

    class Scatter:
        def __init__(self, buffer, landing, sems):
            self.buffer, self.landing, self.sems = buffer, landing, sems
            self.copies = []

        def send(self):
            for step in range(1, groups):
                target = (atom + step) % groups
                copy = remote(
                    self.buffer.at[owner_of(target)],
                    self.landing.at[step - 1],
                    self.sems,
                    (step - 1,),
                    (mode, target),
                )
                copy.start()
                self.copies.append(copy)

        def value(self, row):
            total = self.buffer[mine, row].astype(F32)
            for step in range(1, groups):
                total = total + self.landing[step - 1, row].astype(F32)
            return total

        def await_all(self):
            for copy in self.copies[: groups - 1]:
                copy.wait_recv()

        def hand_over(self, target, rows_sent):
            self.await_all()
            for row in range(self.buffer.shape[1]):
                self.buffer[mine, row] = self.value(row).astype(BF16)
            source = self.buffer.at[mine]
            if rows_sent is not None:
                source = source.at[:, rows_sent]
            copy = remote(source, target, self.sems, (groups - 1,), (mate, atom))
            copy.start()
            self.copies.append(copy)

    early_sum = Scatter(red_early, in_early, early_sem)
    early_sum.send()
    own_main = jnp.concatenate([own[j, EDGE : EDGE + rows, :] for j in range(2)], axis=1)
    for c in range(2):
        blocks = own_main if c else own[0, EDGE : EDGE + rows, :]
        product = jnp.dot(app_own[c], blocks, preferred_element_type=F32)
        for at, (first, b) in enumerate(SELF_PAIRS):
            if first == c:
                for a in range(3):
                    piece = product[a * modes : (a + 1) * modes, b * modes : (b + 1) * modes]
                    store(red_self, 3 * at + a, piece)
    self_sum = Scatter(red_self, in_self, self_sem)
    self_sum.send()

    @pl.when(has_up)
    def _():
        side_wait(0, 0).wait_recv()

    def add_next(t, start):
        span = slice(t * WIDE, (t + 1) * WIDE)
        for c in range(2):
            term = jnp.dot(
                app_own[c, :, span],
                up[1, EDGE + t * WIDE : EDGE + (t + 1) * WIDE, :],
                preferred_element_type=F32,
            )
            acc_next[c] = term if start else acc_next[c] + term

    def add_skip(first, last, start):
        span = slice(first * WIDE, (last + 1) * WIDE)
        term = jnp.dot(app_up[1, :, span], dn[1, span, :], preferred_element_type=F32)
        acc_skip[...] = term if start else acc_skip[...] + term
        term = jnp.dot(app_up[y, :, span], dn[other, span, :], preferred_element_type=F32)
        acc_mixed[...] = term if start else acc_mixed[...] + term

    direct_sum = Scatter(red_direct, in_direct, direct_sem)
    next_sum = Scatter(red_next, in_next, next_sem)

    def finish_direct():
        @pl.when(has_up)
        def _():
            side_wait(0, 1).wait_recv()

        for u in (0, tiles):
            transposed(up.at[0], up_t.at[0], u)
        for v in (0, tiles - 1):
            apply_up(0, v)
        product = jnp.dot(app_up[0], dn[0], preferred_element_type=F32)
        for a in range(3):
            store(red_direct, a, product[a * modes : (a + 1) * modes])

    moved, done, arrived = set(), set(), set()
    started = False
    skip_copies = []
    for at, t in enumerate(order):
        await_chunks(1, [t], [t])
        arrived.add(t)
        if at == 1:

            @pl.when(has_up)
            def _():
                side_copy(1, 0).start()
                side_copy(1, 1).start()

        add_next(t, at == 0)
        if at == 1:
            early_sum.hand_over(from_mate.at[pl.ds(0, 6)], None)
        if at == 2:
            finish_direct()
            direct_sum.send()

            @pl.when(has_up)
            def _():
                side_wait(1, 0).wait_recv()
                side_wait(1, 1).wait_recv()

        if at == 3:
            self_sum.hand_over(self_mate, mate_rows)
        if at == tiles - 1:
            for c in range(2):
                for a in range(3):
                    store(red_next, 3 * c + a, acc_next[c, a * modes : (a + 1) * modes, :])
            next_sum.send()
            direct_sum.hand_over(from_mate.at[pl.ds(6, 3)], None)
        if at >= 2:
            blocks, ready = schedule(arrived, moved, done)
            for u in blocks:
                transposed(up.at[1], up_t.at[1], u)
            for v in ready:
                apply_up(1, v)
            runs = [v for v in ready if v - 1 not in ready]
            for v in runs:
                last = v
                while last + 1 in ready:
                    last += 1
                add_skip(v, last, not started)
                started = True

    for a in range(3):
        rows_a = slice(a * modes, (a + 1) * modes)
        store(red_skip, a, acc_skip[rows_a, :])
        store(red_skip, 3 + a, acc_mixed[rows_a, :])
    for step in list(range(1, groups)) + [0]:
        target = (atom + step) % groups
        skip_copies.append(
            remote(
                red_skip.at[owner_of(target), pl.ds(3, 3), mate_rows],
                in_mixed.at[groups - 1 + step],
                mixed_sem,
                (groups - 1 + step,),
                (mate, target),
            )
        )
    for step in range(1, groups):
        target = (atom + step) % groups
        skip_copies.append(
            remote(
                red_skip.at[owner_of(target), pl.ds(3, 3), mine_rows],
                in_mixed.at[step - 1],
                mixed_sem,
                (step - 1,),
                (mode, target),
            )
        )
        skip_copies.append(
            remote(
                red_skip.at[owner_of(target), pl.ds(0, 3)],
                in_skip.at[step - 1],
                skip_sem,
                (step - 1,),
                (mode, target),
            )
        )
    for copy in skip_copies:
        copy.start()

    def frequency(block):
        index = jnp.clip(block, 0, blocks_all - 1)
        return freq_ref[pl.ds(index, 1), :]

    def account(values, first_row, count, c_index, b_index, valid, same=False):
        lane = lax.broadcasted_iota(jnp.int32, (count, modes), 1)
        spot = lane == lax.broadcasted_iota(jnp.int32, (count, modes), 0) + first_row
        squares = None
        for value in values:
            square = value * value
            squares = square if squares is None else squares + square
        c_row = frequency(2 * s - 2 + c_index)
        b_row = frequency(2 * s - 2 + b_index)
        c_col = jnp.sum(jnp.where(spot, c_row, 0.0), axis=1, keepdims=True)
        offset = b_row - c_col
        terms = squares * (half_width / math.pi / (offset * offset + half_width * half_width))
        if valid is not None:
            terms = jnp.where(valid, terms, 0.0)

        def folded(value):
            return jnp.sum(value.reshape(count // 8, 8, modes), axis=0)

        given[b_index] = given[b_index] + folded(terms)
        if not same:
            col_sum = jnp.sum(terms, axis=1, keepdims=True)
            given[c_index] = given[c_index] + folded(jnp.where(spot, col_sum, 0.0))

    self_sum.copies[-1].wait_recv()
    for at, (c, b) in enumerate(SELF_PAIRS):
        values = [
            red_self[mine, 3 * at + a, mine_rows].astype(F32) + self_mate[3 * at + a].astype(F32)
            for a in range(3)
        ]
        account(values, mine * part + y * share, share, 2 + c, 2 + b, None, c == b)

    early_sum.copies[-1].wait_recv()
    direct_sum.copies[-1].wait_recv()
    next_sum.await_all()
    for c in range(2):
        values = [
            next_sum.value(3 * c + a) + from_mate[3 * c + a].astype(F32) for a in range(3)
        ]
        account(values, mine * part, part, 2 + c, 4 + other, has_up)

    both = jnp.logical_and(has_up, has_dn)
    for copy in skip_copies:
        copy.wait_recv()
    values = []
    for a in range(3):
        value = red_skip[mine, a].astype(F32) + from_mate[6 + a].astype(F32)
        for step in range(1, groups):
            value = value + in_skip[step - 1, a].astype(F32)
        values.append(value)
    account(values, mine * part, part, 4 + other, other, both)
    values = []
    for a in range(3):
        value = red_skip[mine, 3 + a, mine_rows].astype(F32)
        for i in range(owners - 1):
            value = value + in_mixed[i, a].astype(F32)
        values.append(value)
    account(values, mine * part + y * share, share, 4, 1, both)

    rank = y * groups + atom

    def final_copy(delta, side, slab):
        slot = (1 - delta) * owners + rank
        return pltpu.make_async_remote_copy(
            src_ref=packed.at[2 * (delta + 1) + side, pl.ds(0, 1)],
            dst_ref=taken.at[slot, pl.ds(0, 1)],
            send_sem=fin_sem.at[0, (delta + 1) * owners + side * groups + slab],
            recv_sem=fin_sem.at[1, slot],
            device_id=(2 * (s + delta) + side, slab),
            device_id_type=MESH,
        )

    def final_wait(delta, side, slab):
        slot = (delta + 1) * owners + side * groups + slab
        return pltpu.make_async_remote_copy(
            src_ref=packed.at[0, pl.ds(0, 1)],
            dst_ref=taken.at[slot, pl.ds(0, 1)],
            send_sem=fin_sem.at[0, slot],
            recv_sem=fin_sem.at[1, slot],
            device_id=(2 * (s + delta) + side, slab),
            device_id_type=MESH,
        )

    def for_all(action):
        for delta, valid in ((1, has_up), (-1, has_dn), (0, None)):
            for turn in (1, 0):
                for step in range(1, groups + 1):
                    if delta == 0 and turn == 0 and step == groups:
                        continue
                    at = (delta, (y + turn) % 2, (atom + step) % groups)
                    if valid is None:
                        action(*at)
                    else:
                        pl.when(valid)(functools.partial(action, *at))

    packed[:, 0:1, :] = jnp.sum(given[...], axis=1, keepdims=True)
    for_all(lambda *at: final_copy(*at).start())
    taken[owners + rank, 0:1] = packed[2 + y, 0:1]
    for_all(lambda *at: final_wait(*at).wait_recv())
    total = jnp.sum(taken[:, 0:1, :], axis=0)
    own_freq = frequency(mode)
    out_ref[...] = total / (own_freq * own_freq)

    for_all(lambda *at: final_copy(*at).wait_send())
    for group in (self_sum, early_sum, direct_sum, next_sum):
        for copy in group.copies:
            copy.wait_send()
    for copy in skip_copies:
        copy.wait_send()
    y_edge().wait_send()
    outer_edge().wait_send()
    across_edge().wait_send()
    for t in range(tiles):
        y_copy(t).wait_send()

    @pl.when(has_up)
    def _():
        for relay in range(2):
            side_copy(relay, 0).wait_send()
            side_copy(relay, 1).wait_send()
            for t in range(tiles):
                z_copy(1, relay, t).wait_send()

    @pl.when(has_dn)
    def _():
        for relay in range(2):
            for t in range(tiles):
                z_copy(0, relay, t).wait_send()


def local(vectors, couplings, neighbours, frequency):
    rows_dev, modes = vectors.shape
    blocks_all = lax.axis_size("mode")
    groups = lax.axis_size("atom")
    half_width = WIDTH_MODES / (modes * blocks_all)
    rows = rows_dev // 2
    tiles = rows // WIDE
    padded = rows + 2 * EDGE
    owners = 2 * groups
    share = modes // owners
    part = modes // groups

    blocks = couplings.transpose(1, 2, 3, 0, 4).reshape(27, SLOTS, rows_dev // 3)
    sizes = (blocks_all, groups, rows_dev, modes, half_width)
    dma = pltpu.SemaphoreType.DMA
    result = pl.pallas_call(
        functools.partial(kernel, sizes),
        out_shape=jax.ShapeDtypeStruct((1, modes), F32),
        in_specs=[pl.BlockSpec(memory_space=pltpu.HBM)] * 4,
        out_specs=pl.BlockSpec(memory_space=pltpu.VMEM),
        scratch_shapes=[
            pltpu.VMEM((2, padded, modes), BF16),
            pltpu.VMEM((2, padded, modes), BF16),
            pltpu.VMEM((2, rows, modes), BF16),
            pltpu.VMEM((2, modes, padded), BF16),
            pltpu.VMEM((2, modes, padded), BF16),
            pltpu.VMEM((27, SLOTS, rows // 3), F32),
            pltpu.VMEM((SLOTS, rows // 3), jnp.int32),
            pltpu.VMEM((blocks_all, modes), F32),
            pltpu.VMEM((3, PERIOD, rows // 3), F32),
            pltpu.VMEM((tiles, 3, 2 * WIDE, WIDE), BF16),
            pltpu.VMEM((WIDE, WIDE), BF16),
            pltpu.VMEM((3 * SLOTS * PERIOD + 16 * SLOTS, PERIOD), BF16),
            pltpu.VMEM((TILE, TILE), BF16),
            pltpu.VMEM((tiles, PERIOD, WIDE), BF16),
            pltpu.VMEM((3 * SLOTS * PERIOD + 16 * SLOTS, WIDE), BF16),
            pltpu.VMEM((2, 3 * modes, rows), BF16),
            pltpu.VMEM((2, 3 * modes, rows), BF16),
            pltpu.VMEM((2, 3 * modes, modes), F32),
            pltpu.VMEM((3 * modes, modes), F32),
            pltpu.VMEM((3 * modes, modes), F32),
            pltpu.VMEM((groups, 9, part, modes), BF16),
            pltpu.VMEM((groups - 1, 9, part, modes), BF16),
            pltpu.VMEM((9, share, modes), BF16),
            pltpu.VMEM((groups, 6, part, modes), BF16),
            pltpu.VMEM((groups - 1, 6, part, modes), BF16),
            pltpu.VMEM((groups, 3, part, modes), BF16),
            pltpu.VMEM((groups - 1, 3, part, modes), BF16),
            pltpu.VMEM((9, part, modes), BF16),
            pltpu.VMEM((groups, 6, part, modes), BF16),
            pltpu.VMEM((groups - 1, 6, part, modes), BF16),
            pltpu.VMEM((groups, 6, part, modes), BF16),
            pltpu.VMEM((groups - 1, 3, part, modes), BF16),
            pltpu.VMEM((owners - 1, 3, share, modes), BF16),
            pltpu.VMEM((6, 8, modes), F32),
            pltpu.VMEM((6, 8, modes), F32),
            pltpu.VMEM((3 * owners, 8, modes), F32),
            dma((4,)),
            dma((2, tiles)),
            dma((2, 2, 2, tiles)),
            dma((2, 3)),
            dma((2, 2, 2)),
            dma((2, groups)),
            dma((2, groups)),
            dma((2, groups)),
            dma((2, groups - 1)),
            dma((2, groups - 1)),
            dma((2, owners - 1)),
            dma((2, 3 * owners)),
        ],
        compiler_params=pltpu.CompilerParams(
            collective_id=0, has_side_effects=True, vmem_limit_bytes=55210 * 1024
        ),
        name="diffusivity",
    )(vectors, blocks, neighbours, frequency.reshape(blocks_all, modes))
    return result.reshape(modes) * (math.pi / 3.0)


def solution(mesh):
    return jax.shard_map(
        local,
        mesh=mesh,
        in_specs=(P("atom", "mode"), P(None, None, None, None, "atom"), P(None, "atom"), P()),
        out_specs=P("mode"),
        check_vma=False,
    )
```

```python
import functools
import math

import jax
import jax.numpy as jnp
from jax import lax
from jax.experimental import pallas as pl
from jax.experimental.pallas import tpu as pltpu
from jax.sharding import PartitionSpec as P

HALO = 64
PARTNERS = 4
WIDTH_MODES = 320
TILE = 128
WIDE = 3 * TILE
EDGE = 3 * HALO
PERIOD = 48
SLOTS = 4
MESH = pl.DeviceIdType.MESH
BF16 = jnp.bfloat16
F32 = jnp.float32

SELF_PAIRS = ((0, 0), (1, 0), (1, 1))


def aligned(value):
    return pl.multiple_of(value, 16)


def band_groups(lane_tile):
    first = (TILE * lane_tile) // 3
    last = (TILE * lane_tile + TILE - 1) // 3
    down = range((3 * first) // PERIOD, (3 * (last + HALO - 2) + 2) // PERIOD + 1)
    up = range((3 * (HALO + first + 2)) // PERIOD, (3 * (2 * HALO + last) + 2) // PERIOD + 1)
    return down, up


def kernel(
    sizes,
    vec,
    couplings,
    neighbours,
    frequencies,
    out_ref,
    own,
    up,
    dn,
    own_t,
    up_t,
    raw,
    near,
    freq_ref,
    gathered,
    weights,
    spread,
    expand,
    eye,
    mixed,
    pattern,
    app_own,
    app_up,
    acc_next,
    acc_skip,
    acc_mixed,
    red_self,
    in_self,
    self_mate,
    red_early,
    in_early,
    red_direct,
    in_direct,
    from_mate,
    red_next,
    in_next,
    red_skip,
    in_skip,
    in_mixed,
    given,
    packed,
    taken,
    local_sem,
    y_sem,
    z_sem,
    edge_sem,
    side_sem,
    self_sem,
    early_sem,
    direct_sem,
    next_sem,
    skip_sem,
    mixed_sem,
    fin_sem,
):
    blocks_all, groups, rows_dev, modes, half_width = sizes
    rows = rows_dev // 2
    atoms = rows // 3
    tiles = rows // WIDE
    owners = 2 * groups
    share = modes // owners
    part = modes // groups

    mode = lax.axis_index("mode")
    atom = lax.axis_index("atom")
    s = mode // 2
    y = mode % 2
    other = 1 - y
    mate = mode + 1 - 2 * y
    h = (y + atom) % 2
    supers = blocks_all // 2
    has_up = s < supers - 1
    has_dn = s > 0
    outer = (atom + 2 * h - 1 + groups) % groups
    across = (atom + 1 - 2 * h + groups) % groups

    def remote(src, dst, sems, at, device):
        return pltpu.make_async_remote_copy(
            src_ref=src,
            dst_ref=dst,
            send_sem=sems.at[(0,) + at],
            recv_sem=sems.at[(1,) + at],
            device_id=device,
            device_id_type=MESH,
        )

    def local_copy():
        size = rows + EDGE
        return pltpu.make_async_copy(
            vec.at[pl.ds(aligned(h * (rows - EDGE)), size), :],
            own.at[y, pl.ds(aligned((1 - h) * EDGE), size), :],
            local_sem.at[0],
        )

    half_lanes = pl.ds(pl.multiple_of(h * atoms, TILE), atoms)
    loads = [
        pltpu.make_async_copy(couplings.at[:, :, half_lanes], raw, local_sem.at[1]),
        pltpu.make_async_copy(neighbours.at[:, half_lanes], near, local_sem.at[2]),
        pltpu.make_async_copy(frequencies, freq_ref, local_sem.at[3]),
    ]
    for load in loads:
        load.start()
    local_copy().start()

    barrier = pltpu.get_barrier_semaphore()

    def greet(device):
        pl.semaphore_signal(barrier, inc=1, device_id=device, device_id_type=MESH)

    pl.when(has_up)(lambda: greet((mode + 2, atom)))
    pl.when(has_dn)(lambda: greet((mode - 2, atom)))
    for step in range(groups):
        slab = (atom + step) % groups
        greet((mate, slab))
        if step:
            greet((mode, slab))
    sides = has_up.astype(jnp.int32) + has_dn.astype(jnp.int32)
    pl.semaphore_wait(barrier, owners - 1 + sides)

    def y_copy(t):
        return remote(
            vec.at[pl.ds(aligned((1 - h) * rows + t * WIDE), WIDE), :],
            own.at[y, pl.ds(aligned(EDGE + t * WIDE), WIDE), :],
            y_sem,
            (t,),
            (mate, atom),
        )

    def y_edge():
        return remote(
            vec.at[pl.ds(aligned(rows - EDGE + h * EDGE), EDGE), :],
            own.at[y, pl.ds(aligned(h * (rows + EDGE)), EDGE), :],
            edge_sem,
            (0,),
            (mate, atom),
        )

    def outer_edge():
        return remote(
            vec.at[pl.ds(aligned(h * (rows_dev - EDGE)), EDGE), :],
            own.at[y, pl.ds(aligned((1 - h) * (rows + EDGE)), EDGE), :],
            edge_sem,
            (1,),
            (mode, outer),
        )

    def across_edge():
        return remote(
            vec.at[pl.ds(aligned((1 - h) * (rows_dev - EDGE)), EDGE), :],
            own.at[y, pl.ds(aligned(h * (rows + EDGE)), EDGE), :],
            edge_sem,
            (2,),
            (mate, across),
        )

    def z_copy(upward, relay, t):
        if relay:
            src = own.at[other, pl.ds(aligned(EDGE + t * WIDE), WIDE), :]
        else:
            src = vec.at[pl.ds(aligned(h * rows + t * WIDE), WIDE), :]
        if upward:
            dst = dn.at[relay, pl.ds(aligned(t * WIDE), WIDE), :]
            return remote(src, dst, z_sem, (0, relay, t), (mode + 2, atom))
        dst = up.at[relay, pl.ds(aligned(EDGE + t * WIDE), WIDE), :]
        return remote(src, dst, z_sem, (1, relay, t), (mode - 2, atom))

    def side_copy(relay, inner):
        if inner:
            src = EDGE + (1 - h) * (rows - EDGE)
            dst = h * (rows + EDGE)
            device = (mate, atom)
            place = 1 - relay
        else:
            src = EDGE + h * (rows - EDGE)
            dst = (1 - h) * (rows + EDGE)
            device = (mode, outer)
            place = relay
        return pltpu.make_async_remote_copy(
            src_ref=up.at[relay, pl.ds(aligned(src), EDGE), :],
            dst_ref=up.at[place, pl.ds(aligned(dst), EDGE), :],
            send_sem=side_sem.at[0, relay, inner],
            recv_sem=side_sem.at[1, place, inner],
            device_id=device,
            device_id_type=MESH,
        )

    def side_wait(place, inner):
        return pltpu.make_async_remote_copy(
            src_ref=up.at[place, pl.ds(0, EDGE), :],
            dst_ref=up.at[place, pl.ds(0, EDGE), :],
            send_sem=side_sem.at[0, place, inner],
            recv_sem=side_sem.at[1, place, inner],
            device_id=(mate, atom),
            device_id_type=MESH,
        )

    order = [tiles - 1] + list(range(tiles - 1))
    for at, t in enumerate(order):
        y_copy(t).start()

        @pl.when(has_up)
        def _():
            z_copy(1, 0, t).start()

        @pl.when(has_dn)
        def _():
            z_copy(0, 0, t).start()

        if at == 1:
            y_edge().start()
            outer_edge().start()
            across_edge().start()

    @pl.when(jnp.logical_not(has_dn))
    def _():
        taken[0:owners] = jnp.zeros((owners, 8, modes), F32)

    @pl.when(jnp.logical_not(has_up))
    def _():
        taken[2 * owners : 3 * owners] = jnp.zeros((owners, 8, modes), F32)

    given[...] = jnp.zeros((6, 8, modes), F32)

    row = lax.broadcasted_iota(jnp.int32, (WIDE, WIDE), 0)
    col = lax.broadcasted_iota(jnp.int32, (WIDE, WIDE), 1)
    spread[...] = jnp.where(col == 3 * (row % TILE) + row // TILE, 1.0, 0.0).astype(BF16)
    row = lax.broadcasted_iota(jnp.int32, (TILE, TILE), 0)
    col = lax.broadcasted_iota(jnp.int32, (TILE, TILE), 1)
    eye[...] = jnp.where(row == col, 1.0, 0.0).astype(BF16)
    height = 3 * SLOTS * PERIOD
    row = lax.broadcasted_iota(jnp.int32, (height + 16 * SLOTS, PERIOD), 0)
    col = lax.broadcasted_iota(jnp.int32, (height + 16 * SLOTS, PERIOD), 1)
    pair = row // PERIOD
    value_col = (3 * (pair % 3) + (row % PERIOD) % 3) * SLOTS + pair // 3
    place_col = 9 * SLOTS + (row - height) // 16
    want = jnp.where(row < height, value_col, place_col)
    expand[...] = jnp.where(col == want, 1.0, 0.0).astype(BF16)

    for load in loads:
        load.wait()
    lane = lax.broadcasted_iota(jnp.int32, (SLOTS, atoms), 1)
    here = atom * (2 * atoms) + h * atoms + lane
    offset = near[...] - here
    total_atoms = 2 * atoms * groups
    offset = jnp.where(offset > HALO, offset - total_atoms, offset)
    offset = jnp.where(offset < -HALO, offset + total_atoms, offset)
    place = (offset + HALO + lane % TILE).astype(F32)
    for p in range(3):
        for a in range(3):
            for q in range(3):
                first = SLOTS * (3 * a + q)
                gathered[p, first : first + SLOTS, :] = raw[9 * a + 3 * p + q]
        gathered[p, 9 * SLOTS : 10 * SLOTS, :] = place
        gathered[p, 10 * SLOTS : PERIOD, :] = jnp.zeros((PERIOD - 10 * SLOTS, atoms), F32)
    stacked = []
    for t in range(tiles):
        lanes = slice(t * TILE, (t + 1) * TILE)
        stacked.append(
            jnp.concatenate([gathered[p, :, lanes].astype(BF16) for p in range(3)], axis=1)
        )
    stacked = jnp.concatenate(stacked, axis=0)
    mixed[...] = (
        jnp.dot(stacked, spread[...], preferred_element_type=F32)
        .astype(BF16)
        .reshape(tiles, PERIOD, WIDE)
    )

    atom_row = (lax.broadcasted_iota(jnp.int32, (PERIOD, TILE), 0) // 3).astype(F32).astype(BF16)
    atom_row = atom_row.reshape(3, 16, TILE)

    def build(t):
        pattern[...] = jnp.dot(expand[...], mixed[t], preferred_element_type=F32).astype(BF16)
        for lane_tile in range(3):
            lanes = slice(lane_tile * TILE, (lane_tile + 1) * TILE)
            down, above = band_groups(lane_tile)
            for g in range(2 * WIDE // PERIOD):
                slots = ([0, 1] if g in above else []) + ([2, 3] if g in down else [])
                span = slice(g * PERIOD, (g + 1) * PERIOD)
                if not slots:
                    for a in range(3):
                        weights[t, a, span, lanes] = jnp.zeros((PERIOD, TILE), BF16)
                    continue
                here = atom_row + jnp.asarray(16.0 * g, BF16)
                flags = {}
                for k in slots:
                    target = pattern[height + 16 * k : height + 16 * (k + 1), lanes]
                    flags[k] = here == target[None]
                for a in range(3):
                    total = None
                    for k in slots:
                        first = (3 * k + a) * PERIOD
                        value = pattern[first : first + PERIOD, lanes].reshape(3, 16, TILE)
                        term = jnp.where(flags[k], value, jnp.zeros_like(value))
                        total = term if total is None else total + term
                    weights[t, a, span, lanes] = total.reshape(PERIOD, TILE)

    def build_step(t, carry):
        build(t)
        return carry

    lax.fori_loop(0, tiles, build_step, 0)

    def transposed(source, target, u):
        span = pl.ds(pl.multiple_of(u * WIDE, WIDE), WIDE)
        target[:, span] = lax.dot_general(
            eye[...], source[span, :], (((1,), (1,)), ((), ())), preferred_element_type=F32
        ).astype(BF16)

    def apply_own(parity, t):
        window = own_t[parity, :, t * WIDE : (t + 2) * WIDE]
        for a in range(3):
            app_own[parity, a * modes : (a + 1) * modes, t * WIDE : (t + 1) * WIDE] = jnp.dot(
                window, weights[t, a], preferred_element_type=F32
            ).astype(BF16)

    def apply_up(relay, t):
        window = up_t[relay, :, t * WIDE : (t + 2) * WIDE]
        for a in range(3):
            app_up[relay, a * modes : (a + 1) * modes, t * WIDE : (t + 1) * WIDE] = jnp.dot(
                window, weights[t, a], preferred_element_type=F32
            ).astype(BF16)

    def schedule(arrived, moved, done):
        blocks = []
        for u in range(tiles + 1):
            need = {v for v in (u - 1, u) if 0 <= v < tiles}
            if u not in moved and need <= arrived:
                blocks.append(u)
                moved.add(u)
        ready = [v for v in range(tiles) if v not in done and {v, v + 1} <= moved]
        done.update(ready)
        return blocks, ready

    def forward(t):
        y_copy(t).wait_recv()

        @pl.when(has_up)
        def _():
            z_copy(1, 1, t).start()

        @pl.when(has_dn)
        def _():
            z_copy(0, 1, t).start()

    def await_chunks(relay, from_up, from_dn):
        @pl.when(has_up)
        def _():
            for t in from_up:
                z_copy(0, relay, t).wait_recv()

        @pl.when(has_dn)
        def _():
            for t in from_dn:
                z_copy(1, relay, t).wait_recv()

    forward(order[0])
    local_copy().wait()
    outer_edge().wait_recv()
    for u in range(tiles + 1):
        transposed(own.at[y], own_t.at[y], u)
    for v in range(tiles):
        apply_own(y, v)
        if v == 1:
            forward(order[1])
    await_chunks(0, order[:2], [])

    @pl.when(has_up)
    def _():
        side_copy(0, 0).start()
        side_copy(0, 1).start()

    moved, done, arrived = set(), set(), set(order[:2])

    def own_step():
        blocks, ready = schedule(arrived, moved, done)
        for u in blocks:
            transposed(own.at[other], own_t.at[other], u)
        for v in ready:
            apply_own(other, v)

    await_chunks(0, order[2:3], [])
    transposed(up.at[0], up_t.at[0], 1)
    forward(order[2])
    arrived.add(order[2])
    y_edge().wait_recv()
    across_edge().wait_recv()
    own_step()
    await_chunks(0, order[3:4], [])
    transposed(up.at[0], up_t.at[0], 2)
    apply_up(0, 1)
    forward(order[3])
    arrived.add(order[3])
    own_step()
    await_chunks(0, order[4:], order)
    for u in range(3, tiles):
        transposed(up.at[0], up_t.at[0], u)
    for v in range(2, tiles - 1):
        apply_up(0, v)

    def store(buffer, index, piece):
        count = buffer.shape[0]
        buffer[:, index] = piece.astype(BF16).reshape(count, modes // count, modes)

    def early(c):
        product = jnp.dot(app_own[c], up[0, EDGE : EDGE + rows, :], preferred_element_type=F32)
        for a in range(3):
            store(red_early, 3 * c + a, product[a * modes : (a + 1) * modes])

    early(y)
    for t in order[4:]:
        forward(t)
        arrived.add(t)
        own_step()
    early(other)

    def owner_of(slab):
        place = 0
        bit = 1
        while bit < groups:
            place = 2 * place + (slab // bit) % 2
            bit *= 2
        return place

    mine = owner_of(atom)
    mine_rows = pl.ds(aligned(y * share), share)
    mate_rows = pl.ds(aligned(other * share), share)

    class Scatter:
        def __init__(self, buffer, landing, sems):
            self.buffer, self.landing, self.sems = buffer, landing, sems
            self.copies = []

        def send(self):
            for step in range(1, groups):
                target = (atom + step) % groups
                copy = remote(
                    self.buffer.at[owner_of(target)],
                    self.landing.at[step - 1],
                    self.sems,
                    (step - 1,),
                    (mode, target),
                )
                copy.start()
                self.copies.append(copy)

        def value(self, row):
            total = self.buffer[mine, row].astype(F32)
            for step in range(1, groups):
                total = total + self.landing[step - 1, row].astype(F32)
            return total

        def await_all(self):
            for copy in self.copies[: groups - 1]:
                copy.wait_recv()

        def hand_over(self, target, rows_sent):
            self.await_all()
            for row in range(self.buffer.shape[1]):
                self.buffer[mine, row] = self.value(row).astype(BF16)
            source = self.buffer.at[mine]
            if rows_sent is not None:
                source = source.at[:, rows_sent]
            copy = remote(source, target, self.sems, (groups - 1,), (mate, atom))
            copy.start()
            self.copies.append(copy)

    early_sum = Scatter(red_early, in_early, early_sem)
    early_sum.send()
    own_main = jnp.concatenate([own[j, EDGE : EDGE + rows, :] for j in range(2)], axis=1)
    for c in range(2):
        blocks = own_main if c else own[0, EDGE : EDGE + rows, :]
        product = jnp.dot(app_own[c], blocks, preferred_element_type=F32)
        for at, (first, b) in enumerate(SELF_PAIRS):
            if first == c:
                for a in range(3):
                    piece = product[a * modes : (a + 1) * modes, b * modes : (b + 1) * modes]
                    store(red_self, 3 * at + a, piece)
    self_sum = Scatter(red_self, in_self, self_sem)
    self_sum.send()

    @pl.when(has_up)
    def _():
        side_wait(0, 0).wait_recv()

    def add_next(t, start):
        span = slice(t * WIDE, (t + 1) * WIDE)
        for c in range(2):
            term = jnp.dot(
                app_own[c, :, span],
                up[1, EDGE + t * WIDE : EDGE + (t + 1) * WIDE, :],
                preferred_element_type=F32,
            )
            acc_next[c] = term if start else acc_next[c] + term

    def add_skip(first, last, start):
        span = slice(first * WIDE, (last + 1) * WIDE)
        term = jnp.dot(app_up[1, :, span], dn[1, span, :], preferred_element_type=F32)
        acc_skip[...] = term if start else acc_skip[...] + term
        term = jnp.dot(app_up[y, :, span], dn[other, span, :], preferred_element_type=F32)
        acc_mixed[...] = term if start else acc_mixed[...] + term

    direct_sum = Scatter(red_direct, in_direct, direct_sem)
    next_sum = Scatter(red_next, in_next, next_sem)

    def finish_direct():
        @pl.when(has_up)
        def _():
            side_wait(0, 1).wait_recv()

        for u in (0, tiles):
            transposed(up.at[0], up_t.at[0], u)
        for v in (0, tiles - 1):
            apply_up(0, v)
        product = jnp.dot(app_up[0], dn[0], preferred_element_type=F32)
        for a in range(3):
            store(red_direct, a, product[a * modes : (a + 1) * modes])

    moved, done, arrived = set(), set(), set()
    started = False
    skip_copies = []
    for at, t in enumerate(order):
        await_chunks(1, [t], [t])
        arrived.add(t)
        if at == 1:

            @pl.when(has_up)
            def _():
                side_copy(1, 0).start()
                side_copy(1, 1).start()

        add_next(t, at == 0)
        if at == 2:
            finish_direct()
            direct_sum.send()
            early_sum.hand_over(from_mate.at[pl.ds(0, 6)], None)

            @pl.when(has_up)
            def _():
                side_wait(1, 0).wait_recv()
                side_wait(1, 1).wait_recv()

        if at == tiles - 1:
            for c in range(2):
                for a in range(3):
                    store(red_next, 3 * c + a, acc_next[c, a * modes : (a + 1) * modes, :])
            next_sum.send()
            self_sum.hand_over(self_mate, mate_rows)
            direct_sum.hand_over(from_mate.at[pl.ds(6, 3)], None)
        if at >= 2:
            blocks, ready = schedule(arrived, moved, done)
            for u in blocks:
                transposed(up.at[1], up_t.at[1], u)
            for v in ready:
                apply_up(1, v)
            runs = [v for v in ready if v - 1 not in ready]
            for v in runs:
                last = v
                while last + 1 in ready:
                    last += 1
                add_skip(v, last, not started)
                started = True

    for a in range(3):
        rows_a = slice(a * modes, (a + 1) * modes)
        store(red_skip, a, acc_skip[rows_a, :])
        store(red_skip, 3 + a, acc_mixed[rows_a, :])
    for step in list(range(1, groups)) + [0]:
        target = (atom + step) % groups
        skip_copies.append(
            remote(
                red_skip.at[owner_of(target), pl.ds(3, 3), mate_rows],
                in_mixed.at[groups - 1 + step],
                mixed_sem,
                (groups - 1 + step,),
                (mate, target),
            )
        )
    for step in range(1, groups):
        target = (atom + step) % groups
        skip_copies.append(
            remote(
                red_skip.at[owner_of(target), pl.ds(3, 3), mine_rows],
                in_mixed.at[step - 1],
                mixed_sem,
                (step - 1,),
                (mode, target),
            )
        )
        skip_copies.append(
            remote(
                red_skip.at[owner_of(target), pl.ds(0, 3)],
                in_skip.at[step - 1],
                skip_sem,
                (step - 1,),
                (mode, target),
            )
        )
    for copy in skip_copies:
        copy.start()

    def frequency(block):
        index = jnp.clip(block, 0, blocks_all - 1)
        return freq_ref[pl.ds(index, 1), :]

    def account(values, first_row, count, c_index, b_index, valid, same=False):
        lane = lax.broadcasted_iota(jnp.int32, (count, modes), 1)
        spot = lane == lax.broadcasted_iota(jnp.int32, (count, modes), 0) + first_row
        squares = None
        for value in values:
            square = value * value
            squares = square if squares is None else squares + square
        c_row = frequency(2 * s - 2 + c_index)
        b_row = frequency(2 * s - 2 + b_index)
        c_col = jnp.sum(jnp.where(spot, c_row, 0.0), axis=1, keepdims=True)
        offset = b_row - c_col
        terms = squares * (half_width / math.pi / (offset * offset + half_width * half_width))
        if valid is not None:
            terms = jnp.where(valid, terms, 0.0)

        def folded(value):
            return jnp.sum(value.reshape(count // 8, 8, modes), axis=0)

        given[b_index] = given[b_index] + folded(terms)
        if not same:
            col_sum = jnp.sum(terms, axis=1, keepdims=True)
            given[c_index] = given[c_index] + folded(jnp.where(spot, col_sum, 0.0))

    self_sum.copies[-1].wait_recv()
    for at, (c, b) in enumerate(SELF_PAIRS):
        values = [
            red_self[mine, 3 * at + a, mine_rows].astype(F32) + self_mate[3 * at + a].astype(F32)
            for a in range(3)
        ]
        account(values, mine * part + y * share, share, 2 + c, 2 + b, None, c == b)

    early_sum.copies[-1].wait_recv()
    direct_sum.copies[-1].wait_recv()
    next_sum.await_all()
    for c in range(2):
        values = [
            next_sum.value(3 * c + a) + from_mate[3 * c + a].astype(F32) for a in range(3)
        ]
        account(values, mine * part, part, 2 + c, 4 + other, has_up)

    both = jnp.logical_and(has_up, has_dn)
    for copy in skip_copies:
        copy.wait_recv()
    values = []
    for a in range(3):
        value = red_skip[mine, a].astype(F32) + from_mate[6 + a].astype(F32)
        for step in range(1, groups):
            value = value + in_skip[step - 1, a].astype(F32)
        values.append(value)
    account(values, mine * part, part, 4 + other, other, both)
    values = []
    for a in range(3):
        value = red_skip[mine, 3 + a, mine_rows].astype(F32)
        for i in range(owners - 1):
            value = value + in_mixed[i, a].astype(F32)
        values.append(value)
    account(values, mine * part + y * share, share, 4, 1, both)

    rank = y * groups + atom

    def final_copy(delta, side, slab):
        slot = (1 - delta) * owners + rank
        return pltpu.make_async_remote_copy(
            src_ref=packed.at[2 * (delta + 1) + side, pl.ds(0, 1)],
            dst_ref=taken.at[slot, pl.ds(0, 1)],
            send_sem=fin_sem.at[0, (delta + 1) * owners + side * groups + slab],
            recv_sem=fin_sem.at[1, slot],
            device_id=(2 * (s + delta) + side, slab),
            device_id_type=MESH,
        )

    def final_wait(delta, side, slab):
        slot = (delta + 1) * owners + side * groups + slab
        return pltpu.make_async_remote_copy(
            src_ref=packed.at[0, pl.ds(0, 1)],
            dst_ref=taken.at[slot, pl.ds(0, 1)],
            send_sem=fin_sem.at[0, slot],
            recv_sem=fin_sem.at[1, slot],
            device_id=(2 * (s + delta) + side, slab),
            device_id_type=MESH,
        )

    def for_all(action):
        for delta, valid in ((1, has_up), (-1, has_dn), (0, None)):
            for turn in (1, 0):
                for step in range(1, groups + 1):
                    if delta == 0 and turn == 0 and step == groups:
                        continue
                    at = (delta, (y + turn) % 2, (atom + step) % groups)
                    if valid is None:
                        action(*at)
                    else:
                        pl.when(valid)(functools.partial(action, *at))

    packed[:, 0:1, :] = jnp.sum(given[...], axis=1, keepdims=True)
    for_all(lambda *at: final_copy(*at).start())
    taken[owners + rank, 0:1] = packed[2 + y, 0:1]
    for_all(lambda *at: final_wait(*at).wait_recv())
    total = jnp.sum(taken[:, 0:1, :], axis=0)
    own_freq = frequency(mode)
    out_ref[...] = total / (own_freq * own_freq)

    for_all(lambda *at: final_copy(*at).wait_send())
    for group in (self_sum, early_sum, direct_sum, next_sum):
        for copy in group.copies:
            copy.wait_send()
    for copy in skip_copies:
        copy.wait_send()
    y_edge().wait_send()
    outer_edge().wait_send()
    across_edge().wait_send()
    for t in range(tiles):
        y_copy(t).wait_send()

    @pl.when(has_up)
    def _():
        for relay in range(2):
            side_copy(relay, 0).wait_send()
            side_copy(relay, 1).wait_send()
            for t in range(tiles):
                z_copy(1, relay, t).wait_send()

    @pl.when(has_dn)
    def _():
        for relay in range(2):
            for t in range(tiles):
                z_copy(0, relay, t).wait_send()


def local(vectors, couplings, neighbours, frequency):
    rows_dev, modes = vectors.shape
    blocks_all = lax.axis_size("mode")
    groups = lax.axis_size("atom")
    half_width = WIDTH_MODES / (modes * blocks_all)
    rows = rows_dev // 2
    tiles = rows // WIDE
    padded = rows + 2 * EDGE
    owners = 2 * groups
    share = modes // owners
    part = modes // groups

    blocks = couplings.transpose(1, 2, 3, 0, 4).reshape(27, SLOTS, rows_dev // 3)
    sizes = (blocks_all, groups, rows_dev, modes, half_width)
    dma = pltpu.SemaphoreType.DMA
    result = pl.pallas_call(
        functools.partial(kernel, sizes),
        out_shape=jax.ShapeDtypeStruct((1, modes), F32),
        in_specs=[pl.BlockSpec(memory_space=pltpu.HBM)] * 4,
        out_specs=pl.BlockSpec(memory_space=pltpu.VMEM),
        scratch_shapes=[
            pltpu.VMEM((2, padded, modes), BF16),
            pltpu.VMEM((2, padded, modes), BF16),
            pltpu.VMEM((2, rows, modes), BF16),
            pltpu.VMEM((2, modes, padded), BF16),
            pltpu.VMEM((2, modes, padded), BF16),
            pltpu.VMEM((27, SLOTS, rows // 3), F32),
            pltpu.VMEM((SLOTS, rows // 3), jnp.int32),
            pltpu.VMEM((blocks_all, modes), F32),
            pltpu.VMEM((3, PERIOD, rows // 3), F32),
            pltpu.VMEM((tiles, 3, 2 * WIDE, WIDE), BF16),
            pltpu.VMEM((WIDE, WIDE), BF16),
            pltpu.VMEM((3 * SLOTS * PERIOD + 16 * SLOTS, PERIOD), BF16),
            pltpu.VMEM((TILE, TILE), BF16),
            pltpu.VMEM((tiles, PERIOD, WIDE), BF16),
            pltpu.VMEM((3 * SLOTS * PERIOD + 16 * SLOTS, WIDE), BF16),
            pltpu.VMEM((2, 3 * modes, rows), BF16),
            pltpu.VMEM((2, 3 * modes, rows), BF16),
            pltpu.VMEM((2, 3 * modes, modes), F32),
            pltpu.VMEM((3 * modes, modes), F32),
            pltpu.VMEM((3 * modes, modes), F32),
            pltpu.VMEM((groups, 9, part, modes), BF16),
            pltpu.VMEM((groups - 1, 9, part, modes), BF16),
            pltpu.VMEM((9, share, modes), BF16),
            pltpu.VMEM((groups, 6, part, modes), BF16),
            pltpu.VMEM((groups - 1, 6, part, modes), BF16),
            pltpu.VMEM((groups, 3, part, modes), BF16),
            pltpu.VMEM((groups - 1, 3, part, modes), BF16),
            pltpu.VMEM((9, part, modes), BF16),
            pltpu.VMEM((groups, 6, part, modes), BF16),
            pltpu.VMEM((groups - 1, 6, part, modes), BF16),
            pltpu.VMEM((groups, 6, part, modes), BF16),
            pltpu.VMEM((groups - 1, 3, part, modes), BF16),
            pltpu.VMEM((owners - 1, 3, share, modes), BF16),
            pltpu.VMEM((6, 8, modes), F32),
            pltpu.VMEM((6, 8, modes), F32),
            pltpu.VMEM((3 * owners, 8, modes), F32),
            dma((4,)),
            dma((2, tiles)),
            dma((2, 2, 2, tiles)),
            dma((2, 3)),
            dma((2, 2, 2)),
            dma((2, groups)),
            dma((2, groups)),
            dma((2, groups)),
            dma((2, groups - 1)),
            dma((2, groups - 1)),
            dma((2, owners - 1)),
            dma((2, 3 * owners)),
        ],
        compiler_params=pltpu.CompilerParams(
            collective_id=0, has_side_effects=True, vmem_limit_bytes=55210 * 1024
        ),
        name="diffusivity",
    )(vectors, blocks, neighbours, frequency.reshape(blocks_all, modes))
    return result.reshape(modes) * (math.pi / 3.0)


def solution(mesh):
    return jax.shard_map(
        local,
        mesh=mesh,
        in_specs=(P("atom", "mode"), P(None, None, None, None, "atom"), P(None, "atom"), P()),
        out_specs=P("mode"),
        check_vma=False,
    )
```

```python
import functools
import math

import jax
import jax.numpy as jnp
from jax import lax
from jax.experimental import pallas as pl
from jax.experimental.pallas import tpu as pltpu
from jax.sharding import PartitionSpec as P

HALO = 64
PARTNERS = 4
WIDTH_MODES = 320
TILE = 128
WIDE = 3 * TILE
EDGE = 3 * HALO
PERIOD = 48
SLOTS = 4
MESH = pl.DeviceIdType.MESH
BF16 = jnp.bfloat16
F32 = jnp.float32

SELF_PAIRS = ((0, 0), (1, 0), (1, 1))


def aligned(value):
    return pl.multiple_of(value, 16)


def band_groups(lane_tile):
    first = (TILE * lane_tile) // 3
    last = (TILE * lane_tile + TILE - 1) // 3
    down = range((3 * first) // PERIOD, (3 * (last + HALO - 2) + 2) // PERIOD + 1)
    up = range((3 * (HALO + first + 2)) // PERIOD, (3 * (2 * HALO + last) + 2) // PERIOD + 1)
    return down, up


def kernel(
    sizes,
    vec,
    couplings,
    neighbours,
    frequencies,
    out_ref,
    own,
    up,
    dn,
    own_t,
    up_t,
    raw,
    near,
    freq_ref,
    gathered,
    weights,
    spread,
    expand,
    eye,
    mixed,
    pattern,
    app_own,
    app_up,
    acc_next,
    acc_skip,
    acc_mixed,
    red_self,
    in_self,
    self_mate,
    red_early,
    in_early,
    red_direct,
    in_direct,
    from_mate,
    red_next,
    in_next,
    red_skip,
    in_skip,
    in_mixed,
    given,
    packed,
    taken,
    local_sem,
    y_sem,
    z_sem,
    edge_sem,
    side_sem,
    self_sem,
    early_sem,
    direct_sem,
    next_sem,
    skip_sem,
    mixed_sem,
    fin_sem,
):
    blocks_all, groups, rows_dev, modes, half_width = sizes
    rows = rows_dev // 2
    atoms = rows // 3
    tiles = rows // WIDE
    owners = 2 * groups
    share = modes // owners
    part = modes // groups

    mode = lax.axis_index("mode")
    atom = lax.axis_index("atom")
    s = mode // 2
    y = mode % 2
    other = 1 - y
    mate = mode + 1 - 2 * y
    h = (y + atom) % 2
    supers = blocks_all // 2
    has_up = s < supers - 1
    has_dn = s > 0
    outer = (atom + 2 * h - 1 + groups) % groups
    across = (atom + 1 - 2 * h + groups) % groups

    def remote(src, dst, sems, at, device):
        return pltpu.make_async_remote_copy(
            src_ref=src,
            dst_ref=dst,
            send_sem=sems.at[(0,) + at],
            recv_sem=sems.at[(1,) + at],
            device_id=device,
            device_id_type=MESH,
        )

    def local_copy():
        size = rows + EDGE
        return pltpu.make_async_copy(
            vec.at[pl.ds(aligned(h * (rows - EDGE)), size), :],
            own.at[y, pl.ds(aligned((1 - h) * EDGE), size), :],
            local_sem.at[0],
        )

    half_lanes = pl.ds(pl.multiple_of(h * atoms, TILE), atoms)
    loads = [
        pltpu.make_async_copy(couplings.at[:, :, half_lanes], raw, local_sem.at[1]),
        pltpu.make_async_copy(neighbours.at[:, half_lanes], near, local_sem.at[2]),
        pltpu.make_async_copy(frequencies, freq_ref, local_sem.at[3]),
    ]
    for load in loads:
        load.start()
    local_copy().start()

    barrier = pltpu.get_barrier_semaphore()

    def greet(device):
        pl.semaphore_signal(barrier, inc=1, device_id=device, device_id_type=MESH)

    pl.when(has_up)(lambda: greet((mode + 2, atom)))
    pl.when(has_dn)(lambda: greet((mode - 2, atom)))
    for step in range(groups):
        slab = (atom + step) % groups
        greet((mate, slab))
        if step:
            greet((mode, slab))
    sides = has_up.astype(jnp.int32) + has_dn.astype(jnp.int32)
    pl.semaphore_wait(barrier, owners - 1 + sides)

    def y_copy(t):
        return remote(
            vec.at[pl.ds(aligned((1 - h) * rows + t * WIDE), WIDE), :],
            own.at[y, pl.ds(aligned(EDGE + t * WIDE), WIDE), :],
            y_sem,
            (t,),
            (mate, atom),
        )

    def y_edge():
        return remote(
            vec.at[pl.ds(aligned(rows - EDGE + h * EDGE), EDGE), :],
            own.at[y, pl.ds(aligned(h * (rows + EDGE)), EDGE), :],
            edge_sem,
            (0,),
            (mate, atom),
        )

    def outer_edge():
        return remote(
            vec.at[pl.ds(aligned(h * (rows_dev - EDGE)), EDGE), :],
            own.at[y, pl.ds(aligned((1 - h) * (rows + EDGE)), EDGE), :],
            edge_sem,
            (1,),
            (mode, outer),
        )

    def across_edge():
        return remote(
            vec.at[pl.ds(aligned((1 - h) * (rows_dev - EDGE)), EDGE), :],
            own.at[y, pl.ds(aligned(h * (rows + EDGE)), EDGE), :],
            edge_sem,
            (2,),
            (mate, across),
        )

    def z_copy(upward, relay, t):
        if relay:
            src = own.at[other, pl.ds(aligned(EDGE + t * WIDE), WIDE), :]
        else:
            src = vec.at[pl.ds(aligned(h * rows + t * WIDE), WIDE), :]
        if upward:
            dst = dn.at[relay, pl.ds(aligned(t * WIDE), WIDE), :]
            return remote(src, dst, z_sem, (0, relay, t), (mode + 2, atom))
        dst = up.at[relay, pl.ds(aligned(EDGE + t * WIDE), WIDE), :]
        return remote(src, dst, z_sem, (1, relay, t), (mode - 2, atom))

    def side_copy(relay, inner):
        if inner:
            src = EDGE + (1 - h) * (rows - EDGE)
            dst = h * (rows + EDGE)
            device = (mate, atom)
            place = 1 - relay
        else:
            src = EDGE + h * (rows - EDGE)
            dst = (1 - h) * (rows + EDGE)
            device = (mode, outer)
            place = relay
        return pltpu.make_async_remote_copy(
            src_ref=up.at[relay, pl.ds(aligned(src), EDGE), :],
            dst_ref=up.at[place, pl.ds(aligned(dst), EDGE), :],
            send_sem=side_sem.at[0, relay, inner],
            recv_sem=side_sem.at[1, place, inner],
            device_id=device,
            device_id_type=MESH,
        )

    def side_wait(place, inner):
        return pltpu.make_async_remote_copy(
            src_ref=up.at[place, pl.ds(0, EDGE), :],
            dst_ref=up.at[place, pl.ds(0, EDGE), :],
            send_sem=side_sem.at[0, place, inner],
            recv_sem=side_sem.at[1, place, inner],
            device_id=(mate, atom),
            device_id_type=MESH,
        )

    order = [tiles - 1] + list(range(tiles - 1))
    for at, t in enumerate(order):
        y_copy(t).start()

        @pl.when(has_up)
        def _():
            z_copy(1, 0, t).start()

        @pl.when(has_dn)
        def _():
            z_copy(0, 0, t).start()

        if at == 1:
            y_edge().start()
            outer_edge().start()
            across_edge().start()

    @pl.when(jnp.logical_not(has_dn))
    def _():
        taken[0:owners] = jnp.zeros((owners, 8, modes), F32)

    @pl.when(jnp.logical_not(has_up))
    def _():
        taken[2 * owners : 3 * owners] = jnp.zeros((owners, 8, modes), F32)

    given[...] = jnp.zeros((6, 8, modes), F32)

    row = lax.broadcasted_iota(jnp.int32, (WIDE, WIDE), 0)
    col = lax.broadcasted_iota(jnp.int32, (WIDE, WIDE), 1)
    spread[...] = jnp.where(col == 3 * (row % TILE) + row // TILE, 1.0, 0.0).astype(BF16)
    row = lax.broadcasted_iota(jnp.int32, (TILE, TILE), 0)
    col = lax.broadcasted_iota(jnp.int32, (TILE, TILE), 1)
    eye[...] = jnp.where(row == col, 1.0, 0.0).astype(BF16)
    height = 3 * SLOTS * PERIOD
    row = lax.broadcasted_iota(jnp.int32, (height + 16 * SLOTS, PERIOD), 0)
    col = lax.broadcasted_iota(jnp.int32, (height + 16 * SLOTS, PERIOD), 1)
    pair = row // PERIOD
    value_col = (3 * (pair % 3) + (row % PERIOD) % 3) * SLOTS + pair // 3
    place_col = 9 * SLOTS + (row - height) // 16
    want = jnp.where(row < height, value_col, place_col)
    expand[...] = jnp.where(col == want, 1.0, 0.0).astype(BF16)

    for load in loads:
        load.wait()
    lane = lax.broadcasted_iota(jnp.int32, (SLOTS, atoms), 1)
    here = atom * (2 * atoms) + h * atoms + lane
    offset = near[...] - here
    total_atoms = 2 * atoms * groups
    offset = jnp.where(offset > HALO, offset - total_atoms, offset)
    offset = jnp.where(offset < -HALO, offset + total_atoms, offset)
    place = (offset + HALO + lane % TILE).astype(F32)
    for p in range(3):
        for a in range(3):
            for q in range(3):
                first = SLOTS * (3 * a + q)
                gathered[p, first : first + SLOTS, :] = raw[9 * a + 3 * p + q]
        gathered[p, 9 * SLOTS : 10 * SLOTS, :] = place
        gathered[p, 10 * SLOTS : PERIOD, :] = jnp.zeros((PERIOD - 10 * SLOTS, atoms), F32)
    stacked = []
    for t in range(tiles):
        lanes = slice(t * TILE, (t + 1) * TILE)
        stacked.append(
            jnp.concatenate([gathered[p, :, lanes].astype(BF16) for p in range(3)], axis=1)
        )
    stacked = jnp.concatenate(stacked, axis=0)
    mixed[...] = (
        jnp.dot(stacked, spread[...], preferred_element_type=F32)
        .astype(BF16)
        .reshape(tiles, PERIOD, WIDE)
    )

    atom_row = (lax.broadcasted_iota(jnp.int32, (PERIOD, TILE), 0) // 3).astype(F32).astype(BF16)
    atom_row = atom_row.reshape(3, 16, TILE)

    def build(t):
        pattern[...] = jnp.dot(expand[...], mixed[t], preferred_element_type=F32).astype(BF16)
        for lane_tile in range(3):
            lanes = slice(lane_tile * TILE, (lane_tile + 1) * TILE)
            down, above = band_groups(lane_tile)
            for g in range(2 * WIDE // PERIOD):
                slots = ([0, 1] if g in above else []) + ([2, 3] if g in down else [])
                span = slice(g * PERIOD, (g + 1) * PERIOD)
                if not slots:
                    for a in range(3):
                        weights[t, a, span, lanes] = jnp.zeros((PERIOD, TILE), BF16)
                    continue
                here = atom_row + jnp.asarray(16.0 * g, BF16)
                flags = {}
                for k in slots:
                    target = pattern[height + 16 * k : height + 16 * (k + 1), lanes]
                    flags[k] = here == target[None]
                for a in range(3):
                    total = None
                    for k in slots:
                        first = (3 * k + a) * PERIOD
                        value = pattern[first : first + PERIOD, lanes].reshape(3, 16, TILE)
                        term = jnp.where(flags[k], value, jnp.zeros_like(value))
                        total = term if total is None else total + term
                    weights[t, a, span, lanes] = total.reshape(PERIOD, TILE)

    def build_step(t, carry):
        build(t)
        return carry

    lax.fori_loop(0, tiles, build_step, 0)

    def transposed(source, target, u):
        span = pl.ds(pl.multiple_of(u * WIDE, WIDE), WIDE)
        target[:, span] = lax.dot_general(
            eye[...], source[span, :], (((1,), (1,)), ((), ())), preferred_element_type=F32
        ).astype(BF16)

    def apply_own(parity, t):
        window = own_t[parity, :, t * WIDE : (t + 2) * WIDE]
        for a in range(3):
            app_own[parity, a * modes : (a + 1) * modes, t * WIDE : (t + 1) * WIDE] = jnp.dot(
                window, weights[t, a], preferred_element_type=F32
            ).astype(BF16)

    def apply_up(relay, t):
        window = up_t[relay, :, t * WIDE : (t + 2) * WIDE]
        for a in range(3):
            app_up[relay, a * modes : (a + 1) * modes, t * WIDE : (t + 1) * WIDE] = jnp.dot(
                window, weights[t, a], preferred_element_type=F32
            ).astype(BF16)

    def schedule(arrived, moved, done):
        blocks = []
        for u in range(tiles + 1):
            need = {v for v in (u - 1, u) if 0 <= v < tiles}
            if u not in moved and need <= arrived:
                blocks.append(u)
                moved.add(u)
        ready = [v for v in range(tiles) if v not in done and {v, v + 1} <= moved]
        done.update(ready)
        return blocks, ready

    def forward(t):
        y_copy(t).wait_recv()

        @pl.when(has_up)
        def _():
            z_copy(1, 1, t).start()

        @pl.when(has_dn)
        def _():
            z_copy(0, 1, t).start()

    def await_chunks(relay, from_up, from_dn):
        @pl.when(has_up)
        def _():
            for t in from_up:
                z_copy(0, relay, t).wait_recv()

        @pl.when(has_dn)
        def _():
            for t in from_dn:
                z_copy(1, relay, t).wait_recv()

    forward(order[0])
    local_copy().wait()
    outer_edge().wait_recv()
    for u in range(tiles + 1):
        transposed(own.at[y], own_t.at[y], u)
    for v in range(tiles):
        apply_own(y, v)
        if v == 1:
            forward(order[1])
    await_chunks(0, order[:2], [])

    @pl.when(has_up)
    def _():
        side_copy(0, 0).start()
        side_copy(0, 1).start()

    moved, done, arrived = set(), set(), set(order[:2])

    def own_step():
        blocks, ready = schedule(arrived, moved, done)
        for u in blocks:
            transposed(own.at[other], own_t.at[other], u)
        for v in ready:
            apply_own(other, v)

    await_chunks(0, order[2:3], [])
    transposed(up.at[0], up_t.at[0], 1)
    forward(order[2])
    arrived.add(order[2])
    y_edge().wait_recv()
    across_edge().wait_recv()
    own_step()
    await_chunks(0, order[3:4], [])
    transposed(up.at[0], up_t.at[0], 2)
    apply_up(0, 1)
    forward(order[3])
    arrived.add(order[3])
    own_step()
    await_chunks(0, order[4:], order)
    for u in range(3, tiles):
        transposed(up.at[0], up_t.at[0], u)
    for v in range(2, tiles - 1):
        apply_up(0, v)

    def store(buffer, index, piece):
        count = buffer.shape[0]
        buffer[:, index] = piece.astype(BF16).reshape(count, modes // count, modes)

    def early(c):
        product = jnp.dot(app_own[c], up[0, EDGE : EDGE + rows, :], preferred_element_type=F32)
        for a in range(3):
            store(red_early, 3 * c + a, product[a * modes : (a + 1) * modes])

    early(y)
    for t in order[4:]:
        forward(t)
        arrived.add(t)
        own_step()
    early(other)

    def owner_of(slab):
        place = 0
        bit = 1
        while bit < groups:
            place = 2 * place + (slab // bit) % 2
            bit *= 2
        return place

    mine = owner_of(atom)
    mine_rows = pl.ds(aligned(y * share), share)
    mate_rows = pl.ds(aligned(other * share), share)

    class Scatter:
        def __init__(self, buffer, landing, sems):
            self.buffer, self.landing, self.sems = buffer, landing, sems
            self.copies = []

        def send(self):
            for step in range(1, groups):
                target = (atom + step) % groups
                copy = remote(
                    self.buffer.at[owner_of(target)],
                    self.landing.at[step - 1],
                    self.sems,
                    (step - 1,),
                    (mode, target),
                )
                copy.start()
                self.copies.append(copy)

        def value(self, row):
            total = self.buffer[mine, row].astype(F32)
            for step in range(1, groups):
                total = total + self.landing[step - 1, row].astype(F32)
            return total

        def await_all(self):
            for copy in self.copies[: groups - 1]:
                copy.wait_recv()

        def hand_over(self, target, rows_sent):
            self.await_all()
            for row in range(self.buffer.shape[1]):
                self.buffer[mine, row] = self.value(row).astype(BF16)
            source = self.buffer.at[mine]
            if rows_sent is not None:
                source = source.at[:, rows_sent]
            copy = remote(source, target, self.sems, (groups - 1,), (mate, atom))
            copy.start()
            self.copies.append(copy)

    early_sum = Scatter(red_early, in_early, early_sem)
    early_sum.send()
    own_main = jnp.concatenate([own[j, EDGE : EDGE + rows, :] for j in range(2)], axis=1)
    for c in range(2):
        blocks = own_main if c else own[0, EDGE : EDGE + rows, :]
        product = jnp.dot(app_own[c], blocks, preferred_element_type=F32)
        for at, (first, b) in enumerate(SELF_PAIRS):
            if first == c:
                for a in range(3):
                    piece = product[a * modes : (a + 1) * modes, b * modes : (b + 1) * modes]
                    store(red_self, 3 * at + a, piece)
    self_sum = Scatter(red_self, in_self, self_sem)
    self_sum.send()

    @pl.when(has_up)
    def _():
        side_wait(0, 0).wait_recv()

    def add_next(t, start):
        span = slice(t * WIDE, (t + 1) * WIDE)
        for c in range(2):
            term = jnp.dot(
                app_own[c, :, span],
                up[1, EDGE + t * WIDE : EDGE + (t + 1) * WIDE, :],
                preferred_element_type=F32,
            )
            acc_next[c] = term if start else acc_next[c] + term

    def add_skip(first, last, start):
        span = slice(first * WIDE, (last + 1) * WIDE)
        term = jnp.dot(app_up[1, :, span], dn[1, span, :], preferred_element_type=F32)
        acc_skip[...] = term if start else acc_skip[...] + term
        term = jnp.dot(app_up[y, :, span], dn[other, span, :], preferred_element_type=F32)
        acc_mixed[...] = term if start else acc_mixed[...] + term

    direct_sum = Scatter(red_direct, in_direct, direct_sem)
    next_sum = Scatter(red_next, in_next, next_sem)

    def finish_direct():
        @pl.when(has_up)
        def _():
            side_wait(0, 1).wait_recv()

        for u in (0, tiles):
            transposed(up.at[0], up_t.at[0], u)
        for v in (0, tiles - 1):
            apply_up(0, v)
        product = jnp.dot(app_up[0], dn[0], preferred_element_type=F32)
        for a in range(3):
            store(red_direct, a, product[a * modes : (a + 1) * modes])

    moved, done, arrived = set(), set(), set()
    started = False
    skip_copies = []
    for at, t in enumerate(order):
        await_chunks(1, [t], [t])
        arrived.add(t)
        if at == 1:

            @pl.when(has_up)
            def _():
                side_copy(1, 0).start()
                side_copy(1, 1).start()

        add_next(t, at == 0)
        if at == 2:
            finish_direct()
            direct_sum.send()
            early_sum.hand_over(from_mate.at[pl.ds(0, 6)], None)

            @pl.when(has_up)
            def _():
                side_wait(1, 0).wait_recv()
                side_wait(1, 1).wait_recv()

        if at == tiles - 1:
            for c in range(2):
                for a in range(3):
                    store(red_next, 3 * c + a, acc_next[c, a * modes : (a + 1) * modes, :])
            next_sum.send()
            self_sum.hand_over(self_mate, mate_rows)
            direct_sum.hand_over(from_mate.at[pl.ds(6, 3)], None)
        if at >= 2:
            blocks, ready = schedule(arrived, moved, done)
            for u in blocks:
                transposed(up.at[1], up_t.at[1], u)
            for v in ready:
                apply_up(1, v)
            runs = [v for v in ready if v - 1 not in ready]
            for v in runs:
                last = v
                while last + 1 in ready:
                    last += 1
                add_skip(v, last, not started)
                started = True

    for a in range(3):
        rows_a = slice(a * modes, (a + 1) * modes)
        store(red_skip, a, acc_skip[rows_a, :])
        store(red_skip, 3 + a, acc_mixed[rows_a, :])
    for step in list(range(1, groups)) + [0]:
        target = (atom + step) % groups
        skip_copies.append(
            remote(
                red_skip.at[owner_of(target), pl.ds(3, 3), mate_rows],
                in_mixed.at[groups - 1 + step],
                mixed_sem,
                (groups - 1 + step,),
                (mate, target),
            )
        )
    for step in range(1, groups):
        target = (atom + step) % groups
        skip_copies.append(
            remote(
                red_skip.at[owner_of(target), pl.ds(3, 3), mine_rows],
                in_mixed.at[step - 1],
                mixed_sem,
                (step - 1,),
                (mode, target),
            )
        )
        skip_copies.append(
            remote(
                red_skip.at[owner_of(target), pl.ds(0, 3)],
                in_skip.at[step - 1],
                skip_sem,
                (step - 1,),
                (mode, target),
            )
        )
    for copy in skip_copies:
        copy.start()

    def frequency(block):
        index = jnp.clip(block, 0, blocks_all - 1)
        return freq_ref[pl.ds(index, 1), :]

    def account(values, first_row, count, c_index, b_index, valid, same=False):
        lane = lax.broadcasted_iota(jnp.int32, (count, modes), 1)
        spot = lane == lax.broadcasted_iota(jnp.int32, (count, modes), 0) + first_row
        squares = None
        for value in values:
            square = value * value
            squares = square if squares is None else squares + square
        c_row = frequency(2 * s - 2 + c_index)
        b_row = frequency(2 * s - 2 + b_index)
        c_col = jnp.sum(jnp.where(spot, c_row, 0.0), axis=1, keepdims=True)
        offset = b_row - c_col
        terms = squares * (half_width / math.pi / (offset * offset + half_width * half_width))
        if valid is not None:
            terms = jnp.where(valid, terms, 0.0)

        def folded(value):
            return jnp.sum(value.reshape(count // 8, 8, modes), axis=0)

        given[b_index] = given[b_index] + folded(terms)
        if not same:
            col_sum = jnp.sum(terms, axis=1, keepdims=True)
            given[c_index] = given[c_index] + folded(jnp.where(spot, col_sum, 0.0))

    self_sum.copies[-1].wait_recv()
    for at, (c, b) in enumerate(SELF_PAIRS):
        values = [
            red_self[mine, 3 * at + a, mine_rows].astype(F32) + self_mate[3 * at + a].astype(F32)
            for a in range(3)
        ]
        account(values, mine * part + y * share, share, 2 + c, 2 + b, None, c == b)

    early_sum.copies[-1].wait_recv()
    direct_sum.copies[-1].wait_recv()
    next_sum.await_all()
    for c in range(2):
        values = [
            next_sum.value(3 * c + a) + from_mate[3 * c + a].astype(F32) for a in range(3)
        ]
        account(values, mine * part, part, 2 + c, 4 + other, has_up)

    both = jnp.logical_and(has_up, has_dn)
    for copy in skip_copies:
        copy.wait_recv()
    values = []
    for a in range(3):
        value = red_skip[mine, a].astype(F32) + from_mate[6 + a].astype(F32)
        for step in range(1, groups):
            value = value + in_skip[step - 1, a].astype(F32)
        values.append(value)
    account(values, mine * part, part, 4 + other, other, both)
    values = []
    for a in range(3):
        value = red_skip[mine, 3 + a, mine_rows].astype(F32)
        for i in range(owners - 1):
            value = value + in_mixed[i, a].astype(F32)
        values.append(value)
    account(values, mine * part + y * share, share, 4, 1, both)

    rank = y * groups + atom

    def final_copy(delta, side, slab):
        slot = (1 - delta) * owners + rank
        return pltpu.make_async_remote_copy(
            src_ref=packed.at[2 * (delta + 1) + side, pl.ds(0, 1)],
            dst_ref=taken.at[slot, pl.ds(0, 1)],
            send_sem=fin_sem.at[0, (delta + 1) * owners + side * groups + slab],
            recv_sem=fin_sem.at[1, slot],
            device_id=(2 * (s + delta) + side, slab),
            device_id_type=MESH,
        )

    def final_wait(delta, side, slab):
        slot = (delta + 1) * owners + side * groups + slab
        return pltpu.make_async_remote_copy(
            src_ref=packed.at[0, pl.ds(0, 1)],
            dst_ref=taken.at[slot, pl.ds(0, 1)],
            send_sem=fin_sem.at[0, slot],
            recv_sem=fin_sem.at[1, slot],
            device_id=(2 * (s + delta) + side, slab),
            device_id_type=MESH,
        )

    def for_all(action):
        for delta, valid in ((1, has_up), (-1, has_dn), (0, None)):
            for turn in (1, 0):
                for step in range(1, groups + 1):
                    if delta == 0 and turn == 0 and step == groups:
                        continue
                    at = (delta, (y + turn) % 2, (atom + step) % groups)
                    if valid is None:
                        action(*at)
                    else:
                        pl.when(valid)(functools.partial(action, *at))

    packed[:, 0:1, :] = jnp.sum(given[...], axis=1, keepdims=True)
    for_all(lambda *at: final_copy(*at).start())
    taken[owners + rank, 0:1] = packed[2 + y, 0:1]
    for group in (self_sum, early_sum, direct_sum, next_sum):
        for copy in group.copies:
            copy.wait_send()
    for copy in skip_copies:
        copy.wait_send()
    y_edge().wait_send()
    outer_edge().wait_send()
    across_edge().wait_send()
    for t in range(tiles):
        y_copy(t).wait_send()

    @pl.when(has_up)
    def _():
        for relay in range(2):
            side_copy(relay, 0).wait_send()
            side_copy(relay, 1).wait_send()
            for t in range(tiles):
                z_copy(1, relay, t).wait_send()

    @pl.when(has_dn)
    def _():
        for relay in range(2):
            for t in range(tiles):
                z_copy(0, relay, t).wait_send()

    for_all(lambda *at: final_wait(*at).wait_recv())
    total = jnp.sum(taken[:, 0:1, :], axis=0)
    own_freq = frequency(mode)
    out_ref[...] = total / (own_freq * own_freq)

    for_all(lambda *at: final_copy(*at).wait_send())


def local(vectors, couplings, neighbours, frequency):
    rows_dev, modes = vectors.shape
    blocks_all = lax.axis_size("mode")
    groups = lax.axis_size("atom")
    half_width = WIDTH_MODES / (modes * blocks_all)
    rows = rows_dev // 2
    tiles = rows // WIDE
    padded = rows + 2 * EDGE
    owners = 2 * groups
    share = modes // owners
    part = modes // groups

    blocks = couplings.transpose(1, 2, 3, 0, 4).reshape(27, SLOTS, rows_dev // 3)
    sizes = (blocks_all, groups, rows_dev, modes, half_width)
    dma = pltpu.SemaphoreType.DMA
    result = pl.pallas_call(
        functools.partial(kernel, sizes),
        out_shape=jax.ShapeDtypeStruct((1, modes), F32),
        in_specs=[pl.BlockSpec(memory_space=pltpu.HBM)] * 4,
        out_specs=pl.BlockSpec(memory_space=pltpu.VMEM),
        scratch_shapes=[
            pltpu.VMEM((2, padded, modes), BF16),
            pltpu.VMEM((2, padded, modes), BF16),
            pltpu.VMEM((2, rows, modes), BF16),
            pltpu.VMEM((2, modes, padded), BF16),
            pltpu.VMEM((2, modes, padded), BF16),
            pltpu.VMEM((27, SLOTS, rows // 3), F32),
            pltpu.VMEM((SLOTS, rows // 3), jnp.int32),
            pltpu.VMEM((blocks_all, modes), F32),
            pltpu.VMEM((3, PERIOD, rows // 3), F32),
            pltpu.VMEM((tiles, 3, 2 * WIDE, WIDE), BF16),
            pltpu.VMEM((WIDE, WIDE), BF16),
            pltpu.VMEM((3 * SLOTS * PERIOD + 16 * SLOTS, PERIOD), BF16),
            pltpu.VMEM((TILE, TILE), BF16),
            pltpu.VMEM((tiles, PERIOD, WIDE), BF16),
            pltpu.VMEM((3 * SLOTS * PERIOD + 16 * SLOTS, WIDE), BF16),
            pltpu.VMEM((2, 3 * modes, rows), BF16),
            pltpu.VMEM((2, 3 * modes, rows), BF16),
            pltpu.VMEM((2, 3 * modes, modes), F32),
            pltpu.VMEM((3 * modes, modes), F32),
            pltpu.VMEM((3 * modes, modes), F32),
            pltpu.VMEM((groups, 9, part, modes), BF16),
            pltpu.VMEM((groups - 1, 9, part, modes), BF16),
            pltpu.VMEM((9, share, modes), BF16),
            pltpu.VMEM((groups, 6, part, modes), BF16),
            pltpu.VMEM((groups - 1, 6, part, modes), BF16),
            pltpu.VMEM((groups, 3, part, modes), BF16),
            pltpu.VMEM((groups - 1, 3, part, modes), BF16),
            pltpu.VMEM((9, part, modes), BF16),
            pltpu.VMEM((groups, 6, part, modes), BF16),
            pltpu.VMEM((groups - 1, 6, part, modes), BF16),
            pltpu.VMEM((groups, 6, part, modes), BF16),
            pltpu.VMEM((groups - 1, 3, part, modes), BF16),
            pltpu.VMEM((owners - 1, 3, share, modes), BF16),
            pltpu.VMEM((6, 8, modes), F32),
            pltpu.VMEM((6, 8, modes), F32),
            pltpu.VMEM((3 * owners, 8, modes), F32),
            dma((4,)),
            dma((2, tiles)),
            dma((2, 2, 2, tiles)),
            dma((2, 3)),
            dma((2, 2, 2)),
            dma((2, groups)),
            dma((2, groups)),
            dma((2, groups)),
            dma((2, groups - 1)),
            dma((2, groups - 1)),
            dma((2, owners - 1)),
            dma((2, 3 * owners)),
        ],
        compiler_params=pltpu.CompilerParams(
            collective_id=0, has_side_effects=True, vmem_limit_bytes=55210 * 1024
        ),
        name="diffusivity",
    )(vectors, blocks, neighbours, frequency.reshape(blocks_all, modes))
    return result.reshape(modes) * (math.pi / 3.0)


def solution(mesh):
    return jax.shard_map(
        local,
        mesh=mesh,
        in_specs=(P("atom", "mode"), P(None, None, None, None, "atom"), P(None, "atom"), P()),
        out_specs=P("mode"),
        check_vma=False,
    )
```
